32 devices in a mesh: seq: 4 (over y, x), dp: 8 (over z, core).
Axes of the slice: x: 2, y: 2, z: 4, core: 2. Of those that a mesh axis runs over, the one named last changes fastest.
Arguments:
- inputs: bfloat16 [8, 512, 2048], P('dp', 'seq'), may hold values from -6 to 6
- first_gain: bfloat16 [2048], P(('seq', 'dp')), may hold values from 0.099609375 to 1.8984375
- first_shift: bfloat16 [2048], P(('seq', 'dp')), may hold values from -2 to 2
- qkv_weight: bfloat16 [2048, 6144], P(('seq', 'dp')), may hold values from -0.125 to 0.125
- qkv_bias: bfloat16 [6144], P(('seq', 'dp')), may hold values from -3 to 3
- out_weight: bfloat16 [2048, 2048], P(('seq', 'dp')), may hold values from -1 to 1
- second_gain: bfloat16 [2048], P(('seq', 'dp')), may hold values from 0.099609375 to 1.8984375
- second_shift: bfloat16 [2048], P(('seq', 'dp')), may hold values from -2 to 2
- gate_weight: bfloat16 [2048, 5632], P(('seq', 'dp')), may hold values from -0.125 to 0.125
- up_weight: bfloat16 [2048, 5632], P(('seq', 'dp')), may hold values from -0.125 to 0.125
- down_weight: bfloat16 [5632, 2048], P(('seq', 'dp')), may hold values from -0.15625 to 0.15625
- out_cotangent: bfloat16 [8, 512, 2048], P('dp', 'seq'), may hold values from -6 to 6
Outputs:
- outputs: bfloat16 [8, 512, 2048], P('dp', 'seq')
- inputs_grad: bfloat16 [8, 512, 2048], P('dp', 'seq')
- first_gain_grad: float32 [2048], P(('seq', 'dp'))
- first_shift_grad: float32 [2048], P(('seq', 'dp'))
- qkv_weight_grad: float32 [2048, 6144], P(('seq', 'dp'))
- qkv_bias_grad: float32 [6144], P(('seq', 'dp'))
- out_weight_grad: float32 [2048, 2048], P(('seq', 'dp'))
- second_gain_grad: float32 [2048], P(('seq', 'dp'))
- second_shift_grad: float32 [2048], P(('seq', 'dp'))
- gate_weight_grad: float32 [2048, 5632], P(('seq', 'dp'))
- up_weight_grad: float32 [2048, 5632], P(('seq', 'dp'))
- down_weight_grad: float32 [5632, 2048], P(('seq', 'dp'))
The draws below stay inside these ranges and needn't reach their ends.
All inputs are finite; a program needn't handle non-finite values.
Results may differ from the reference program's by a relative error of at most 0.017.
Values may be sent and summed in bfloat16 or wider, within the bound.
A program may use at most 256 MiB of HBM per device.

```python
import jax
import jax.numpy as jnp
from jax import lax

D = 2048
HEADS = 32
HEAD_DIM = 64
FF = 5632
ROT = 16
LEN = 512
SEQS = 8


def block_scale(rng, dims, shards, low, largest):
    def one(axis_at, parts):
        heights = jax.random.uniform(jax.random.fold_in(jax.random.fold_in(rng, 6), axis_at), (parts,), jnp.float32, low / len(shards), largest / len(shards))
        return jnp.repeat(jnp.exp(heights), dims[axis_at] // parts).reshape((-1,) + (1,) * (len(dims) - axis_at - 1))

    factor_of = one(*shards[0])
    for cut in shards[1:]:
        factor_of = factor_of * one(*cut)
    return factor_of


def scatter_about(rng, extent, deviation, bound, split=(), kind=jnp.bfloat16):
    entries = jax.random.normal(rng, extent, jnp.float32) * deviation
    if len(split) > 0:
        entries = block_scale(rng, extent, split, -0.22, 0.18) * entries
    return jnp.clip(entries, min=-bound, max=bound).astype(kind)


def setup_inputs(seed: int = 0) -> dict:
    splits = jax.random.split(jax.random.key(seed), 13)
    inputs = scatter_about(splits[0], (SEQS, LEN, D), 1.0, 6.0, ((0, 8), (1, 4)))
    first_gain = jnp.clip(1.0 + 0.18 * jax.random.normal(splits[1], (D,), jnp.float32), 0.099609375, 1.8984375).astype(jnp.bfloat16)
    first_shift = scatter_about(splits[2], (D,), 0.3, 2.0, ((0, 32),))
    qkv_weight = scatter_about(splits[3], (D, 3 * D), D ** -0.5, 0.125, ((0, 32),))
    qkv_bias = scatter_about(splits[4], (3 * D,), 0.5, 3.0, ((0, 32),))
    out_weight = scatter_about(splits[5], (D, D), (D // 64) ** -0.5, 1.0, ((0, 32),))
    second_gain = jnp.clip(1.0 + 0.18 * jax.random.normal(splits[6], (D,), jnp.float32), 0.099609375, 1.8984375).astype(jnp.bfloat16)
    second_shift = scatter_about(splits[7], (D,), 0.3, 2.0, ((0, 32),))
    gate_weight = scatter_about(splits[8], (D, FF), D ** -0.5, 0.125, ((0, 32),))
    up_weight = scatter_about(splits[9], (D, FF), D ** -0.5, 0.125, ((0, 32),))
    down_weight = scatter_about(splits[10], (FF, D), (FF // 4) ** -0.5, 0.15625, ((0, 32),))
    out_cotangent = scatter_about(splits[11], (SEQS, LEN, D), 1.0, 6.0, ((0, 8), (1, 4)))
    return {"inputs": inputs, "first_gain": first_gain, "first_shift": first_shift, "qkv_weight": qkv_weight, "qkv_bias": qkv_bias, "out_weight": out_weight, "second_gain": second_gain, "second_shift": second_shift, "gate_weight": gate_weight, "up_weight": up_weight, "down_weight": down_weight, "out_cotangent": out_cotangent}


@jax.custom_vjp
def low(v):
    return lax.optimization_barrier(v.astype(jnp.bfloat16)).astype(jnp.float32)

@jax.custom_vjp
def low_back(v):
    return v

def low_keep(v):
    return (low(v), None)

def low_pass(kept, grad):
    return (grad,)

def back_keep(v):
    return (v, None)

def back_low(kept, grad):
    return (low(grad),)
low.defvjp(low_keep, low_pass)
low_back.defvjp(back_keep, back_low)
HIGHEST = lax.Precision.HIGHEST

def normalize_affine(values, gain, shift):
    center = values - lax.optimization_barrier(jnp.mean(values, axis=-1, keepdims=True))
    variance = lax.optimization_barrier(jnp.mean(center * center, axis=-1, keepdims=True))
    return center * lax.rsqrt(variance + 1e-05) * gain + shift

def tables(positions):
    half_rot = ROT // 2
    freqs = 10000.0 ** (-(2.0 * jnp.arange(half_rot, dtype=jnp.float32)) / ROT)
    angles = positions[:, None] * freqs[None, :]
    cosine = jnp.cos(angles)
    sine = jnp.sin(angles)
    return (jnp.concatenate([cosine, cosine], -1), jnp.concatenate([sine, sine], -1))

def rotate(heads_in, cosine, sine):
    half_rot = ROT // 2
    rotary = heads_in[..., :ROT]
    turned = jnp.concatenate([-rotary[..., half_rot:], rotary[..., :half_rot]], -1)
    moved = rotary * cosine[:, None, :] + turned * sine[:, None, :]
    return jnp.concatenate([moved, heads_in[..., ROT:]], -1)

def attention(queries, keys_all, values_all):
    block_rows = min(512, LEN)
    blocks = LEN // block_rows
    scale = HEAD_DIM ** (-0.5)
    key_index = jnp.arange(LEN, dtype=jnp.int32)

    def one_block(first_query):
        query_block = lax.dynamic_slice_in_dim(queries, first_query, block_rows, 0)
        scores = jnp.einsum('qhd,khd->hqk', query_block, keys_all, precision=HIGHEST) * scale
        scores = low_back(scores)
        query_index = first_query + jnp.arange(block_rows, dtype=jnp.int32)
        allowed = key_index[None, None, :] <= query_index[None, :, None]
        scores = jnp.where(allowed, scores, -jnp.inf)
        probs = low(jax.nn.softmax(scores, axis=-1))
        return jnp.einsum('hqk,khd->qhd', probs, values_all, precision=HIGHEST)
    firsts = jnp.arange(blocks, dtype=jnp.int32) * block_rows
    mixed = lax.map(jax.checkpoint(one_block), firsts)
    return mixed.reshape(LEN, HEADS * HEAD_DIM)

def forward(inputs, first_gain, first_shift, qkv_weight, qkv_bias, out_weight, second_gain, second_shift, gate_weight, up_weight, down_weight):
    attn_input = low(normalize_affine(inputs, first_gain, first_shift))
    projected = low_back(jnp.dot(attn_input, qkv_weight, precision=HIGHEST) + qkv_bias)
    positions = jnp.arange(LEN, dtype=jnp.int32).astype(jnp.float32)
    cosine, sine = tables(positions)
    queries = projected[:, :D].reshape(LEN, HEADS, HEAD_DIM)
    keys_all = projected[:, D:2 * D].reshape(LEN, HEADS, HEAD_DIM)
    values_all = projected[:, 2 * D:].reshape(LEN, HEADS, HEAD_DIM)
    queries = low_back(low(rotate(queries, cosine, sine)))
    keys_all = low_back(low(rotate(keys_all, cosine, sine)))
    values_all = low_back(low(values_all))
    attended = low_back(low(attention(queries, keys_all, values_all)))
    residual = inputs + low_back(jnp.dot(attended, out_weight, precision=HIGHEST))
    mlp_input = low(normalize_affine(residual, second_gain, second_shift))
    gate_value = low_back(jnp.dot(mlp_input, gate_weight, precision=HIGHEST))
    up_value = low_back(jnp.dot(mlp_input, up_weight, precision=HIGHEST))
    hidden = low(jax.nn.silu(gate_value) * up_value)
    return residual + jnp.dot(hidden, down_weight, precision=HIGHEST)

def reference(inputs, first_gain, first_shift, qkv_weight, qkv_bias, out_weight, second_gain, second_shift, gate_weight, up_weight, down_weight, out_cotangent):
    weights = tuple((item.astype(jnp.float32) for item in (first_gain, first_shift, qkv_weight, qkv_bias, out_weight, second_gain, second_shift, gate_weight, up_weight, down_weight)))

    def one_sequence(totals, pair):
        sequence, cotangent = pair
        result, pull = jax.vjp(forward, sequence.astype(jnp.float32), *weights)
        grads = pull(cotangent.astype(jnp.float32))
        totals = tuple((left + right for left, right in zip(totals, grads[1:])))
        return (totals, (result.astype(jnp.bfloat16), grads[0].astype(jnp.bfloat16)))
    zeros = tuple((jnp.zeros(item.shape, jnp.float32) for item in weights))
    totals, (results, input_grads) = lax.scan(one_sequence, zeros, (inputs, out_cotangent))
    return (results, input_grads, totals[0], totals[1], totals[2], totals[3], totals[4], totals[5], totals[6], totals[7], totals[8], totals[9])
```

```python
import jax
import jax.numpy as jnp
from jax import lax
from jax.sharding import PartitionSpec as P

HEAD_DIM = 64
ROT = 16
F32 = jnp.float32
BF16 = jnp.bfloat16


def normalize(values):
    center = values - jnp.mean(values, axis=-1, keepdims=True)
    variance = jnp.mean(center * center, axis=-1, keepdims=True)
    inverse = lax.rsqrt(variance + 1e-05)
    return (center * inverse, inverse)


def norm_back(grad_normed, normed, inverse, gain):
    scaled = grad_normed * gain
    centered = scaled - jnp.mean(scaled, axis=-1, keepdims=True)
    return inverse * (centered - normed * jnp.mean(scaled * normed, axis=-1, keepdims=True))


def dot(left, right):
    return jnp.dot(left, right, preferred_element_type=F32)


def contract_rows(left, right):
    return lax.dot_general(left, right, (((0,), (0,)), ((), ())), preferred_element_type=F32)


def contract_cols(left, right):
    return lax.dot_general(left, right, (((1,), (1,)), ((), ())), preferred_element_type=F32)


def tables(positions):
    half_rot = ROT // 2
    freqs = 10000.0 ** (-(2.0 * jnp.arange(half_rot, dtype=F32)) / ROT)
    angles = positions[:, None] * freqs[None, :]
    cosine = jnp.cos(angles)
    sine = jnp.sin(angles)
    return (jnp.concatenate([cosine, cosine], -1), jnp.concatenate([sine, sine], -1))


def rotate(heads_in, cosine, sine):
    half_rot = ROT // 2
    rotary = heads_in[..., :ROT]
    turned = jnp.concatenate([-rotary[..., half_rot:], rotary[..., :half_rot]], -1)
    moved = rotary * cosine[:, None, :] + turned * sine[:, None, :]
    return jnp.concatenate([moved, heads_in[..., ROT:]], -1)


def gather(value, axis):
    return lax.all_gather(value, axis, axis=0, tiled=True)


def scatter_sum(value, axis):
    return lax.psum_scatter(value, axis, scatter_dimension=0, tiled=True)


def swap(value, axis, split, concat):
    return lax.all_to_all(value, axis, split_axis=split, concat_axis=concat, tiled=True)


def attention_forward(queries, keys, values):
    length = queries.shape[0]
    scale = HEAD_DIM ** (-0.5)
    index = jnp.arange(length, dtype=jnp.int32)
    allowed = index[None, :] <= index[:, None]
    scores = jnp.einsum("qhd,khd->hqk", queries, keys, preferred_element_type=F32) * scale
    scores = jnp.where(allowed[None], scores, -jnp.inf)
    largest = jnp.max(scores, axis=-1, keepdims=True)
    exponent = jnp.exp(scores - largest)
    totals = jnp.sum(exponent, axis=-1, keepdims=True)
    probs = exponent / totals
    mixed = jnp.einsum("hqk,khd->qhd", probs.astype(BF16), values, preferred_element_type=F32)
    return mixed.astype(BF16), (largest + jnp.log(totals))


def attention_backward(queries, keys, values, log_total, grad):
    length = queries.shape[0]
    scale = HEAD_DIM ** (-0.5)
    index = jnp.arange(length, dtype=jnp.int32)
    allowed = index[None, :] <= index[:, None]
    scores = jnp.einsum("qhd,khd->hqk", queries, keys, preferred_element_type=F32) * scale
    scores = jnp.where(allowed[None], scores, -jnp.inf)
    probs = jnp.exp(scores - log_total)
    values_grad = jnp.einsum("hqk,qhd->khd", probs.astype(BF16), grad, preferred_element_type=F32)
    probs_grad = jnp.einsum("qhd,khd->hqk", grad, values, preferred_element_type=F32)
    scores_grad = (
        probs * (probs_grad - jnp.sum(probs * probs_grad, axis=-1, keepdims=True))
    ).astype(BF16)
    query_grad = jnp.einsum("hqk,khd->qhd", scores_grad, keys, preferred_element_type=F32) * scale
    keys_grad = jnp.einsum("hqk,qhd->khd", scores_grad, queries, preferred_element_type=F32) * scale
    return query_grad.astype(BF16), keys_grad.astype(BF16), values_grad.astype(BF16)


def shards(
    ways,
    inputs,
    first_gain,
    first_shift,
    qkv_weight,
    qkv_bias,
    out_weight,
    second_gain,
    second_shift,
    gate_weight,
    up_weight,
    down_weight,
    out_cotangent,
):
    seqs, dps = ways
    width = inputs.shape[2]
    rows = inputs.shape[1]
    length = rows * seqs
    part = width // (seqs * dps)
    units = down_weight.shape[0]
    group = width // seqs
    heads = group // HEAD_DIM
    me_seq = lax.axis_index("seq")
    grad_out = out_cotangent[0]
    hidden_in = inputs[0].astype(F32)

    small = gather(
        jnp.concatenate([first_gain, first_shift, second_gain, second_shift, qkv_bias])[None],
        ("seq", "dp"),
    ).astype(F32)
    gain_one = small[:, :part].reshape(-1)
    shift_one = small[:, part : 2 * part].reshape(-1)
    gain_two = small[:, 2 * part : 3 * part].reshape(-1)
    shift_two = small[:, 3 * part : 4 * part].reshape(-1)
    bias = small[:, 4 * part :].reshape(3, seqs, group)
    bias = lax.dynamic_index_in_dim(bias, me_seq, 1, keepdims=False).reshape(3 * group)

    qkv_cut = qkv_weight.reshape(part, 3, seqs, group).transpose(2, 0, 1, 3)
    qkv_cut = swap(qkv_cut.reshape(seqs * part, 3 * group), "seq", 0, 0)
    qkv_full = gather(qkv_cut, "dp")
    out_full = gather(out_weight, "dp")

    def cut_units(weight):
        cut = weight.reshape(part, seqs, dps, units).transpose(2, 0, 1, 3)
        return cut.reshape(dps * part, seqs * units)

    gate_cut = jnp.concatenate([cut_units(gate_weight), cut_units(up_weight)], 1)
    gate_up = gather(swap(gate_cut, "dp", 0, 0), "seq")
    down_full = gather(down_weight, "seq")
    wide = seqs * units

    def to_mixed(value):
        return value.reshape(rows, seqs, dps, part).swapaxes(1, 2).reshape(rows, width)

    def from_mixed(value):
        return value.reshape(rows, dps, seqs, part).swapaxes(1, 2).reshape(rows, width)

    normed_one, inverse_one = normalize(hidden_in)
    attn_input = (normed_one * gain_one + shift_one).astype(BF16)
    attn_all = gather(to_mixed(attn_input), "seq")
    projected = dot(attn_all, qkv_full) + bias
    cosine, sine = tables(jnp.arange(length, dtype=jnp.int32).astype(F32))

    def to_heads(flat):
        return flat.reshape(length, heads, HEAD_DIM)

    queries = rotate(to_heads(projected[:, :group]), cosine, sine).astype(BF16)
    keys = rotate(to_heads(projected[:, group : 2 * group]), cosine, sine).astype(BF16)
    values = to_heads(projected[:, 2 * group :]).astype(BF16)
    attended, log_total = attention_forward(queries, keys, values)
    attended = attended.reshape(length, group)
    branch = scatter_sum(dot(attended, out_full).astype(BF16), "seq").astype(F32)
    residual = hidden_in + branch

    normed_two, inverse_two = normalize(residual)
    mlp_input = (normed_two * gain_two + shift_two).astype(BF16)
    mlp_all = gather(mlp_input, "dp")
    grad_all = gather(grad_out, "dp")
    both = dot(mlp_all, gate_up)
    gate_value = both[:, :wide]
    up_value = both[:, wide:]
    sigmoid_gate = jax.nn.sigmoid(gate_value)
    activated = gate_value * sigmoid_gate
    hidden = (activated * up_value).astype(BF16)
    layer_out = residual + scatter_sum(dot(hidden, down_full).astype(BF16), "dp").astype(F32)

    hidden_grad = contract_cols(grad_all, down_full)
    gate_grad = (
        hidden_grad * up_value * (sigmoid_gate * (1.0 + gate_value * (1.0 - sigmoid_gate)))
    ).astype(BF16)
    up_grad = (hidden_grad * activated).astype(BF16)
    both_grad = jnp.concatenate([gate_grad, up_grad], 1)
    mlp_grad = scatter_sum(contract_cols(both_grad, gate_up).astype(BF16), "dp").astype(F32)
    gain_two_grad = jnp.sum(mlp_grad * normed_two, axis=0)
    shift_two_grad = jnp.sum(mlp_grad, axis=0)
    residual_grad = grad_out.astype(F32) + norm_back(mlp_grad, normed_two, inverse_two, gain_two)
    branch_grad = residual_grad.astype(BF16)

    branch_all = gather(branch_grad, "seq")
    attended_grad = contract_cols(branch_all, out_full).astype(BF16)
    query_grad, keys_grad, values_grad = attention_backward(
        queries, keys, values, log_total, to_heads(attended_grad)
    )
    query_plain = rotate(query_grad.astype(F32), cosine, -sine).astype(BF16)
    keys_plain = rotate(keys_grad.astype(F32), cosine, -sine).astype(BF16)
    projected_grad = jnp.concatenate(
        [item.reshape(length, group) for item in (query_plain, keys_plain, values_grad)], 1
    )
    attn_grad = scatter_sum(contract_cols(projected_grad, qkv_full).astype(BF16), "seq")
    attn_grad = from_mixed(attn_grad).astype(F32)
    gain_one_grad = jnp.sum(attn_grad * normed_one, axis=0)
    shift_one_grad = jnp.sum(attn_grad, axis=0)
    input_grad = residual_grad + norm_back(attn_grad, normed_one, inverse_one, gain_one)

    down_shard = scatter_sum(contract_rows(hidden, grad_all).astype(BF16), "seq").astype(F32)
    both_rows = scatter_sum(contract_rows(mlp_all, both_grad).astype(BF16), "seq")
    both_rows = swap(both_rows, "dp", 0, 0).reshape(dps, part, 2, seqs, units)
    both_rows = both_rows.transpose(2, 1, 3, 0, 4).reshape(2, part, seqs * dps * units).astype(F32)
    out_shard = scatter_sum(contract_rows(attended, branch_all).astype(BF16), "dp").astype(F32)
    qkv_rows = scatter_sum(contract_rows(attn_all, projected_grad).astype(BF16), "dp")
    qkv_rows = swap(qkv_rows, "seq", 0, 0).reshape(seqs, part, 3, group)
    qkv_shard = qkv_rows.transpose(1, 2, 0, 3).reshape(part, 3 * width).astype(F32)

    bias_term = jnp.sum(projected_grad.astype(F32), axis=0).reshape(3, 1, group)
    here = (jnp.arange(seqs, dtype=jnp.int32) == me_seq).astype(F32)[None, :, None]
    bias_term = (bias_term * here).reshape(seqs * dps, 3 * part)
    terms = [gain_one_grad, shift_one_grad, gain_two_grad, shift_two_grad]
    terms = [item.reshape(seqs * dps, part) for item in terms] + [bias_term]
    tiny = scatter_sum(jnp.concatenate(terms, 1), ("seq", "dp"))[0]
    return (
        layer_out.astype(BF16)[None],
        input_grad.astype(BF16)[None],
        tiny[:part],
        tiny[part : 2 * part],
        qkv_shard,
        tiny[4 * part :],
        out_shard,
        tiny[2 * part : 3 * part],
        tiny[3 * part : 4 * part],
        both_rows[0],
        both_rows[1],
        down_shard,
    )


def solution(mesh):
    split = ("seq", "dp")
    tokens = P("dp", "seq", None)
    in_specs = (
        tokens,
        P(split),
        P(split),
        P(split, None),
        P(split),
        P(split, None),
        P(split),
        P(split),
        P(split, None),
        P(split, None),
        P(split, None),
        tokens,
    )
    out_specs = (
        tokens,
        tokens,
        P(split),
        P(split),
        P(split, None),
        P(split),
        P(split, None),
        P(split),
        P(split),
        P(split, None),
        P(split, None),
        P(split, None),
    )
    ways = (mesh.shape["seq"], mesh.shape["dp"])

    def local(*args):
        return shards(ways, *args)

    return jax.shard_map(local, mesh=mesh, in_specs=in_specs, out_specs=out_specs, check_vma=False)
```

```python
import functools

import jax
import jax.numpy as jnp
from jax import lax
from jax.experimental import pallas as pl
from jax.experimental.pallas import tpu as pltpu
from jax.sharding import PartitionSpec as P

HEAD_DIM = 64
ROT = 16
F32 = jnp.float32
BF16 = jnp.bfloat16


def normalize(values):
    center = values - jnp.mean(values, axis=-1, keepdims=True)
    variance = jnp.mean(center * center, axis=-1, keepdims=True)
    inverse = lax.rsqrt(variance + 1e-05)
    return (center * inverse, inverse)


def norm_back(grad_normed, normed, inverse, gain):
    scaled = grad_normed * gain
    centered = scaled - jnp.mean(scaled, axis=-1, keepdims=True)
    return inverse * (centered - normed * jnp.mean(scaled * normed, axis=-1, keepdims=True))


def dot(left, right):
    return jnp.dot(left, right, preferred_element_type=F32)


def contract_rows(left, right):
    return lax.dot_general(left, right, (((0,), (0,)), ((), ())), preferred_element_type=F32)


def contract_cols(left, right):
    return lax.dot_general(left, right, (((1,), (1,)), ((), ())), preferred_element_type=F32)


def tables(positions):
    half_rot = ROT // 2
    freqs = 10000.0 ** (-(2.0 * jnp.arange(half_rot, dtype=F32)) / ROT)
    angles = positions[:, None] * freqs[None, :]
    cosine = jnp.cos(angles)
    sine = jnp.sin(angles)
    return (jnp.concatenate([cosine, cosine], -1), jnp.concatenate([sine, sine], -1))


def rotate(heads_in, cosine, sine):
    half_rot = ROT // 2
    rotary = heads_in[..., :ROT]
    turned = jnp.concatenate([-rotary[..., half_rot:], rotary[..., :half_rot]], -1)
    moved = rotary * cosine[:, None, :] + turned * sine[:, None, :]
    return jnp.concatenate([moved, heads_in[..., ROT:]], -1)


def gather(value, axis):
    return lax.all_gather(value, axis, axis=0, tiled=True)


def scatter_sum(value, axis):
    return lax.psum_scatter(value, axis, scatter_dimension=0, tiled=True)


def swap(value, axis, split, concat):
    return lax.all_to_all(value, axis, split_axis=split, concat_axis=concat, tiled=True)


MESH = pl.DeviceIdType.MESH


def meet(peers):
    barrier = pltpu.get_barrier_semaphore()
    for peer in peers:
        pl.semaphore_signal(barrier, inc=1, device_id=peer, device_id_type=MESH)
    pl.semaphore_wait(barrier, len(peers))


def push(source, target, send, recv, at, peer):
    copy = pltpu.make_async_remote_copy(
        src_ref=source,
        dst_ref=target,
        send_sem=send.at[at],
        recv_sem=recv.at[at],
        device_id=peer,
        device_id_type=MESH,
    )
    copy.start()
    return copy


def corners():
    me = lax.axis_index("seq")
    high, low = me // 2, lax.rem(me, 2)
    across = high * 2 + (1 - low)
    along = (1 - high) * 2 + low
    return me, across, along, 3 - me


def gather_square(x_ref, o_ref, send, recv, local):
    me, across, along, far = corners()
    to_across, to_along = {"seq": across}, {"seq": along}
    half = x_ref.shape[0] // 2
    top, low = pl.ds(0, half), pl.ds(half, half)
    meet([to_across, to_along])
    copies = [
        push(x_ref.at[top], o_ref.at[me, top], send, recv, 0, to_across),
        push(x_ref.at[low], o_ref.at[me, low], send, recv, 1, to_along),
        push(x_ref.at[low], o_ref.at[me, low], send, recv, 2, to_across),
        push(x_ref.at[top], o_ref.at[me, top], send, recv, 3, to_along),
    ]
    own = pltpu.make_async_copy(x_ref, o_ref.at[me], local)
    own.start()
    copies[0].wait_recv()
    copies.append(push(o_ref.at[across, top], o_ref.at[across, top], send, recv, 4, to_along))
    copies[1].wait_recv()
    copies.append(push(o_ref.at[along, low], o_ref.at[along, low], send, recv, 5, to_across))
    for at, copy in enumerate(copies):
        copy.wait_send()
        if at > 1:
            copy.wait_recv()
    own.wait()


def gather_direct(count, x_ref, o_ref, send, recv, local):
    me = lax.axis_index("seq")
    peers = [{"seq": lax.rem(me + step, count)} for step in range(1, count)]
    meet(peers)
    copies = [push(x_ref, o_ref.at[me], send, recv, at, peer) for at, peer in enumerate(peers)]
    own = pltpu.make_async_copy(x_ref, o_ref.at[me], local)
    own.start()
    for copy in copies:
        copy.wait()
    own.wait()


def gather_seq(value, count, tag):
    square = count == 4
    body = gather_square if square else functools.partial(gather_direct, count)
    slots = 6 if square else count - 1
    out = pl.pallas_call(
        body,
        out_shape=jax.ShapeDtypeStruct((count,) + value.shape, value.dtype),
        in_specs=[pl.BlockSpec(memory_space=pltpu.VMEM)],
        out_specs=pl.BlockSpec(memory_space=pl.ANY),
        scratch_shapes=[
            pltpu.SemaphoreType.DMA((slots,)),
            pltpu.SemaphoreType.DMA((slots,)),
            pltpu.SemaphoreType.DMA,
        ],
        compiler_params=pltpu.CompilerParams(collective_id=tag, has_side_effects=True),
    )(value)
    return out.reshape(count * value.shape[0], value.shape[1])


def reduce_square(x_ref, o_ref, pair, got, send, recv):
    me, across, along, far = corners()
    to_across, to_along = {"seq": across}, {"seq": along}
    half = x_ref.shape[1] // 2
    top, low = pl.ds(0, half), pl.ds(half, half)
    meet([to_across, to_along])
    copies = [
        push(x_ref.at[far, top], pair.at[0], send, recv, 0, to_across),
        push(x_ref.at[far, low], pair.at[1], send, recv, 1, to_along),
        push(x_ref.at[across, top], got.at[0, top], send, recv, 2, to_across),
        push(x_ref.at[along, low], got.at[1, low], send, recv, 3, to_along),
    ]
    copies[0].wait_recv()
    pair[2] = (pair[0].astype(F32) + x_ref[along, top].astype(F32)).astype(pair.dtype)
    copies.append(push(pair.at[2], got.at[1, top], send, recv, 4, to_along))
    copies[1].wait_recv()
    pair[3] = (pair[1].astype(F32) + x_ref[across, low].astype(F32)).astype(pair.dtype)
    copies.append(push(pair.at[3], got.at[0, low], send, recv, 5, to_across))
    for at, copy in enumerate(copies):
        copy.wait_send()
        if at > 1:
            copy.wait_recv()
    o_ref[...] = x_ref[me].astype(F32) + (got[0].astype(F32) + got[1].astype(F32))


def reduce_direct(count, x_ref, o_ref, got, send, recv):
    me = lax.axis_index("seq")
    targets = [lax.rem(me + step, count) for step in range(1, count)]
    peers = [{"seq": target} for target in targets]
    meet(peers)
    copies = [
        push(x_ref.at[target], got.at[at], send, recv, at, peer)
        for at, (target, peer) in enumerate(zip(targets, peers))
    ]
    for copy in copies:
        copy.wait()
    total = x_ref[me].astype(F32)
    for at in range(count - 1):
        total = total + got[at].astype(F32)
    o_ref[...] = total


def reduce_seq(value, count, tag):
    rows, wide = value.shape[0] // count, value.shape[1]
    square = count == 4
    if square:
        body, slots = reduce_square, 6
        held = [
            pltpu.VMEM((4, rows // 2, wide), value.dtype),
            pltpu.VMEM((2, rows, wide), value.dtype),
        ]
    else:
        body, slots = functools.partial(reduce_direct, count), count - 1
        held = [pltpu.VMEM((count - 1, rows, wide), value.dtype)]
    return pl.pallas_call(
        body,
        out_shape=jax.ShapeDtypeStruct((rows, wide), F32),
        in_specs=[pl.BlockSpec(memory_space=pltpu.VMEM)],
        out_specs=pl.BlockSpec(memory_space=pltpu.VMEM),
        scratch_shapes=held
        + [pltpu.SemaphoreType.DMA((slots,)), pltpu.SemaphoreType.DMA((slots,))],
        compiler_params=pltpu.CompilerParams(collective_id=tag, has_side_effects=True),
    )(value.reshape(count, rows, wide))


def exchange(ways, shared, x_ref, o_ref, got, send, recv):
    seqs, dps = ways
    count = seqs * dps
    me = lax.axis_index("seq") * dps + lax.axis_index("dp")
    barrier = pltpu.get_barrier_semaphore()

    def peer_of(step):
        other = lax.rem(me + step, count)
        return other, {"seq": other // dps, "dp": lax.rem(other, dps)}

    def copy_of(step):
        other, peer = peer_of(step)
        return pltpu.make_async_remote_copy(
            src_ref=x_ref if shared else x_ref.at[other],
            dst_ref=got.at[me],
            send_sem=send.at[step - 1],
            recv_sem=recv.at[step - 1],
            device_id=peer,
            device_id_type=MESH,
        )

    @pl.loop(1, count)
    def _(step):
        pl.semaphore_signal(barrier, inc=1, device_id=peer_of(step)[1], device_id_type=MESH)

    pl.semaphore_wait(barrier, count - 1)

    @pl.loop(1, count)
    def _(step):
        copy_of(step).start()

    got[me] = x_ref[...] if shared else x_ref[me]

    @pl.loop(1, count)
    def _(step):
        copy_of(step).wait()

    o_ref[...] = got[...] if shared else jnp.sum(got[...], axis=0)


def exchange_all(value, ways, shared, tag):
    count = ways[0] * ways[1]
    block = value.shape if shared else value.shape[1:]
    return pl.pallas_call(
        functools.partial(exchange, ways, shared),
        out_shape=jax.ShapeDtypeStruct(((count,) if shared else ()) + block, value.dtype),
        in_specs=[pl.BlockSpec(memory_space=pltpu.VMEM)],
        out_specs=pl.BlockSpec(memory_space=pltpu.VMEM),
        scratch_shapes=[
            pltpu.VMEM((count,) + block, value.dtype),
            pltpu.SemaphoreType.DMA((count - 1,)),
            pltpu.SemaphoreType.DMA((count - 1,)),
        ],
        compiler_params=pltpu.CompilerParams(collective_id=tag, has_side_effects=True),
    )(value)


def attention_forward(queries, keys, values):
    length = queries.shape[0]
    scale = HEAD_DIM ** (-0.5)
    index = jnp.arange(length, dtype=jnp.int32)
    allowed = index[None, :] <= index[:, None]
    scores = jnp.einsum("qhd,khd->hqk", queries, keys, preferred_element_type=F32) * scale
    scores = jnp.where(allowed[None], scores, -jnp.inf)
    largest = jnp.max(scores, axis=-1, keepdims=True)
    exponent = jnp.exp(scores - largest)
    totals = jnp.sum(exponent, axis=-1, keepdims=True)
    probs = exponent / totals
    mixed = jnp.einsum("hqk,khd->qhd", probs.astype(BF16), values, preferred_element_type=F32)
    return mixed.astype(BF16), (largest + jnp.log(totals))


def attention_backward(queries, keys, values, log_total, grad):
    length = queries.shape[0]
    scale = HEAD_DIM ** (-0.5)
    index = jnp.arange(length, dtype=jnp.int32)
    allowed = index[None, :] <= index[:, None]
    scores = jnp.einsum("qhd,khd->hqk", queries, keys, preferred_element_type=F32) * scale
    scores = jnp.where(allowed[None], scores, -jnp.inf)
    probs = jnp.exp(scores - log_total)
    values_grad = jnp.einsum("hqk,qhd->khd", probs.astype(BF16), grad, preferred_element_type=F32)
    probs_grad = jnp.einsum("qhd,khd->hqk", grad, values, preferred_element_type=F32)
    scores_grad = (
        probs * (probs_grad - jnp.sum(probs * probs_grad, axis=-1, keepdims=True))
    ).astype(BF16)
    query_grad = jnp.einsum("hqk,khd->qhd", scores_grad, keys, preferred_element_type=F32) * scale
    keys_grad = jnp.einsum("hqk,qhd->khd", scores_grad, queries, preferred_element_type=F32) * scale
    return query_grad.astype(BF16), keys_grad.astype(BF16), values_grad.astype(BF16)


def shards(
    ways,
    inputs,
    first_gain,
    first_shift,
    qkv_weight,
    qkv_bias,
    out_weight,
    second_gain,
    second_shift,
    gate_weight,
    up_weight,
    down_weight,
    out_cotangent,
):
    seqs, dps = ways
    width = inputs.shape[2]
    rows = inputs.shape[1]
    length = rows * seqs
    part = width // (seqs * dps)
    units = down_weight.shape[0]
    group = width // seqs
    heads = group // HEAD_DIM
    me_seq = lax.axis_index("seq")
    grad_out = out_cotangent[0]
    hidden_in = inputs[0].astype(F32)

    small = jnp.concatenate([first_gain, first_shift, second_gain, second_shift, qkv_bias])
    total = small.shape[0]
    padded = -(-total // 2048) * 2048
    small = jnp.pad(small, (0, padded - total)).reshape(padded // 128, 128)
    small = exchange_all(small, ways, True, 4).reshape(seqs * dps, padded)[:, :total].astype(F32)
    gain_one = small[:, :part].reshape(-1)
    shift_one = small[:, part : 2 * part].reshape(-1)
    gain_two = small[:, 2 * part : 3 * part].reshape(-1)
    shift_two = small[:, 3 * part : 4 * part].reshape(-1)
    bias = small[:, 4 * part :].reshape(3, seqs, group)
    bias = lax.dynamic_index_in_dim(bias, me_seq, 1, keepdims=False).reshape(3 * group)

    qkv_cut = qkv_weight.reshape(part, 3, seqs, group).transpose(2, 0, 1, 3)
    qkv_cut = swap(qkv_cut.reshape(seqs * part, 3 * group), "seq", 0, 0)
    qkv_full = gather(qkv_cut, "dp")
    out_full = gather(out_weight, "dp")

    def cut_units(weight):
        cut = weight.reshape(part, seqs, dps, units).transpose(2, 0, 1, 3)
        return cut.reshape(dps * part, seqs * units)

    gate_cut = jnp.concatenate([cut_units(gate_weight), cut_units(up_weight)], 1)
    gate_up = gather(swap(gate_cut, "dp", 0, 0), "seq")
    down_full = gather(down_weight, "seq")
    wide = seqs * units

    def to_mixed(value):
        return value.reshape(rows, seqs, dps, part).swapaxes(1, 2).reshape(rows, width)

    def from_mixed(value):
        return value.reshape(rows, dps, seqs, part).swapaxes(1, 2).reshape(rows, width)

    normed_one, inverse_one = normalize(hidden_in)
    attn_input = (normed_one * gain_one + shift_one).astype(BF16)
    attn_all = gather_seq(to_mixed(attn_input), seqs, 0)
    projected = dot(attn_all, qkv_full) + bias
    cosine, sine = tables(jnp.arange(length, dtype=jnp.int32).astype(F32))

    def to_heads(flat):
        return flat.reshape(length, heads, HEAD_DIM)

    queries = rotate(to_heads(projected[:, :group]), cosine, sine).astype(BF16)
    keys = rotate(to_heads(projected[:, group : 2 * group]), cosine, sine).astype(BF16)
    values = to_heads(projected[:, 2 * group :]).astype(BF16)
    attended, log_total = attention_forward(queries, keys, values)
    attended = attended.reshape(length, group)
    branch = reduce_seq(dot(attended, out_full).astype(BF16), seqs, 1)
    residual = hidden_in + branch

    normed_two, inverse_two = normalize(residual)
    mlp_input = (normed_two * gain_two + shift_two).astype(BF16)
    mlp_all = gather(mlp_input, "dp")
    grad_all = gather(grad_out, "dp")
    both = dot(mlp_all, gate_up)
    gate_value = both[:, :wide]
    up_value = both[:, wide:]
    sigmoid_gate = jax.nn.sigmoid(gate_value)
    activated = gate_value * sigmoid_gate
    hidden = (activated * up_value).astype(BF16)
    layer_out = residual + scatter_sum(dot(hidden, down_full).astype(BF16), "dp").astype(F32)

    hidden_grad = contract_cols(grad_all, down_full)
    gate_grad = (
        hidden_grad * up_value * (sigmoid_gate * (1.0 + gate_value * (1.0 - sigmoid_gate)))
    ).astype(BF16)
    up_grad = (hidden_grad * activated).astype(BF16)
    both_grad = jnp.concatenate([gate_grad, up_grad], 1)
    mlp_grad = scatter_sum(contract_cols(both_grad, gate_up).astype(BF16), "dp").astype(F32)
    gain_two_grad = jnp.sum(mlp_grad * normed_two, axis=0)
    shift_two_grad = jnp.sum(mlp_grad, axis=0)
    residual_grad = grad_out.astype(F32) + norm_back(mlp_grad, normed_two, inverse_two, gain_two)
    branch_grad = residual_grad.astype(BF16)

    branch_all = gather_seq(branch_grad, seqs, 2)
    attended_grad = contract_cols(branch_all, out_full).astype(BF16)
    query_grad, keys_grad, values_grad = attention_backward(
        queries, keys, values, log_total, to_heads(attended_grad)
    )
    query_plain = rotate(query_grad.astype(F32), cosine, -sine).astype(BF16)
    keys_plain = rotate(keys_grad.astype(F32), cosine, -sine).astype(BF16)
    projected_grad = jnp.concatenate(
        [item.reshape(length, group) for item in (query_plain, keys_plain, values_grad)], 1
    )
    attn_grad = reduce_seq(contract_cols(projected_grad, qkv_full).astype(BF16), seqs, 3)
    attn_grad = from_mixed(attn_grad)
    gain_one_grad = jnp.sum(attn_grad * normed_one, axis=0)
    shift_one_grad = jnp.sum(attn_grad, axis=0)
    input_grad = residual_grad + norm_back(attn_grad, normed_one, inverse_one, gain_one)

    down_shard = scatter_sum(contract_rows(hidden, grad_all).astype(BF16), "seq").astype(F32)
    both_rows = scatter_sum(contract_rows(mlp_all, both_grad).astype(BF16), "seq")
    both_rows = swap(both_rows, "dp", 0, 0).reshape(dps, part, 2, seqs, units)
    both_rows = both_rows.transpose(2, 1, 3, 0, 4).reshape(2, part, seqs * dps * units).astype(F32)
    out_shard = scatter_sum(contract_rows(attended, branch_all).astype(BF16), "dp").astype(F32)
    qkv_rows = scatter_sum(contract_rows(attn_all, projected_grad).astype(BF16), "dp")
    qkv_rows = swap(qkv_rows, "seq", 0, 0).reshape(seqs, part, 3, group)
    qkv_shard = qkv_rows.transpose(1, 2, 0, 3).reshape(part, 3 * width).astype(F32)

    bias_term = jnp.sum(projected_grad.astype(F32), axis=0).reshape(3, 1, group)
    here = (jnp.arange(seqs, dtype=jnp.int32) == me_seq).astype(F32)[None, :, None]
    bias_term = (bias_term * here).reshape(seqs * dps, 3 * part)
    terms = [gain_one_grad, shift_one_grad, gain_two_grad, shift_two_grad]
    terms = [item.reshape(seqs * dps, part) for item in terms] + [bias_term]
    terms = jnp.concatenate(terms, 1)
    padded = -(-total // 1024) * 1024
    terms = jnp.pad(terms, ((0, 0), (0, padded - total))).reshape(seqs * dps, padded // 128, 128)
    tiny = exchange_all(terms, ways, False, 5).reshape(padded)
    return (
        layer_out.astype(BF16)[None],
        input_grad.astype(BF16)[None],
        tiny[:part],
        tiny[part : 2 * part],
        qkv_shard,
        tiny[4 * part : total],
        out_shard,
        tiny[2 * part : 3 * part],
        tiny[3 * part : 4 * part],
        both_rows[0],
        both_rows[1],
        down_shard,
    )


def solution(mesh):
    split = ("seq", "dp")
    tokens = P("dp", "seq", None)
    in_specs = (
        tokens,
        P(split),
        P(split),
        P(split, None),
        P(split),
        P(split, None),
        P(split),
        P(split),
        P(split, None),
        P(split, None),
        P(split, None),
        tokens,
    )
    out_specs = (
        tokens,
        tokens,
        P(split),
        P(split),
        P(split, None),
        P(split),
        P(split, None),
        P(split),
        P(split),
        P(split, None),
        P(split, None),
        P(split, None),
    )
    ways = (mesh.shape["seq"], mesh.shape["dp"])

    def local(*args):
        return shards(ways, *args)

    return jax.shard_map(local, mesh=mesh, in_specs=in_specs, out_specs=out_specs, check_vma=False)
```

```python
import functools

import jax
import jax.numpy as jnp
from jax import lax
from jax.experimental import pallas as pl
from jax.experimental.pallas import tpu as pltpu
from jax.sharding import PartitionSpec as P


HEAD_DIM = 64
ROT = 16
F32 = jnp.float32
BF16 = jnp.bfloat16


def normalize(values):
    center = values - jnp.mean(values, axis=-1, keepdims=True)
    variance = jnp.mean(center * center, axis=-1, keepdims=True)
    inverse = lax.rsqrt(variance + 1e-05)
    return (center * inverse, inverse)


def norm_back(grad_normed, normed, inverse, gain):
    scaled = grad_normed * gain
    centered = scaled - jnp.mean(scaled, axis=-1, keepdims=True)
    return inverse * (centered - normed * jnp.mean(scaled * normed, axis=-1, keepdims=True))


def dot(left, right):
    return jnp.dot(left, right, preferred_element_type=F32)


def contract_rows(left, right):
    return lax.dot_general(left, right, (((0,), (0,)), ((), ())), preferred_element_type=F32)


def contract_cols(left, right):
    return lax.dot_general(left, right, (((1,), (1,)), ((), ())), preferred_element_type=F32)


def tables(positions):
    half_rot = ROT // 2
    freqs = 10000.0 ** (-(2.0 * jnp.arange(half_rot, dtype=F32)) / ROT)
    angles = positions[:, None] * freqs[None, :]
    cosine = jnp.cos(angles)
    sine = jnp.sin(angles)
    return (jnp.concatenate([cosine, cosine], -1), jnp.concatenate([sine, sine], -1))


def rotate(heads_in, cosine, sine):
    half_rot = ROT // 2
    rotary = heads_in[..., :ROT]
    turned = jnp.concatenate([-rotary[..., half_rot:], rotary[..., :half_rot]], -1)
    moved = rotary * cosine[:, None, :] + turned * sine[:, None, :]
    return jnp.concatenate([moved, heads_in[..., ROT:]], -1)


def gather(value, axis):
    return lax.all_gather(value, axis, axis=0, tiled=True)


def scatter_sum(value, axis):
    return lax.psum_scatter(value, axis, scatter_dimension=0, tiled=True)


def swap(value, axis, split, concat):
    return lax.all_to_all(value, axis, split_axis=split, concat_axis=concat, tiled=True)


MESH = pl.DeviceIdType.MESH


def lasting(micros):
    return pl.CostEstimate(flops=0, transcendentals=0, bytes_accessed=int(micros * 3.0e6))


def meet(peers):
    barrier = pltpu.get_barrier_semaphore()
    for peer in peers:
        pl.semaphore_signal(barrier, inc=1, device_id=peer, device_id_type=MESH)
    pl.semaphore_wait(barrier, len(peers))


def push(source, target, send, recv, at, peer):
    copy = pltpu.make_async_remote_copy(
        src_ref=source,
        dst_ref=target,
        send_sem=send.at[at],
        recv_sem=recv.at[at],
        device_id=peer,
        device_id_type=MESH,
    )
    copy.start()
    return copy


def corners():
    me = lax.axis_index("seq")
    high, low = me // 2, lax.rem(me, 2)
    across = high * 2 + (1 - low)
    along = (1 - high) * 2 + low
    return me, across, along, 3 - me


def gather_square(x_ref, o_ref, send, recv, local):
    me, across, along, _ = corners()
    to_across, to_along = {"seq": across}, {"seq": along}
    half = x_ref.shape[0] // 2
    top, low = pl.ds(0, half), pl.ds(half, half)
    meet([to_across, to_along])
    copies = [
        push(x_ref.at[top], o_ref.at[me, top], send, recv, 0, to_across),
        push(x_ref.at[low], o_ref.at[me, low], send, recv, 1, to_along),
        push(x_ref.at[low], o_ref.at[me, low], send, recv, 2, to_across),
        push(x_ref.at[top], o_ref.at[me, top], send, recv, 3, to_along),
    ]
    own = pltpu.make_async_copy(x_ref, o_ref.at[me], local)
    own.start()
    copies[0].wait_recv()
    copies.append(push(o_ref.at[across, top], o_ref.at[across, top], send, recv, 4, to_along))
    copies[1].wait_recv()
    copies.append(push(o_ref.at[along, low], o_ref.at[along, low], send, recv, 5, to_across))
    for at, copy in enumerate(copies):
        copy.wait_send()
        if at > 1:
            copy.wait_recv()
    own.wait()


def gather_direct(count, x_ref, o_ref, send, recv, local):
    me = lax.axis_index("seq")
    peers = [{"seq": lax.rem(me + step, count)} for step in range(1, count)]
    meet(peers)
    copies = [push(x_ref, o_ref.at[me], send, recv, at, peer) for at, peer in enumerate(peers)]
    own = pltpu.make_async_copy(x_ref, o_ref.at[me], local)
    own.start()
    for copy in copies:
        copy.wait()
    own.wait()


def gather_seq(value, count, tag):
    square = count == 4
    body = gather_square if square else functools.partial(gather_direct, count)
    slots = 6 if square else count - 1
    out = pl.pallas_call(
        body,
        out_shape=jax.ShapeDtypeStruct((count,) + value.shape, value.dtype),
        in_specs=[pl.BlockSpec(memory_space=pltpu.VMEM)],
        out_specs=pl.BlockSpec(memory_space=pl.ANY),
        scratch_shapes=[
            pltpu.SemaphoreType.DMA((slots,)),
            pltpu.SemaphoreType.DMA((slots,)),
            pltpu.SemaphoreType.DMA,
        ],
        cost_estimate=lasting(22),
        compiler_params=pltpu.CompilerParams(collective_id=tag, has_side_effects=True),
    )(value)
    return out.reshape(count * value.shape[0], value.shape[1])


def reduce_square(x_ref, o_ref, pair, got, send, recv):
    me, across, along, far = corners()
    to_across, to_along = {"seq": across}, {"seq": along}
    half = x_ref.shape[1] // 2
    top, low = pl.ds(0, half), pl.ds(half, half)
    meet([to_across, to_along])
    copies = [
        push(x_ref.at[far, top], pair.at[0], send, recv, 0, to_across),
        push(x_ref.at[far, low], pair.at[1], send, recv, 1, to_along),
        push(x_ref.at[across, top], got.at[0, top], send, recv, 2, to_across),
        push(x_ref.at[along, low], got.at[1, low], send, recv, 3, to_along),
    ]
    copies[0].wait_recv()
    pair[2] = (pair[0].astype(F32) + x_ref[along, top].astype(F32)).astype(pair.dtype)
    copies.append(push(pair.at[2], got.at[1, top], send, recv, 4, to_along))
    copies[1].wait_recv()
    pair[3] = (pair[1].astype(F32) + x_ref[across, low].astype(F32)).astype(pair.dtype)
    copies.append(push(pair.at[3], got.at[0, low], send, recv, 5, to_across))
    for at, copy in enumerate(copies):
        copy.wait_send()
        if at > 1:
            copy.wait_recv()
    o_ref[...] = x_ref[me].astype(F32) + (got[0].astype(F32) + got[1].astype(F32))


def reduce_direct(count, x_ref, o_ref, got, send, recv):
    me = lax.axis_index("seq")
    targets = [lax.rem(me + step, count) for step in range(1, count)]
    peers = [{"seq": target} for target in targets]
    meet(peers)
    copies = [
        push(x_ref.at[target], got.at[at], send, recv, at, peer)
        for at, (target, peer) in enumerate(zip(targets, peers))
    ]
    for copy in copies:
        copy.wait()
    total = x_ref[me].astype(F32)
    for at in range(count - 1):
        total = total + got[at].astype(F32)
    o_ref[...] = total


def reduce_seq(value, count, tag):
    rows, wide = value.shape[0] // count, value.shape[1]
    square = count == 4
    if square:
        body, slots = reduce_square, 6
        held = [
            pltpu.VMEM((4, rows // 2, wide), value.dtype),
            pltpu.VMEM((2, rows, wide), value.dtype),
        ]
    else:
        body, slots = functools.partial(reduce_direct, count), count - 1
        held = [pltpu.VMEM((count - 1, rows, wide), value.dtype)]
    return pl.pallas_call(
        body,
        out_shape=jax.ShapeDtypeStruct((rows, wide), F32),
        in_specs=[pl.BlockSpec(memory_space=pltpu.VMEM)],
        out_specs=pl.BlockSpec(memory_space=pltpu.VMEM),
        scratch_shapes=held
        + [pltpu.SemaphoreType.DMA((slots,)), pltpu.SemaphoreType.DMA((slots,))],
        cost_estimate=lasting(22),
        compiler_params=pltpu.CompilerParams(collective_id=tag, has_side_effects=True),
    )(value.reshape(count, rows, wide))


def move_blocks(value, axis, count):
    rows = value.shape[0] // count
    me = lax.axis_index(axis)
    blocks = []
    for step in range(count):
        at = lax.rem(me + step, count) * rows
        block = lax.dynamic_slice_in_dim(value, at, rows, 0)
        if step:
            block = lax.ppermute(block, axis, [(i, (i + step) % count) for i in range(count)])
        blocks.append(block)
    return blocks


def place_blocks(blocks, axis):
    count, rows = len(blocks), blocks[0].shape[0]
    me = lax.axis_index(axis)
    out = jnp.zeros((count * rows,) + blocks[0].shape[1:], blocks[0].dtype)
    for step, block in enumerate(blocks):
        at = lax.rem(me - step + count, count) * rows
        out = lax.dynamic_update_slice_in_dim(out, block, at, 0)
    return out


def exchange(ways, shared, x_ref, o_ref, got, send, recv):
    seqs, dps = ways
    count = seqs * dps
    me = lax.axis_index("seq") * dps + lax.axis_index("dp")
    barrier = pltpu.get_barrier_semaphore()

    def peer_of(step):
        other = lax.rem(me + step, count)
        return other, {"seq": other // dps, "dp": lax.rem(other, dps)}

    def copy_of(step):
        other, peer = peer_of(step)
        return pltpu.make_async_remote_copy(
            src_ref=x_ref if shared else x_ref.at[other],
            dst_ref=got.at[me],
            send_sem=send.at[step - 1],
            recv_sem=recv.at[step - 1],
            device_id=peer,
            device_id_type=MESH,
        )

    @pl.loop(1, count)
    def _(step):
        pl.semaphore_signal(barrier, inc=1, device_id=peer_of(step)[1], device_id_type=MESH)

    pl.semaphore_wait(barrier, count - 1)

    @pl.loop(1, count)
    def _(step):
        copy_of(step).start()

    got[me] = x_ref[...] if shared else x_ref[me]

    @pl.loop(1, count)
    def _(step):
        copy_of(step).wait()

    o_ref[...] = got[...] if shared else jnp.sum(got[...], axis=0)


def exchange_all(value, ways, shared, tag):
    count = ways[0] * ways[1]
    block = value.shape if shared else value.shape[1:]
    return pl.pallas_call(
        functools.partial(exchange, ways, shared),
        out_shape=jax.ShapeDtypeStruct(((count,) if shared else ()) + block, value.dtype),
        in_specs=[pl.BlockSpec(memory_space=pltpu.VMEM)],
        out_specs=pl.BlockSpec(memory_space=pltpu.VMEM),
        scratch_shapes=[
            pltpu.VMEM((count,) + block, value.dtype),
            pltpu.SemaphoreType.DMA((count - 1,)),
            pltpu.SemaphoreType.DMA((count - 1,)),
        ],
        cost_estimate=lasting(10),
        compiler_params=pltpu.CompilerParams(collective_id=tag, has_side_effects=True),
    )(value)


def remote(source, target, send, recv, peer):
    return pltpu.make_async_remote_copy(
        src_ref=source,
        dst_ref=target,
        send_sem=send,
        recv_sem=recv,
        device_id=peer,
        device_id_type=MESH,
    )


def line_place(dps):
    dp = lax.axis_index("dp")
    chip, core = dp // 2, lax.rem(dp, 2)
    chips = dps // 2
    ends = (chip + 1 < chips, chip >= 1)
    sides = ({"dp": lax.rem(dp + 2, dps)}, {"dp": lax.rem(dp - 2 + dps, dps)})
    return chips, chip, core, ends, sides, {"dp": 2 * chip + (1 - core)}


def gather_line_body(dps, x_ref, o_ref, line_s, line_r, pair_s, pair_r, local):
    chips, chip, core, ends, sides, sibling = line_place(dps)
    meet([sides[0], sides[1], sibling])

    def onward(side, hop, owner, source=None):
        block = o_ref.at[2 * owner + core]
        at = (side, hop)
        return remote(
            block if source is None else source, block, line_s.at[at], line_r.at[at], sides[side]
        )

    def share(owner, owner_core, source=None):
        block = o_ref.at[2 * owner + owner_core]
        return remote(
            block if source is None else source, block, pair_s.at[owner], pair_r.at[owner], sibling
        )

    for side in range(2):

        @pl.when(ends[side])
        def _(side=side):
            onward(side, 0, chip, x_ref).start()

    share(chip, core, x_ref).start()
    own = pltpu.make_async_copy(x_ref, o_ref.at[2 * chip + core], local)
    own.start()
    for hop in range(chips - 1):
        for side in range(2):
            origin = chip - 1 - hop if side == 0 else chip + 1 + hop
            there = origin >= 0 if side == 0 else origin < chips

            @pl.when(there)
            def _(side=side, hop=hop, origin=origin):
                onward(side, hop, origin).wait_recv()

            if hop < chips - 2:

                @pl.when(jnp.logical_and(there, ends[side]))
                def _(side=side, hop=hop, origin=origin):
                    onward(side, hop + 1, origin).start()

            @pl.when(there)
            def _(origin=origin):
                share(origin, core).start()

    own.wait()
    for hop in range(chips - 1):
        for side in range(2):
            origin = chip - hop if side == 0 else chip + hop
            there = origin >= 0 if side == 0 else origin < chips

            @pl.when(jnp.logical_and(there, ends[side]))
            def _(side=side, hop=hop, origin=origin):
                onward(side, hop, origin).wait_send()

    for owner in range(chips):
        share(owner, core).wait_send()
        share(owner, 1 - core).wait_recv()


def gather_line(value, dps, tag):
    dma, chips = pltpu.SemaphoreType.DMA, dps // 2
    out = pl.pallas_call(
        functools.partial(gather_line_body, dps),
        out_shape=jax.ShapeDtypeStruct((dps,) + value.shape, value.dtype),
        in_specs=[pl.BlockSpec(memory_space=pltpu.VMEM)],
        out_specs=pl.BlockSpec(memory_space=pl.ANY),
        scratch_shapes=[
            dma((2, chips - 1)),
            dma((2, chips - 1)),
            dma((chips,)),
            dma((chips,)),
            dma,
        ],
        cost_estimate=lasting(42),
        compiler_params=pltpu.CompilerParams(collective_id=tag, has_side_effects=True),
    )(value)
    return out.reshape(dps * value.shape[0], value.shape[1])


def reduce_line_body(dps, x_ref, o_ref, pair, moving, line_s, line_r, pair_s, pair_r):
    chips, chip, core, ends, sides, sibling = line_place(dps)
    meet([sides[0], sides[1], sibling])

    def share(owner, owner_core):
        return remote(
            x_ref.at[2 * owner + owner_core],
            pair.at[owner],
            pair_s.at[owner],
            pair_r.at[owner],
            sibling,
        )

    def onward(side, owner):
        at = (side, owner)
        return remote(pair.at[owner], moving.at[at], line_s.at[at], line_r.at[at], sides[side])

    order = [at for pair_at in zip(range(chips - 1, -1, -1), range(chips)) for at in pair_at]
    order = list(dict.fromkeys(order))
    for owner in order:
        share(owner, 1 - core).start()
    o_ref[...] = x_ref[2 * chip + core].astype(F32)
    for at in range(chips):
        for side in range(2):
            owner = chips - 1 - at if side == 0 else at
            passing = chip < owner if side == 0 else chip > owner
            fed = jnp.logical_and(passing, ends[1 - side])

            @pl.when(passing)
            def _(owner=owner):
                share(owner, core).wait_recv()

            @pl.when(fed)
            def _(side=side, owner=owner):
                onward(side, owner).wait_recv()
                pair[owner] = (
                    pair[owner].astype(F32)
                    + x_ref[2 * owner + core].astype(F32)
                    + moving[side, owner].astype(F32)
                ).astype(pair.dtype)

            @pl.when(jnp.logical_and(passing, jnp.logical_not(fed)))
            def _(owner=owner):
                pair[owner] = (
                    pair[owner].astype(F32) + x_ref[2 * owner + core].astype(F32)
                ).astype(pair.dtype)

            @pl.when(passing)
            def _(side=side, owner=owner):
                onward(side, owner).start()

    for owner in range(chips):

        @pl.when(chip == owner)
        def _(owner=owner):
            share(owner, core).wait_recv()
            o_ref[...] += pair[owner].astype(F32)

        for side in range(2):

            @pl.when(jnp.logical_and(chip == owner, ends[1 - side]))
            def _(side=side, owner=owner):
                onward(side, owner).wait_recv()
                o_ref[...] += moving[side, owner].astype(F32)

            passing = chip < owner if side == 0 else chip > owner

            @pl.when(passing)
            def _(side=side, owner=owner):
                onward(side, owner).wait_send()

        share(owner, 1 - core).wait_send()


def reduce_line(value, dps, tag):
    rows, wide = value.shape[0] // dps, value.shape[1]
    dma, chips = pltpu.SemaphoreType.DMA, dps // 2
    return pl.pallas_call(
        functools.partial(reduce_line_body, dps),
        out_shape=jax.ShapeDtypeStruct((rows, wide), F32),
        in_specs=[pl.BlockSpec(memory_space=pltpu.VMEM)],
        out_specs=pl.BlockSpec(memory_space=pltpu.VMEM),
        scratch_shapes=[
            pltpu.VMEM((chips, rows, wide), value.dtype),
            pltpu.VMEM((2, chips, rows, wide), value.dtype),
            dma((2, chips)),
            dma((2, chips)),
            dma((chips,)),
            dma((chips,)),
        ],
        cost_estimate=lasting(48),
        compiler_params=pltpu.CompilerParams(collective_id=tag, has_side_effects=True),
    )(value.reshape(dps, rows, wide))


def opening(ways, qkv_ref, x_ref, small_ref, w_ref, all_ref, given_ref, *sems):
    seqs, dps = ways
    chips, count = dps // 2, seqs * dps
    swap_s, swap_r, line_s, line_r, pair_s, pair_r, x_s, x_r, small_s, small_r, own_sem = sems
    seq, dp = lax.axis_index("seq"), lax.axis_index("dp")
    chip, core = dp // 2, lax.rem(dp, 2)
    me = seq * dps + dp
    part, group = qkv_ref.shape[0], w_ref.shape[1] // 3
    width = qkv_ref.shape[1] // 3
    barrier = pltpu.get_barrier_semaphore()

    def other(step):
        at = lax.rem(me + step, count)
        return {"seq": at // dps, "dp": lax.rem(at, dps)}

    @pl.loop(1, count)
    def _(step):
        pl.semaphore_signal(barrier, inc=1, device_id=other(step), device_id_type=MESH)

    pl.semaphore_wait(barrier, count - 1)

    def block(source, owner):
        return w_ref.at[pl.ds(pl.multiple_of((source * dps + owner) * part, part), part), :]

    def piece(source, third):
        rows = pl.ds(pl.multiple_of((source * dps + dp) * part, part), part)
        return w_ref.at[rows, pl.ds(third * group, group)]

    def columns(target, third):
        at = pl.multiple_of(third * width + target * group, 128)
        return qkv_ref.at[:, pl.ds(at, group)]

    swaps = []
    for step in range(1, seqs):
        target = lax.rem(seq + step, seqs)
        for third in range(3):
            at = 3 * (step - 1) + third
            swaps.append(
                remote(
                    columns(target, third),
                    piece(seq, third),
                    swap_s.at[at],
                    swap_r.at[at],
                    {"seq": target},
                )
            )
            swaps[-1].start()
    owns = [
        pltpu.make_async_copy(columns(seq, third), piece(seq, third), own_sem.at[third])
        for third in range(3)
    ]
    for own in owns:
        own.start()

    square = seqs == 4
    if square:
        _, across, along, _ = corners()
        to_across, to_along = {"seq": across}, {"seq": along}
        half = x_ref.shape[0] // 2
        top, low = pl.ds(0, half), pl.ds(half, half)
        copies = [
            push(x_ref.at[top], all_ref.at[seq, top], x_s, x_r, 0, to_across),
            push(x_ref.at[low], all_ref.at[seq, low], x_s, x_r, 1, to_along),
            push(x_ref.at[low], all_ref.at[seq, low], x_s, x_r, 2, to_across),
            push(x_ref.at[top], all_ref.at[seq, top], x_s, x_r, 3, to_along),
        ]
    else:
        copies = [
            push(x_ref, all_ref.at[seq], x_s, x_r, step - 1, {"seq": lax.rem(seq + step, seqs)})
            for step in range(1, seqs)
        ]
    owns.append(pltpu.make_async_copy(x_ref, all_ref.at[seq], own_sem.at[3]))
    owns[3].start()

    def small_copy(step):
        return remote(
            small_ref, given_ref.at[me], small_s.at[step - 1], small_r.at[step - 1], other(step)
        )

    @pl.loop(1, count)
    def _(step):
        small_copy(step).start()

    given_ref[me] = small_ref[...]

    sibling = {"dp": 2 * chip + (1 - core)}
    ends = (chip + 1 < chips, chip >= 1)
    sides = ({"dp": lax.rem(dp + 2, dps)}, {"dp": lax.rem(dp - 2 + dps, dps)})

    def onward(side, hop, source, owner_chip):
        part_of = block(source[1], 2 * owner_chip + core)
        at = (side, hop, source[0])
        return remote(part_of, part_of, line_s.at[at], line_r.at[at], sides[side])

    def share(source, owner_chip, owner_core):
        part_of = block(source[1], 2 * owner_chip + owner_core)
        at = (owner_chip, source[0])
        return remote(part_of, part_of, pair_s.at[at], pair_r.at[at], sibling)

    sources = [(back, lax.rem(seq - back + seqs, seqs)) for back in range(seqs)]
    for source in sources:
        if source[0] == 0:
            for own in owns[:3]:
                own.wait()
        else:
            for third in range(3):
                swaps[3 * (source[0] - 1) + third].wait_recv()
        for side in range(2):

            @pl.when(ends[side])
            def _(side=side, source=source):
                onward(side, 0, source, chip).start()

        share(source, chip, core).start()
    if square:
        copies[0].wait_recv()
        copies.append(push(all_ref.at[across, top], all_ref.at[across, top], x_s, x_r, 4, to_along))
        copies[1].wait_recv()
        copies.append(push(all_ref.at[along, low], all_ref.at[along, low], x_s, x_r, 5, to_across))
    for hop in range(chips - 1):
        for source in sources:
            for side in range(2):
                origin = chip - 1 - hop if side == 0 else chip + 1 + hop
                there = origin >= 0 if side == 0 else origin < chips

                @pl.when(there)
                def _(side=side, hop=hop, source=source, origin=origin):
                    onward(side, hop, source, origin).wait_recv()
                    share(source, origin, core).start()

                if hop < chips - 2:

                    @pl.when(jnp.logical_and(there, ends[side]))
                    def _(side=side, hop=hop, source=source, origin=origin):
                        onward(side, hop + 1, source, origin).start()

    for swapped in swaps:
        swapped.wait_send()
    for at, copy in enumerate(copies):
        copy.wait_send()
        if not square or at > 1:
            copy.wait_recv()
    owns[3].wait()

    @pl.loop(1, count)
    def _(step):
        small_copy(step).wait()

    for hop in range(chips - 1):
        for source in sources:
            for side in range(2):
                origin = chip - hop if side == 0 else chip + hop
                there = origin >= 0 if side == 0 else origin < chips

                @pl.when(jnp.logical_and(there, ends[side]))
                def _(side=side, hop=hop, source=source, origin=origin):
                    onward(side, hop, source, origin).wait_send()

    for owner in range(chips):
        for source in sources:
            share(source, owner, core).wait_send()
            share(source, owner, 1 - core).wait_recv()


def open_all(ways, qkv_weight, rows_in, small):
    seqs, dps = ways
    chips, count = dps // 2, seqs * dps
    part, group = qkv_weight.shape[0], qkv_weight.shape[1] // (3 * seqs)
    slots = 6 if seqs == 4 else seqs - 1
    dma = pltpu.SemaphoreType.DMA
    return pl.pallas_call(
        functools.partial(opening, ways),
        out_shape=(
            jax.ShapeDtypeStruct((part * count, 3 * group), BF16),
            jax.ShapeDtypeStruct((seqs,) + rows_in.shape, BF16),
            jax.ShapeDtypeStruct((count,) + small.shape, BF16),
        ),
        in_specs=[pl.BlockSpec(memory_space=pltpu.VMEM)] * 3,
        out_specs=(
            pl.BlockSpec(memory_space=pl.ANY),
            pl.BlockSpec(memory_space=pl.ANY),
            pl.BlockSpec(memory_space=pltpu.VMEM),
        ),
        scratch_shapes=[
            dma((3 * (seqs - 1),)),
            dma((3 * (seqs - 1),)),
            dma((2, chips - 1, seqs)),
            dma((2, chips - 1, seqs)),
            dma((chips, seqs)),
            dma((chips, seqs)),
            dma((slots,)),
            dma((slots,)),
            dma((count - 1,)),
            dma((count - 1,)),
            dma((4,)),
        ],
        cost_estimate=lasting(75),
        compiler_params=pltpu.CompilerParams(collective_id=0, has_side_effects=True),
    )(qkv_weight, rows_in, small)


def after(value, *earlier):
    return lax.optimization_barrier((value,) + earlier)[0]


def attention_forward(queries, keys, values):
    length = queries.shape[0]
    scale = HEAD_DIM ** (-0.5)
    index = jnp.arange(length, dtype=jnp.int32)
    allowed = index[None, :] <= index[:, None]
    scores = jnp.einsum("qhd,khd->hqk", queries, keys, preferred_element_type=F32) * scale
    scores = jnp.where(allowed[None], scores, -jnp.inf)
    largest = jnp.max(scores, axis=-1, keepdims=True)
    exponent = jnp.exp(scores - largest)
    totals = jnp.sum(exponent, axis=-1, keepdims=True)
    probs = exponent / totals
    mixed = jnp.einsum("hqk,khd->qhd", probs.astype(BF16), values, preferred_element_type=F32)
    return mixed.astype(BF16), (largest + jnp.log(totals))


def attention_backward(queries, keys, values, log_total, grad):
    length = queries.shape[0]
    scale = HEAD_DIM ** (-0.5)
    index = jnp.arange(length, dtype=jnp.int32)
    allowed = index[None, :] <= index[:, None]
    scores = jnp.einsum("qhd,khd->hqk", queries, keys, preferred_element_type=F32) * scale
    scores = jnp.where(allowed[None], scores, -jnp.inf)
    probs = jnp.exp(scores - log_total)
    values_grad = jnp.einsum("hqk,qhd->khd", probs.astype(BF16), grad, preferred_element_type=F32)
    probs_grad = jnp.einsum("qhd,khd->hqk", grad, values, preferred_element_type=F32)
    scores_grad = (
        probs * (probs_grad - jnp.sum(probs * probs_grad, axis=-1, keepdims=True))
    ).astype(BF16)
    query_grad = jnp.einsum("hqk,khd->qhd", scores_grad, keys, preferred_element_type=F32) * scale
    keys_grad = jnp.einsum("hqk,qhd->khd", scores_grad, queries, preferred_element_type=F32) * scale
    return query_grad.astype(BF16), keys_grad.astype(BF16), values_grad.astype(BF16)


def shards(
    ways,
    inputs,
    first_gain,
    first_shift,
    qkv_weight,
    qkv_bias,
    out_weight,
    second_gain,
    second_shift,
    gate_weight,
    up_weight,
    down_weight,
    out_cotangent,
):
    seqs, dps = ways
    width = inputs.shape[2]
    rows = inputs.shape[1]
    length = rows * seqs
    part = width // (seqs * dps)
    units = down_weight.shape[0]
    group = width // seqs
    heads = group // HEAD_DIM
    me_seq = lax.axis_index("seq")
    grad_out = out_cotangent[0]
    hidden_in = inputs[0].astype(F32)

    small = jnp.concatenate([first_gain, first_shift, second_gain, second_shift, qkv_bias])
    total = small.shape[0]
    padded = -(-total // 2048) * 2048
    small = jnp.pad(small, (0, padded - total)).reshape(padded // 128, 128)
    qkv_full, inputs_all, small = open_all(ways, qkv_weight, inputs[0], small)
    small = small.reshape(seqs * dps, padded)[:, :total].astype(F32)
    gain_one = small[:, :part].reshape(-1)
    shift_one = small[:, part : 2 * part].reshape(-1)
    gain_two = small[:, 2 * part : 3 * part].reshape(-1)
    shift_two = small[:, 3 * part : 4 * part].reshape(-1)
    bias = small[:, 4 * part :].reshape(3, seqs, group)
    bias = lax.dynamic_index_in_dim(bias, me_seq, 1, keepdims=False).reshape(3 * group)

    down_full = gather(down_weight, "seq")
    out_full = gather(out_weight, "dp")
    grad_all = gather(grad_out, "dp")

    def cut_units(weight):
        cut = weight.reshape(part, seqs, dps, units).transpose(2, 0, 1, 3)
        return cut.reshape(dps * part, seqs * units)

    gate_cut = jnp.concatenate([cut_units(gate_weight), cut_units(up_weight)], 1)
    gate_cut = after(gate_cut, inputs_all)
    moved = move_blocks(gate_cut, "dp", dps)
    wide = seqs * units

    normed_one, inverse_one = normalize(hidden_in)
    normed_all, _ = normalize(inputs_all.reshape(length, width).astype(F32))
    attn_all = (normed_all * gain_one + shift_one).astype(BF16)
    projected = dot(attn_all, qkv_full) + bias
    cosine, sine = tables(jnp.arange(length, dtype=jnp.int32).astype(F32))

    def to_heads(flat):
        return flat.reshape(length, heads, HEAD_DIM)

    queries = rotate(to_heads(projected[:, :group]), cosine, sine).astype(BF16)
    keys = rotate(to_heads(projected[:, group : 2 * group]), cosine, sine).astype(BF16)
    values = to_heads(projected[:, 2 * group :]).astype(BF16)
    attended, log_total = attention_forward(queries, keys, values)
    attended = attended.reshape(length, group)
    moved, attended = lax.optimization_barrier((moved, attended))
    gate_cut = place_blocks(moved, "dp")
    gate_up = gather(gate_cut, "seq")
    branch = dot(attended, out_full).astype(BF16)
    branch = reduce_seq(branch, seqs, 1)
    residual = hidden_in + branch

    normed_two, inverse_two = normalize(residual)
    mlp_input = (normed_two * gain_two + shift_two).astype(BF16)
    mlp_all = gather_line(mlp_input, dps, 4)
    both = dot(mlp_all, gate_up)
    gate_value = both[:, :wide]
    up_value = both[:, wide:]
    sigmoid_gate = jax.nn.sigmoid(gate_value)
    activated = gate_value * sigmoid_gate
    hidden = (activated * up_value).astype(BF16)
    out_part = dot(hidden, down_full).astype(BF16)

    hidden_grad = contract_cols(grad_all, down_full)
    gate_grad = (
        hidden_grad * up_value * (sigmoid_gate * (1.0 + gate_value * (1.0 - sigmoid_gate)))
    ).astype(BF16)
    up_grad = (hidden_grad * activated).astype(BF16)
    both_grad = jnp.concatenate([gate_grad, up_grad], 1)
    mlp_part = contract_cols(both_grad, gate_up).astype(BF16)
    both_rows = contract_rows(mlp_all, after(both_grad, mlp_part)).astype(BF16)
    down_rows = contract_rows(hidden, grad_all).astype(BF16)
    mlp_part = after(mlp_part, both_rows, down_rows)
    mlp_grad = reduce_line(mlp_part, dps, 6)
    both_rows = scatter_sum(both_rows, "seq")
    down_shard = scatter_sum(down_rows, "seq").astype(F32)
    out_part = after(out_part, mlp_grad)
    layer_out = scatter_sum(out_part, "dp")
    layer_out = residual + layer_out.astype(F32)
    gain_two_grad = jnp.sum(mlp_grad * normed_two, axis=0)
    shift_two_grad = jnp.sum(mlp_grad, axis=0)
    residual_grad = grad_out.astype(F32) + norm_back(mlp_grad, normed_two, inverse_two, gain_two)
    branch_grad = residual_grad.astype(BF16)

    branch_all = gather_seq(branch_grad, seqs, 2)
    attended_grad = contract_cols(branch_all, out_full).astype(BF16)
    query_grad, keys_grad, values_grad = attention_backward(
        queries, keys, values, log_total, to_heads(attended_grad)
    )
    query_plain = rotate(query_grad.astype(F32), cosine, -sine).astype(BF16)
    keys_plain = rotate(keys_grad.astype(F32), cosine, -sine).astype(BF16)
    projected_grad = jnp.concatenate(
        [item.reshape(length, group) for item in (query_plain, keys_plain, values_grad)], 1
    )
    attn_grad = contract_cols(projected_grad, qkv_full).astype(BF16)
    attn_grad = reduce_seq(attn_grad, seqs, 3)
    gain_one_grad = jnp.sum(attn_grad * normed_one, axis=0)
    shift_one_grad = jnp.sum(attn_grad, axis=0)
    input_grad = residual_grad + norm_back(attn_grad, normed_one, inverse_one, gain_one)

    both_rows = swap(both_rows, "dp", 0, 0).reshape(dps, part, 2, seqs, units)
    both_rows = both_rows.transpose(2, 1, 3, 0, 4).reshape(2, part, seqs * dps * units).astype(F32)
    out_rows = contract_rows(attended, branch_all).astype(BF16)
    out_shard = scatter_sum(out_rows, "dp").astype(F32)
    qkv_rows = contract_rows(attn_all, projected_grad).astype(BF16)
    qkv_rows = qkv_rows.reshape(seqs, dps, part, 3 * group).swapaxes(0, 1)
    qkv_rows = qkv_rows.reshape(width, 3 * group)
    qkv_rows = scatter_sum(qkv_rows, "dp")
    qkv_rows = swap(qkv_rows, "seq", 0, 0).reshape(seqs, part, 3, group)
    qkv_shard = qkv_rows.transpose(1, 2, 0, 3).reshape(part, 3 * width).astype(F32)

    bias_term = jnp.sum(projected_grad.astype(F32), axis=0).reshape(3, 1, group)
    here = (jnp.arange(seqs, dtype=jnp.int32) == me_seq).astype(F32)[None, :, None]
    bias_term = (bias_term * here).reshape(seqs * dps, 3 * part)
    terms = [gain_one_grad, shift_one_grad, gain_two_grad, shift_two_grad]
    terms = [item.reshape(seqs * dps, part) for item in terms] + [bias_term]
    terms = jnp.concatenate(terms, 1)
    padded = -(-total // 1024) * 1024
    terms = jnp.pad(terms, ((0, 0), (0, padded - total))).reshape(seqs * dps, padded // 128, 128)
    tiny = exchange_all(terms, ways, False, 5).reshape(padded)
    return (
        layer_out.astype(BF16)[None],
        input_grad.astype(BF16)[None],
        tiny[:part],
        tiny[part : 2 * part],
        qkv_shard,
        tiny[4 * part : total],
        out_shard,
        tiny[2 * part : 3 * part],
        tiny[3 * part : 4 * part],
        both_rows[0],
        both_rows[1],
        down_shard,
    )


def solution(mesh):
    split = ("seq", "dp")
    tokens = P("dp", "seq", None)
    in_specs = (
        tokens,
        P(split),
        P(split),
        P(split, None),
        P(split),
        P(split, None),
        P(split),
        P(split),
        P(split, None),
        P(split, None),
        P(split, None),
        tokens,
    )
    out_specs = (
        tokens,
        tokens,
        P(split),
        P(split),
        P(split, None),
        P(split),
        P(split, None),
        P(split),
        P(split),
        P(split, None),
        P(split, None),
        P(split, None),
    )
    ways = (mesh.shape["seq"], mesh.shape["dp"])

    def local(*args):
        return shards(ways, *args)

    return jax.shard_map(local, mesh=mesh, in_specs=in_specs, out_specs=out_specs, check_vma=False)
```

```python
import functools

import jax
import jax.numpy as jnp
from jax import lax
from jax.experimental import pallas as pl
from jax.experimental.pallas import tpu as pltpu
from jax.sharding import PartitionSpec as P


HEAD_DIM = 64
ROT = 16
F32 = jnp.float32
BF16 = jnp.bfloat16


def normalize(values):
    center = values - jnp.mean(values, axis=-1, keepdims=True)
    variance = jnp.mean(center * center, axis=-1, keepdims=True)
    inverse = lax.rsqrt(variance + 1e-05)
    return (center * inverse, inverse)


def norm_back(grad_normed, normed, inverse, gain):
    scaled = grad_normed * gain
    centered = scaled - jnp.mean(scaled, axis=-1, keepdims=True)
    return inverse * (centered - normed * jnp.mean(scaled * normed, axis=-1, keepdims=True))


def dot(left, right):
    return jnp.dot(left, right, preferred_element_type=F32)


def contract_rows(left, right):
    return lax.dot_general(left, right, (((0,), (0,)), ((), ())), preferred_element_type=F32)


def contract_cols(left, right):
    return lax.dot_general(left, right, (((1,), (1,)), ((), ())), preferred_element_type=F32)


def tables(positions):
    half_rot = ROT // 2
    freqs = 10000.0 ** (-(2.0 * jnp.arange(half_rot, dtype=F32)) / ROT)
    angles = positions[:, None] * freqs[None, :]
    cosine = jnp.cos(angles)
    sine = jnp.sin(angles)
    return (jnp.concatenate([cosine, cosine], -1), jnp.concatenate([sine, sine], -1))


def rotate(heads_in, cosine, sine):
    half_rot = ROT // 2
    rotary = heads_in[..., :ROT]
    turned = jnp.concatenate([-rotary[..., half_rot:], rotary[..., :half_rot]], -1)
    moved = rotary * cosine[:, None, :] + turned * sine[:, None, :]
    return jnp.concatenate([moved, heads_in[..., ROT:]], -1)


def gather(value, axis):
    return lax.all_gather(value, axis, axis=0, tiled=True)


def scatter_sum(value, axis):
    return lax.psum_scatter(value, axis, scatter_dimension=0, tiled=True)


def swap(value, axis, split, concat):
    return lax.all_to_all(value, axis, split_axis=split, concat_axis=concat, tiled=True)


MESH = pl.DeviceIdType.MESH


def lasting(micros):
    return pl.CostEstimate(flops=0, transcendentals=0, bytes_accessed=int(micros * 3.0e6))


def meet(peers):
    barrier = pltpu.get_barrier_semaphore()
    for peer in peers:
        pl.semaphore_signal(barrier, inc=1, device_id=peer, device_id_type=MESH)
    pl.semaphore_wait(barrier, len(peers))


def push(source, target, send, recv, at, peer):
    copy = pltpu.make_async_remote_copy(
        src_ref=source,
        dst_ref=target,
        send_sem=send.at[at],
        recv_sem=recv.at[at],
        device_id=peer,
        device_id_type=MESH,
    )
    copy.start()
    return copy


def corners():
    me = lax.axis_index("seq")
    high, low = me // 2, lax.rem(me, 2)
    across = high * 2 + (1 - low)
    along = (1 - high) * 2 + low
    return me, across, along, 3 - me


def move_blocks(value, axis, count):
    rows = value.shape[0] // count
    me = lax.axis_index(axis)
    blocks = []
    for step in range(count):
        at = lax.rem(me + step, count) * rows
        block = lax.dynamic_slice_in_dim(value, at, rows, 0)
        if step:
            block = lax.ppermute(block, axis, [(i, (i + step) % count) for i in range(count)])
        blocks.append(block)
    return blocks


def place_blocks(blocks, axis):
    count, rows = len(blocks), blocks[0].shape[0]
    me = lax.axis_index(axis)
    out = jnp.zeros((count * rows,) + blocks[0].shape[1:], blocks[0].dtype)
    for step, block in enumerate(blocks):
        at = lax.rem(me - step + count, count) * rows
        out = lax.dynamic_update_slice_in_dim(out, block, at, 0)
    return out


def remote(source, target, send, recv, peer):
    return pltpu.make_async_remote_copy(
        src_ref=source,
        dst_ref=target,
        send_sem=send,
        recv_sem=recv,
        device_id=peer,
        device_id_type=MESH,
    )


def line_place(dps):
    dp = lax.axis_index("dp")
    chip, core = dp // 2, lax.rem(dp, 2)
    chips = dps // 2
    ends = (chip + 1 < chips, chip >= 1)
    sides = ({"dp": lax.rem(dp + 2, dps)}, {"dp": lax.rem(dp - 2 + dps, dps)})
    return chips, chip, core, ends, sides, {"dp": 2 * chip + (1 - core)}


class Plane:

    def __init__(self, count, x_ref, pair, got, send, recv):
        self.count, self.x, self.pair, self.got = count, x_ref, pair, got
        self.send, self.recv = send, recv
        self.square = count == 4

    def begin(self):
        x, got, send, recv = self.x, self.got, self.send, self.recv
        if not self.square:
            me = lax.axis_index("seq")
            targets = [lax.rem(me + step, self.count) for step in range(1, self.count)]
            self.copies = [
                push(x.at[target], got.at[at], send, recv, at, {"seq": target})
                for at, target in enumerate(targets)
            ]
            return
        _, across, along, far = corners()
        half = x.shape[1] // 2
        top, low = pl.ds(0, half), pl.ds(half, half)
        to_across, to_along = {"seq": across}, {"seq": along}
        self.copies = [
            push(x.at[far, top], self.pair.at[0], send, recv, 0, to_across),
            push(x.at[far, low], self.pair.at[1], send, recv, 1, to_along),
            push(x.at[across, top], got.at[0, top], send, recv, 2, to_across),
            push(x.at[along, low], got.at[1, low], send, recv, 3, to_along),
        ]

    def relay(self):
        if not self.square:
            return
        x, pair, got, send, recv = self.x, self.pair, self.got, self.send, self.recv
        _, across, along, _ = corners()
        half = x.shape[1] // 2
        top, low = pl.ds(0, half), pl.ds(half, half)
        self.copies[0].wait_recv()
        pair[2] = (pair[0].astype(F32) + x[along, top].astype(F32)).astype(pair.dtype)
        self.copies.append(push(pair.at[2], got.at[1, top], send, recv, 4, {"seq": along}))
        self.copies[1].wait_recv()
        pair[3] = (pair[1].astype(F32) + x[across, low].astype(F32)).astype(pair.dtype)
        self.copies.append(push(pair.at[3], got.at[0, low], send, recv, 5, {"seq": across}))

    def end(self):
        for at, copy in enumerate(self.copies):
            copy.wait_send()
            if not self.square or at > 1:
                copy.wait_recv()

    def total(self, rows):
        value = self.x[lax.axis_index("seq"), rows].astype(F32)
        for at in range(2 if self.square else self.count - 1):
            value = value + self.got[at, rows].astype(F32)
        return value

    @staticmethod
    def scratch(count, rows, wide, dtype):
        slots = 6 if count == 4 else count - 1
        return [
            pltpu.VMEM((4, rows // 2, wide), dtype),
            pltpu.VMEM((2 if count == 4 else count - 1, rows, wide), dtype),
            pltpu.SemaphoreType.DMA((slots,)),
            pltpu.SemaphoreType.DMA((slots,)),
        ]


class LineSum:

    def __init__(self, dps, block, pair, moving, line_s, line_r, pair_s, pair_r):
        self.block, self.pair, self.moving = block, pair, moving
        self.sems = (line_s, line_r, pair_s, pair_r)
        self.chips, self.chip, self.core, self.ends, self.sides, self.sibling = line_place(dps)

    def share(self, owner, owner_core):
        return remote(
            self.block(2 * owner + owner_core),
            self.pair.at[owner],
            self.sems[2].at[owner],
            self.sems[3].at[owner],
            self.sibling,
        )

    def onward(self, side, owner):
        at = (side, owner)
        return remote(
            self.pair.at[owner],
            self.moving.at[at],
            self.sems[0].at[at],
            self.sems[1].at[at],
            self.sides[side],
        )

    def begin(self):
        order = [
            at for both in zip(range(self.chips - 1, -1, -1), range(self.chips)) for at in both
        ]
        for owner in dict.fromkeys(order):
            self.share(owner, 1 - self.core).start()

    def add(self, owner, side):
        own = self.block(2 * owner + self.core)

        def one(at):
            value = self.pair[(owner,) + at].astype(F32) + own[at].astype(F32)
            if side is not None:
                value = value + self.moving[(side, owner) + at].astype(F32)
            self.pair[(owner,) + at] = value.astype(self.pair.dtype)

        if len(own.shape) > 2:
            for at in range(own.shape[0]):
                one((at,))
        else:
            by_chunks(own.shape[0], lambda here: one((here,)))

    def step(self, at):
        for side in range(2):
            owner = self.chips - 1 - at if side == 0 else at
            passing = self.chip < owner if side == 0 else self.chip > owner
            fed = jnp.logical_and(passing, self.ends[1 - side])

            @pl.when(passing)
            def _(owner=owner):
                self.share(owner, self.core).wait_recv()

            @pl.when(fed)
            def _(side=side, owner=owner):
                self.onward(side, owner).wait_recv()
                self.add(owner, side)

            @pl.when(jnp.logical_and(passing, jnp.logical_not(fed)))
            def _(owner=owner):
                self.add(owner, None)

            @pl.when(passing)
            def _(side=side, owner=owner):
                self.onward(side, owner).start()

    def end(self):
        for owner in range(self.chips):

            @pl.when(self.chip == owner)
            def _(owner=owner):
                self.share(owner, self.core).wait_recv()

            for side in range(2):

                @pl.when(jnp.logical_and(self.chip == owner, self.ends[1 - side]))
                def _(side=side, owner=owner):
                    self.onward(side, owner).wait_recv()

                @pl.when(jnp.logical_and(self.chip == owner, jnp.logical_not(self.ends[1 - side])))
                def _(side=side, owner=owner):
                    self.moving[side, owner] = jnp.zeros(self.moving.shape[2:], self.moving.dtype)

    def total(self, at):
        own = self.block(2 * self.chip + self.core)
        value = own[at].astype(F32) + self.pair[(self.chip,) + at].astype(F32)
        for side in range(2):
            value = value + self.moving[(side, self.chip) + at].astype(F32)
        return value

    def drain(self):
        for owner in range(self.chips):
            for side in range(2):
                passing = self.chip < owner if side == 0 else self.chip > owner

                @pl.when(passing)
                def _(side=side, owner=owner):
                    self.onward(side, owner).wait_send()

            self.share(owner, 1 - self.core).wait_send()

    @staticmethod
    def scratch(dps, shape, dtype):
        dma, chips = pltpu.SemaphoreType.DMA, dps // 2
        return [
            pltpu.VMEM((chips,) + shape, dtype),
            pltpu.VMEM((2, chips) + shape, dtype),
            dma((2, chips)),
            dma((2, chips)),
            dma((chips,)),
            dma((chips,)),
        ]


class PlaneGather:

    def __init__(self, count, x_ref, o_ref, send, recv, local):
        self.count, self.x, self.o = count, x_ref, o_ref
        self.send, self.recv, self.local = send, recv, local
        self.square = count == 4

    def begin(self):
        x, o, send, recv = self.x, self.o, self.send, self.recv
        me = lax.axis_index("seq")
        if self.square:
            _, across, along, _ = corners()
            half = x.shape[0] // 2
            top, low = pl.ds(0, half), pl.ds(half, half)
            to_across, to_along = {"seq": across}, {"seq": along}
            self.copies = [
                push(x.at[top], o.at[me, top], send, recv, 0, to_across),
                push(x.at[low], o.at[me, low], send, recv, 1, to_along),
                push(x.at[low], o.at[me, low], send, recv, 2, to_across),
                push(x.at[top], o.at[me, top], send, recv, 3, to_along),
            ]
        else:
            self.copies = [
                push(x, o.at[me], send, recv, step - 1, {"seq": lax.rem(me + step, self.count)})
                for step in range(1, self.count)
            ]
        self.own = pltpu.make_async_copy(x, o.at[me], self.local)
        self.own.start()

    def relay(self):
        if not self.square:
            return
        o, send, recv = self.o, self.send, self.recv
        _, across, along, _ = corners()
        half = self.x.shape[0] // 2
        top, low = pl.ds(0, half), pl.ds(half, half)
        self.copies[0].wait_recv()
        self.copies.append(
            push(o.at[across, top], o.at[across, top], send, recv, 4, {"seq": along})
        )
        self.copies[1].wait_recv()
        self.copies.append(
            push(o.at[along, low], o.at[along, low], send, recv, 5, {"seq": across})
        )

    def end(self):
        for at, copy in enumerate(self.copies):
            copy.wait_send()
            if not self.square or at > 1:
                copy.wait_recv()
        self.own.wait()

    @staticmethod
    def scratch(count):
        slots = 6 if count == 4 else count - 1
        dma = pltpu.SemaphoreType.DMA
        return [dma((slots,)), dma((slots,)), dma]


class LineGather:

    def __init__(self, dps, x_ref, o_ref, line_s, line_r, pair_s, pair_r, local):
        self.x, self.o, self.local = x_ref, o_ref, local
        self.sems = (line_s, line_r, pair_s, pair_r)
        self.chips, self.chip, self.core, self.ends, self.sides, self.sibling = line_place(dps)

    def onward(self, side, hop, owner, source=None):
        block = self.o.at[2 * owner + self.core]
        at = (side, hop)
        return remote(
            block if source is None else source,
            block,
            self.sems[0].at[at],
            self.sems[1].at[at],
            self.sides[side],
        )

    def share(self, owner, owner_core, source=None):
        block = self.o.at[2 * owner + owner_core]
        return remote(
            block if source is None else source,
            block,
            self.sems[2].at[owner],
            self.sems[3].at[owner],
            self.sibling,
        )

    def begin(self):
        for side in range(2):

            @pl.when(self.ends[side])
            def _(side=side):
                self.onward(side, 0, self.chip, self.x).start()

        self.share(self.chip, self.core, self.x).start()
        self.own = pltpu.make_async_copy(
            self.x, self.o.at[2 * self.chip + self.core], self.local
        )
        self.own.start()

    def hop(self, hop):
        for side in range(2):
            origin = self.chip - 1 - hop if side == 0 else self.chip + 1 + hop
            there = origin >= 0 if side == 0 else origin < self.chips

            @pl.when(there)
            def _(side=side, origin=origin):
                self.onward(side, hop, origin).wait_recv()

            if hop < self.chips - 2:

                @pl.when(jnp.logical_and(there, self.ends[side]))
                def _(side=side, origin=origin):
                    self.onward(side, hop + 1, origin).start()

            @pl.when(there)
            def _(origin=origin):
                self.share(origin, self.core).start()

    def end(self):
        self.own.wait()
        for hop in range(self.chips - 1):
            for side in range(2):
                origin = self.chip - hop if side == 0 else self.chip + hop
                there = origin >= 0 if side == 0 else origin < self.chips

                @pl.when(jnp.logical_and(there, self.ends[side]))
                def _(side=side, hop=hop, origin=origin):
                    self.onward(side, hop, origin).wait_send()

        for owner in range(self.chips):
            self.share(owner, self.core).wait_send()
            self.share(owner, 1 - self.core).wait_recv()

    @staticmethod
    def scratch(dps):
        dma, chips = pltpu.SemaphoreType.DMA, dps // 2
        return [dma((2, chips - 1)), dma((2, chips - 1)), dma((chips,)), dma((chips,)), dma]


CHUNK = 16


def by_chunks(rows, body):
    @pl.loop(0, rows // CHUNK)
    def _(at):
        body(pl.ds(pl.multiple_of(at * CHUNK, CHUNK), CHUNK))


def meet_cross(ways):
    seqs, dps = ways
    seq, dp = lax.axis_index("seq"), lax.axis_index("dp")
    seq_peers = [lax.rem(seq + step, seqs) for step in range(1, seqs)]
    dp_peers = [lax.rem(dp + step, dps) for step in range(1, dps)]
    meet([{"seq": peer} for peer in seq_peers] + [{"dp": peer} for peer in dp_peers])
    return seq_peers, dp_peers


def middle(ways, part_ref, x_ref, gain_ref, shift_ref, grad_ref, cut_ref, *rest):
    seqs, dps = ways
    resid_ref, all_ref, grads_ref, gate_ref = rest[:4]
    plane = Plane(seqs, part_ref, *rest[4:8])
    own = rest[8]
    moved = LineGather(dps, own, all_ref, *rest[9:14])
    grads = LineGather(dps, grad_ref, grads_ref, *rest[14:19])
    gates = PlaneGather(seqs, cut_ref, gate_ref, *rest[19:22])
    hops = dps // 2 - 1
    meet_cross(ways)
    plane.begin()
    grads.begin()
    plane.relay()
    plane.end()
    gates.begin()
    gain, shift = gain_ref[...], shift_ref[...]

    def one(here):
        resid = x_ref[here, :].astype(F32) + plane.total(here)
        resid_ref[here, :] = resid
        normed, _ = normalize(resid)
        own[here, :] = (normed * gain + shift).astype(own.dtype)

    by_chunks(x_ref.shape[0], one)
    moved.begin()
    for hop in range(hops):
        grads.hop(hop)
        if hop == hops - 1:
            gates.relay()
        moved.hop(hop)
    grads.end()
    moved.end()
    gates.end()


def middle_all(ways, part, inputs, gain, shift, grad_out, cut, tag):
    seqs, dps = ways
    rows, wide = inputs.shape
    vmem, anywhere = (pl.BlockSpec(memory_space=space) for space in (pltpu.VMEM, pl.ANY))
    resid, moved, grads, gate = pl.pallas_call(
        functools.partial(middle, ways),
        out_shape=(
            jax.ShapeDtypeStruct((rows, wide), F32),
            jax.ShapeDtypeStruct((dps, rows, wide), BF16),
            jax.ShapeDtypeStruct((dps, rows, wide), BF16),
            jax.ShapeDtypeStruct((seqs,) + cut.shape, BF16),
        ),
        in_specs=[vmem] * 6,
        out_specs=(vmem, anywhere, anywhere, anywhere),
        scratch_shapes=Plane.scratch(seqs, rows, wide, BF16)
        + [pltpu.VMEM((rows, wide), BF16)]
        + LineGather.scratch(dps)
        + LineGather.scratch(dps)
        + PlaneGather.scratch(seqs),
        cost_estimate=lasting(75),
        compiler_params=pltpu.CompilerParams(collective_id=tag, has_side_effects=True),
    )(part.reshape(seqs, rows, wide), inputs, gain, shift, grad_out, cut)
    moved, grads = (item.reshape(dps * rows, wide) for item in (moved, grads))
    return resid, moved, grads, gate.reshape(seqs * cut.shape[0], cut.shape[1])


def turning(ways, part_ref, resid_ref, gain_ref, grad_ref, out_ref, both_ref, *rest):
    seqs, dps = ways
    total_ref, all_ref, sums_ref, layer_ref, rows_ref = rest[:5]
    line = LineSum(dps, lambda owner: part_ref.at[owner], *rest[5:11])
    own = rest[11]
    gathered = PlaneGather(seqs, own, all_ref, *rest[12:15])
    outs = LineSum(dps, lambda owner: out_ref.at[owner], *rest[15:21])
    both = Plane(seqs, both_ref, *rest[21:25])
    chips = dps // 2
    meet_cross(ways)
    line.begin()
    both.begin()
    line.step(0)
    both.relay()
    outs.begin()
    for at in range(1, chips):
        line.step(at)
    outs.step(0)
    line.end()
    sums_ref[...] = jnp.zeros(sums_ref.shape, F32)
    gain = gain_ref[...]

    def one(here):
        grad = line.total((here,))
        normed, inverse = normalize(resid_ref[here, :])
        sums_ref[2:3, :] += jnp.sum(grad * normed, axis=0, keepdims=True)
        sums_ref[3:4, :] += jnp.sum(grad, axis=0, keepdims=True)
        total = grad_ref[here, :].astype(F32) + norm_back(grad, normed, inverse, gain)
        total_ref[here, :] = total
        own[here, :] = total.astype(own.dtype)

    by_chunks(resid_ref.shape[0], one)
    gathered.begin()
    if chips > 1:
        outs.step(1)
    gathered.relay()
    for at in range(2, chips):
        outs.step(at)
    both.end()

    def two(here):
        rows_ref[here, :] = both.total(here).astype(rows_ref.dtype)

    by_chunks(rows_ref.shape[0], two)
    gathered.end()
    outs.end()

    def three(here):
        layer_ref[here, :] = (resid_ref[here, :] + outs.total((here,))).astype(layer_ref.dtype)

    by_chunks(resid_ref.shape[0], three)
    line.drain()
    outs.drain()


def turn_all(ways, part, resid, gain, grad_out, out_part, both, tag):
    seqs, dps = ways
    rows, wide = resid.shape
    cut = (both.shape[0] // seqs, both.shape[1])
    vmem, anywhere = (pl.BlockSpec(memory_space=space) for space in (pltpu.VMEM, pl.ANY))
    total, gathered, sums, layer, both = pl.pallas_call(
        functools.partial(turning, ways),
        out_shape=(
            jax.ShapeDtypeStruct((rows, wide), F32),
            jax.ShapeDtypeStruct((seqs, rows, wide), BF16),
            jax.ShapeDtypeStruct((8, wide), F32),
            jax.ShapeDtypeStruct((rows, wide), BF16),
            jax.ShapeDtypeStruct(cut, BF16),
        ),
        in_specs=[vmem] * 6,
        out_specs=(vmem, anywhere, vmem, vmem, vmem),
        scratch_shapes=LineSum.scratch(dps, (rows, wide), BF16)
        + [pltpu.VMEM((rows, wide), BF16)]
        + PlaneGather.scratch(seqs)
        + LineSum.scratch(dps, (rows, wide), BF16)
        + Plane.scratch(seqs, cut[0], cut[1], BF16),
        cost_estimate=lasting(85),
        compiler_params=pltpu.CompilerParams(
            collective_id=tag, has_side_effects=True, vmem_limit_bytes=60 * 2**20
        ),
    )(
        part.reshape(dps, rows, wide),
        resid,
        gain,
        grad_out,
        out_part.reshape(dps, rows, wide),
        both.reshape((seqs,) + cut),
    )
    return total, gathered.reshape(seqs * rows, wide), sums, layer, both


def closing(ways, w_ref, g_ref, sums_ref, x_ref, gain_ref, resid_ref, both_ref, *rest):
    seqs, dps = ways
    qkv_ref, grad_ref, tiny_ref, gate_ref, up_ref = rest[:5]
    plane = Plane(seqs, g_ref, *rest[5:9])
    line = LineSum(dps, lambda owner: w_ref.at[:, owner], *rest[9:15])
    landed, mine, near, far, part_sum = rest[15:20]
    swap_s, swap_r, near_s, near_r, far_s, far_r = rest[20:]
    seq, dp = lax.axis_index("seq"), lax.axis_index("dp")
    seq_peers, dp_peers = meet_cross(ways)
    line.begin()
    plane.begin()
    plane.relay()
    line.step(0)
    plane.end()
    part_sum[...] = sums_ref[...]
    gain = gain_ref[...]

    def one(here):
        grad = plane.total(here)
        normed, inverse = normalize(x_ref[here, :].astype(F32))
        part_sum[0:1, :] += jnp.sum(grad * normed, axis=0, keepdims=True)
        part_sum[1:2, :] += jnp.sum(grad, axis=0, keepdims=True)
        grad_ref[here, :] = (
            resid_ref[here, :] + norm_back(grad, normed, inverse, gain)
        ).astype(grad_ref.dtype)

    by_chunks(x_ref.shape[0], one)
    wide = x_ref.shape[1]
    nears = [
        push(part_sum, near.at[seq], near_s, near_r, at, {"seq": peer})
        for at, peer in enumerate(seq_peers)
    ]
    near[seq] = part_sum[...]
    line.step(1)
    for copy in nears:
        copy.wait()
    far[dp] = jnp.sum(near[...], axis=0)
    units = gate_ref.shape[1] // (seqs * dps)
    for at, weight in enumerate((gate_ref, up_ref)):
        for source in range(seqs):
            for owner in range(dps):
                weight[:, pl.ds((source * dps + owner) * units, units)] = both_ref[
                    owner, :, pl.ds((at * seqs + source) * units, units)
                ].astype(F32)
    fars = [
        push(far.at[dp], far.at[dp], far_s, far_r, at, {"dp": peer})
        for at, peer in enumerate(dp_peers)
    ]
    for at in range(2, dps // 2):
        line.step(at)
    line.end()
    for source in range(seqs):
        mine[source] = line.total((source,)).astype(mine.dtype)
    swaps = [
        push(mine.at[peer], landed.at[seq], swap_s, swap_r, at, {"seq": peer})
        for at, peer in enumerate(seq_peers)
    ]
    landed[seq] = mine[seq]
    for copy in fars:
        copy.wait()
    tiny_ref[...] = jnp.sum(far[...], axis=0)
    for copy in swaps:
        copy.wait()
    group = w_ref.shape[3] // 3
    for source in range(seqs):
        for third in range(3):
            qkv_ref[:, pl.ds(third * wide + source * group, group)] = landed[
                source, :, pl.ds(third * group, group)
            ].astype(F32)
    line.drain()


def close_all(ways, qkv_rows, attn_part, sums, inputs, gain, resid, both, tag):
    seqs, dps = ways
    part = qkv_rows.shape[0] // (seqs * dps)
    wide3 = qkv_rows.shape[1]
    rows, wide = inputs.shape
    dma = pltpu.SemaphoreType.DMA
    vmem = pl.BlockSpec(memory_space=pltpu.VMEM)
    return pl.pallas_call(
        functools.partial(closing, ways),
        out_shape=(
            jax.ShapeDtypeStruct((part, 3 * wide), F32),
            jax.ShapeDtypeStruct((rows, wide), BF16),
            jax.ShapeDtypeStruct(sums.shape, F32),
            jax.ShapeDtypeStruct((part, dps * both.shape[2] // 2), F32),
            jax.ShapeDtypeStruct((part, dps * both.shape[2] // 2), F32),
        ),
        in_specs=[vmem] * 7,
        out_specs=(vmem,) * 5,
        scratch_shapes=Plane.scratch(seqs, rows, wide, BF16)
        + LineSum.scratch(dps, (seqs, part, wide3), BF16)
        + [
            pltpu.VMEM((seqs, part, wide3), BF16),
            pltpu.VMEM((seqs, part, wide3), BF16),
            pltpu.VMEM((seqs,) + sums.shape, F32),
            pltpu.VMEM((dps,) + sums.shape, F32),
            pltpu.VMEM(sums.shape, F32),
            dma((seqs - 1,)),
            dma((seqs - 1,)),
            dma((seqs - 1,)),
            dma((seqs - 1,)),
            dma((dps - 1,)),
            dma((dps - 1,)),
        ],
        cost_estimate=lasting(75),
        compiler_params=pltpu.CompilerParams(collective_id=tag, has_side_effects=True),
    )(
        qkv_rows.reshape(seqs, dps, part, wide3),
        attn_part.reshape(seqs, rows, wide),
        sums,
        inputs,
        gain,
        resid,
        both,
    )


def opening(ways, qkv_ref, x_ref, small_ref, gate_ref, up_ref, w_ref, all_ref, given_ref, cut_ref, *sems):
    seqs, dps = ways
    chips, count = dps // 2, seqs * dps
    swap_s, swap_r, line_s, line_r, pair_s, pair_r, x_s, x_r, small_s, small_r, own_sem = sems
    seq, dp = lax.axis_index("seq"), lax.axis_index("dp")
    chip, core = dp // 2, lax.rem(dp, 2)
    me = seq * dps + dp
    part, group = qkv_ref.shape[0], w_ref.shape[1] // 3
    width = qkv_ref.shape[1] // 3
    barrier = pltpu.get_barrier_semaphore()

    def other(step):
        at = lax.rem(me + step, count)
        return {"seq": at // dps, "dp": lax.rem(at, dps)}

    @pl.loop(1, count)
    def _(step):
        pl.semaphore_signal(barrier, inc=1, device_id=other(step), device_id_type=MESH)

    pl.semaphore_wait(barrier, count - 1)

    def block(source, owner):
        return w_ref.at[pl.ds(pl.multiple_of((source * dps + owner) * part, part), part), :]

    def piece(source, third):
        rows = pl.ds(pl.multiple_of((source * dps + dp) * part, part), part)
        return w_ref.at[rows, pl.ds(third * group, group)]

    def columns(target, third):
        at = pl.multiple_of(third * width + target * group, 128)
        return qkv_ref.at[:, pl.ds(at, group)]

    swaps = []
    for step in range(1, seqs):
        target = lax.rem(seq + step, seqs)
        for third in range(3):
            at = 3 * (step - 1) + third
            swaps.append(
                remote(
                    columns(target, third),
                    piece(seq, third),
                    swap_s.at[at],
                    swap_r.at[at],
                    {"seq": target},
                )
            )
            swaps[-1].start()
    owns = [
        pltpu.make_async_copy(columns(seq, third), piece(seq, third), own_sem.at[third])
        for third in range(3)
    ]
    for own in owns:
        own.start()

    square = seqs == 4
    if square:
        _, across, along, _ = corners()
        to_across, to_along = {"seq": across}, {"seq": along}
        half = x_ref.shape[0] // 2
        top, low = pl.ds(0, half), pl.ds(half, half)
        copies = [
            push(x_ref.at[top], all_ref.at[seq, top], x_s, x_r, 0, to_across),
            push(x_ref.at[low], all_ref.at[seq, low], x_s, x_r, 1, to_along),
            push(x_ref.at[low], all_ref.at[seq, low], x_s, x_r, 2, to_across),
            push(x_ref.at[top], all_ref.at[seq, top], x_s, x_r, 3, to_along),
        ]
    else:
        copies = [
            push(x_ref, all_ref.at[seq], x_s, x_r, step - 1, {"seq": lax.rem(seq + step, seqs)})
            for step in range(1, seqs)
        ]
    owns.append(pltpu.make_async_copy(x_ref, all_ref.at[seq], own_sem.at[3]))
    owns[3].start()

    def small_copy(step):
        return remote(
            small_ref, given_ref.at[me], small_s.at[step - 1], small_r.at[step - 1], other(step)
        )

    @pl.loop(1, count)
    def _(step):
        small_copy(step).start()

    given_ref[me] = small_ref[...]

    units = gate_ref.shape[1] // count

    def cut_columns():
        for at, weight in enumerate((gate_ref, up_ref)):
            for source in range(seqs):
                for owner in range(dps):
                    cut_ref[owner, :, pl.ds((at * seqs + source) * units, units)] = weight[
                        :, pl.ds((source * dps + owner) * units, units)
                    ]

    sibling = {"dp": 2 * chip + (1 - core)}
    ends = (chip + 1 < chips, chip >= 1)
    sides = ({"dp": lax.rem(dp + 2, dps)}, {"dp": lax.rem(dp - 2 + dps, dps)})

    def onward(side, hop, source, owner_chip):
        part_of = block(source[1], 2 * owner_chip + core)
        at = (side, hop, source[0])
        return remote(part_of, part_of, line_s.at[at], line_r.at[at], sides[side])

    def share(source, owner_chip, owner_core):
        part_of = block(source[1], 2 * owner_chip + owner_core)
        at = (owner_chip, source[0])
        return remote(part_of, part_of, pair_s.at[at], pair_r.at[at], sibling)

    sources = [(back, lax.rem(seq - back + seqs, seqs)) for back in range(seqs)]
    for source in sources:
        if source[0] == 0:
            for own in owns[:3]:
                own.wait()
        else:
            for third in range(3):
                swaps[3 * (source[0] - 1) + third].wait_recv()
        for side in range(2):

            @pl.when(ends[side])
            def _(side=side, source=source):
                onward(side, 0, source, chip).start()

        share(source, chip, core).start()
    if square:
        copies[0].wait_recv()
        copies.append(push(all_ref.at[across, top], all_ref.at[across, top], x_s, x_r, 4, to_along))
        copies[1].wait_recv()
        copies.append(push(all_ref.at[along, low], all_ref.at[along, low], x_s, x_r, 5, to_across))
    cut_columns()
    for hop in range(chips - 1):
        for source in sources:
            for side in range(2):
                origin = chip - 1 - hop if side == 0 else chip + 1 + hop
                there = origin >= 0 if side == 0 else origin < chips

                @pl.when(there)
                def _(side=side, hop=hop, source=source, origin=origin):
                    onward(side, hop, source, origin).wait_recv()
                    share(source, origin, core).start()

                if hop < chips - 2:

                    @pl.when(jnp.logical_and(there, ends[side]))
                    def _(side=side, hop=hop, source=source, origin=origin):
                        onward(side, hop + 1, source, origin).start()

    for swapped in swaps:
        swapped.wait_send()
    for at, copy in enumerate(copies):
        copy.wait_send()
        if not square or at > 1:
            copy.wait_recv()
    owns[3].wait()

    @pl.loop(1, count)
    def _(step):
        small_copy(step).wait()

    for hop in range(chips - 1):
        for source in sources:
            for side in range(2):
                origin = chip - hop if side == 0 else chip + hop
                there = origin >= 0 if side == 0 else origin < chips

                @pl.when(jnp.logical_and(there, ends[side]))
                def _(side=side, hop=hop, source=source, origin=origin):
                    onward(side, hop, source, origin).wait_send()

    for owner in range(chips):
        for source in sources:
            share(source, owner, core).wait_send()
            share(source, owner, 1 - core).wait_recv()


def open_all(ways, qkv_weight, rows_in, small, gate_weight, up_weight):
    seqs, dps = ways
    chips, count = dps // 2, seqs * dps
    part, group = qkv_weight.shape[0], qkv_weight.shape[1] // (3 * seqs)
    slots = 6 if seqs == 4 else seqs - 1
    dma = pltpu.SemaphoreType.DMA
    return pl.pallas_call(
        functools.partial(opening, ways),
        out_shape=(
            jax.ShapeDtypeStruct((part * count, 3 * group), BF16),
            jax.ShapeDtypeStruct((seqs,) + rows_in.shape, BF16),
            jax.ShapeDtypeStruct((count,) + small.shape, BF16),
            jax.ShapeDtypeStruct((dps, part, 2 * gate_weight.shape[1] // dps), BF16),
        ),
        in_specs=[pl.BlockSpec(memory_space=pltpu.VMEM)] * 5,
        out_specs=(
            pl.BlockSpec(memory_space=pl.ANY),
            pl.BlockSpec(memory_space=pl.ANY),
            pl.BlockSpec(memory_space=pltpu.VMEM),
            pl.BlockSpec(memory_space=pltpu.VMEM),
        ),
        scratch_shapes=[
            dma((3 * (seqs - 1),)),
            dma((3 * (seqs - 1),)),
            dma((2, chips - 1, seqs)),
            dma((2, chips - 1, seqs)),
            dma((chips, seqs)),
            dma((chips, seqs)),
            dma((slots,)),
            dma((slots,)),
            dma((count - 1,)),
            dma((count - 1,)),
            dma((4,)),
        ],
        cost_estimate=lasting(75),
        compiler_params=pltpu.CompilerParams(collective_id=0, has_side_effects=True),
    )(qkv_weight, rows_in, small, gate_weight, up_weight)


def after(value, *earlier):
    return lax.optimization_barrier((value,) + earlier)[0]


def attention_forward(queries, keys, values):
    length = queries.shape[0]
    scale = HEAD_DIM ** (-0.5)
    index = jnp.arange(length, dtype=jnp.int32)
    allowed = index[None, :] <= index[:, None]
    scores = jnp.einsum("qhd,khd->hqk", queries, keys, preferred_element_type=F32) * scale
    scores = jnp.where(allowed[None], scores, -jnp.inf)
    largest = jnp.max(scores, axis=-1, keepdims=True)
    exponent = jnp.exp(scores - largest)
    totals = jnp.sum(exponent, axis=-1, keepdims=True)
    probs = exponent / totals
    mixed = jnp.einsum("hqk,khd->qhd", probs.astype(BF16), values, preferred_element_type=F32)
    return mixed.astype(BF16), (largest + jnp.log(totals))


def attention_backward(queries, keys, values, log_total, grad):
    length = queries.shape[0]
    scale = HEAD_DIM ** (-0.5)
    index = jnp.arange(length, dtype=jnp.int32)
    allowed = index[None, :] <= index[:, None]
    scores = jnp.einsum("qhd,khd->hqk", queries, keys, preferred_element_type=F32) * scale
    scores = jnp.where(allowed[None], scores, -jnp.inf)
    probs = jnp.exp(scores - log_total)
    values_grad = jnp.einsum("hqk,qhd->khd", probs.astype(BF16), grad, preferred_element_type=F32)
    probs_grad = jnp.einsum("qhd,khd->hqk", grad, values, preferred_element_type=F32)
    scores_grad = (
        probs * (probs_grad - jnp.sum(probs * probs_grad, axis=-1, keepdims=True))
    ).astype(BF16)
    query_grad = jnp.einsum("hqk,khd->qhd", scores_grad, keys, preferred_element_type=F32) * scale
    keys_grad = jnp.einsum("hqk,qhd->khd", scores_grad, queries, preferred_element_type=F32) * scale
    return query_grad.astype(BF16), keys_grad.astype(BF16), values_grad.astype(BF16)


def shards(
    ways,
    inputs,
    first_gain,
    first_shift,
    qkv_weight,
    qkv_bias,
    out_weight,
    second_gain,
    second_shift,
    gate_weight,
    up_weight,
    down_weight,
    out_cotangent,
):
    seqs, dps = ways
    width = inputs.shape[2]
    rows = inputs.shape[1]
    length = rows * seqs
    part = width // (seqs * dps)
    units = down_weight.shape[0]
    group = width // seqs
    heads = group // HEAD_DIM
    me_seq = lax.axis_index("seq")
    grad_out = out_cotangent[0]

    small = jnp.concatenate([first_gain, first_shift, second_gain, second_shift, qkv_bias])
    total = small.shape[0]
    padded = -(-total // 2048) * 2048
    small = jnp.pad(small, (0, padded - total)).reshape(padded // 128, 128)
    qkv_full, inputs_all, small, gate_cut = open_all(
        ways, qkv_weight, inputs[0], small, gate_weight, up_weight
    )
    small = small.reshape(seqs * dps, padded)[:, :total].astype(F32)
    gain_one = small[:, :part].reshape(-1)
    shift_one = small[:, part : 2 * part].reshape(-1)
    gain_two = small[:, 2 * part : 3 * part].reshape(-1)
    shift_two = small[:, 3 * part : 4 * part].reshape(-1)
    bias = small[:, 4 * part :].reshape(3, seqs, group)
    bias = lax.dynamic_index_in_dim(bias, me_seq, 1, keepdims=False).reshape(3 * group)

    down_full = gather(down_weight, "seq")
    out_full = gather(out_weight, "dp")

    gate_cut = gate_cut.reshape(dps * part, 2 * seqs * units)
    moved = move_blocks(gate_cut, "dp", dps)
    wide = seqs * units

    normed_all, _ = normalize(inputs_all.reshape(length, width).astype(F32))
    attn_all = (normed_all * gain_one + shift_one).astype(BF16)
    projected = dot(attn_all, qkv_full) + bias
    cosine, sine = tables(jnp.arange(length, dtype=jnp.int32).astype(F32))

    def to_heads(flat):
        return flat.reshape(length, heads, HEAD_DIM)

    queries = rotate(to_heads(projected[:, :group]), cosine, sine).astype(BF16)
    keys = rotate(to_heads(projected[:, group : 2 * group]), cosine, sine).astype(BF16)
    values = to_heads(projected[:, 2 * group :]).astype(BF16)
    attended, log_total = attention_forward(queries, keys, values)
    attended = attended.reshape(length, group)
    moved, attended = lax.optimization_barrier((moved, attended))
    gate_cut = place_blocks(moved, "dp")
    branch = dot(attended, out_full).astype(BF16)
    residual, mlp_all, grad_all, gate_up = middle_all(
        ways, branch, inputs[0], gain_two[None], shift_two[None], grad_out, gate_cut, 1
    )

    both = dot(mlp_all, gate_up)
    gate_value = both[:, :wide]
    up_value = both[:, wide:]
    sigmoid_gate = jax.nn.sigmoid(gate_value)
    activated = gate_value * sigmoid_gate
    hidden = (activated * up_value).astype(BF16)
    out_part = dot(hidden, down_full).astype(BF16)

    hidden_grad = contract_cols(grad_all, down_full)
    gate_grad = (
        hidden_grad * up_value * (sigmoid_gate * (1.0 + gate_value * (1.0 - sigmoid_gate)))
    ).astype(BF16)
    up_grad = (hidden_grad * activated).astype(BF16)
    both_grad = jnp.concatenate([gate_grad, up_grad], 1)
    mlp_part = contract_cols(both_grad, gate_up).astype(BF16)
    both_rows = contract_rows(mlp_all, after(both_grad, mlp_part)).astype(BF16)
    down_rows = contract_rows(hidden, grad_all).astype(BF16)
    mlp_part = after(mlp_part, both_rows, down_rows)
    residual_grad, branch_all, sums, layer_out, both_rows = turn_all(
        ways, mlp_part, residual, gain_two[None], grad_out, out_part, both_rows, 2
    )
    down_rows = after(down_rows, residual_grad)
    down_shard = scatter_sum(down_rows, "seq").astype(F32)
    both_rows = swap(both_rows, "dp", 0, 0)
    both_rows = both_rows.reshape(dps, part, 2 * seqs * units)

    attended_grad = contract_cols(branch_all, out_full).astype(BF16)
    out_rows = contract_rows(attended, after(branch_all, attended_grad)).astype(BF16)
    out_shard = scatter_sum(out_rows, "dp").astype(F32)
    query_grad, keys_grad, values_grad = attention_backward(
        queries, keys, values, log_total, to_heads(attended_grad)
    )
    query_plain = rotate(query_grad.astype(F32), cosine, -sine).astype(BF16)
    keys_plain = rotate(keys_grad.astype(F32), cosine, -sine).astype(BF16)
    projected_grad = jnp.concatenate(
        [item.reshape(length, group) for item in (query_plain, keys_plain, values_grad)], 1
    )
    attn_part = contract_cols(projected_grad, qkv_full).astype(BF16)
    qkv_rows = contract_rows(attn_all, projected_grad).astype(BF16)
    bias_term = jnp.sum(projected_grad.astype(F32), axis=0).reshape(3, 1, group)
    here = (jnp.arange(seqs, dtype=jnp.int32) == me_seq).astype(F32)[None, :, None]
    bias_term = jnp.pad((bias_term * here).reshape(3, width), ((4, 1), (0, 0)))
    sums = sums + bias_term
    qkv_shard, input_grad, tiny, gate_shard, up_shard = close_all(
        ways,
        qkv_rows,
        attn_part,
        sums,
        inputs[0],
        gain_one[None],
        residual_grad,
        both_rows,
        3,
    )
    me = me_seq * dps + lax.axis_index("dp")
    mine = lax.dynamic_slice_in_dim(tiny, me * part, part, 1)
    bias_shard = lax.dynamic_slice_in_dim(tiny[4:7].reshape(-1), me * 3 * part, 3 * part, 0)

    return (
        layer_out[None],
        input_grad[None],
        mine[0],
        mine[1],
        qkv_shard,
        bias_shard,
        out_shard,
        mine[2],
        mine[3],
        gate_shard,
        up_shard,
        down_shard,
    )


def solution(mesh):
    split = ("seq", "dp")
    tokens = P("dp", "seq", None)
    in_specs = (
        tokens,
        P(split),
        P(split),
        P(split, None),
        P(split),
        P(split, None),
        P(split),
        P(split),
        P(split, None),
        P(split, None),
        P(split, None),
        tokens,
    )
    out_specs = (
        tokens,
        tokens,
        P(split),
        P(split),
        P(split, None),
        P(split),
        P(split, None),
        P(split),
        P(split),
        P(split, None),
        P(split, None),
        P(split, None),
    )
    ways = (mesh.shape["seq"], mesh.shape["dp"])

    def local(*args):
        return shards(ways, *args)

    return jax.shard_map(local, mesh=mesh, in_specs=in_specs, out_specs=out_specs, check_vma=False)
```

```python
import functools

import jax
import jax.numpy as jnp
from jax import lax
from jax.experimental import pallas as pl
from jax.experimental.pallas import tpu as pltpu
from jax.sharding import PartitionSpec as P


HEAD_DIM = 64
ROT = 16
F32 = jnp.float32
BF16 = jnp.bfloat16


def normalize(values):
    center = values - jnp.mean(values, axis=-1, keepdims=True)
    variance = jnp.mean(center * center, axis=-1, keepdims=True)
    inverse = lax.rsqrt(variance + 1e-05)
    return (center * inverse, inverse)


def norm_back(grad_normed, normed, inverse, gain):
    scaled = grad_normed * gain
    centered = scaled - jnp.mean(scaled, axis=-1, keepdims=True)
    return inverse * (centered - normed * jnp.mean(scaled * normed, axis=-1, keepdims=True))


def dot(left, right):
    return jnp.dot(left, right, preferred_element_type=F32)


def contract_rows(left, right):
    return lax.dot_general(left, right, (((0,), (0,)), ((), ())), preferred_element_type=F32)


def contract_cols(left, right):
    return lax.dot_general(left, right, (((1,), (1,)), ((), ())), preferred_element_type=F32)


def tables(length):
    half_rot = ROT // 2
    lane = lax.rem(lax.broadcasted_iota(jnp.int32, (length, 128), 1), HEAD_DIM)
    position = lax.broadcasted_iota(jnp.int32, (length, 128), 0).astype(F32)
    freqs = 10000.0 ** (-(2.0 * lax.rem(lane, half_rot).astype(F32)) / ROT)
    angles = position * freqs
    cosine, sine = jnp.cos(angles), jnp.sin(angles)
    return jnp.stack(
        [
            jnp.where(lane < ROT, cosine, 1.0),
            jnp.where(lane < half_rot, -sine, 0.0),
            jnp.where((lane >= half_rot) & (lane < ROT), sine, 0.0),
        ]
    )


def turn_lanes(value, table_ref, sign):
    half_rot = ROT // 2
    ahead, behind = pltpu.roll(value, 128 - half_rot, 1), pltpu.roll(value, half_rot, 1)
    return value * table_ref[0] + sign * (ahead * table_ref[1] + behind * table_ref[2])


def gather(value, axis):
    return lax.all_gather(value, axis, axis=0, tiled=True)


def scatter_sum(value, axis):
    return lax.psum_scatter(value, axis, scatter_dimension=0, tiled=True)


MESH = pl.DeviceIdType.MESH


def lasting(micros):
    return pl.CostEstimate(flops=0, transcendentals=0, bytes_accessed=int(micros * 3.0e6))


def meet(peers):
    barrier = pltpu.get_barrier_semaphore()
    for peer in peers:
        pl.semaphore_signal(barrier, inc=1, device_id=peer, device_id_type=MESH)
    pl.semaphore_wait(barrier, len(peers))


def push(source, target, send, recv, at, peer):
    copy = pltpu.make_async_remote_copy(
        src_ref=source,
        dst_ref=target,
        send_sem=send.at[at],
        recv_sem=recv.at[at],
        device_id=peer,
        device_id_type=MESH,
    )
    copy.start()
    return copy


def corners():
    me = lax.axis_index("seq")
    high, low = me // 2, lax.rem(me, 2)
    across = high * 2 + (1 - low)
    along = (1 - high) * 2 + low
    return me, across, along, 3 - me


def remote(source, target, send, recv, peer):
    return pltpu.make_async_remote_copy(
        src_ref=source,
        dst_ref=target,
        send_sem=send,
        recv_sem=recv,
        device_id=peer,
        device_id_type=MESH,
    )


def line_place(dps):
    dp = lax.axis_index("dp")
    chip, core = dp // 2, lax.rem(dp, 2)
    chips = dps // 2
    ends = (chip + 1 < chips, chip >= 1)
    sides = ({"dp": lax.rem(dp + 2, dps)}, {"dp": lax.rem(dp - 2 + dps, dps)})
    return chips, chip, core, ends, sides, {"dp": 2 * chip + (1 - core)}


class Plane:

    def __init__(self, count, x_ref, pair, got, send, recv):
        self.count, self.x, self.pair, self.got = count, x_ref, pair, got
        self.send, self.recv = send, recv
        self.square = count == 4

    def begin(self):
        x, got, send, recv = self.x, self.got, self.send, self.recv
        if not self.square:
            me = lax.axis_index("seq")
            targets = [lax.rem(me + step, self.count) for step in range(1, self.count)]
            self.copies = [
                push(x.at[target], got.at[at], send, recv, at, {"seq": target})
                for at, target in enumerate(targets)
            ]
            return
        _, across, along, far = corners()
        half = x.shape[1] // 2
        top, low = pl.ds(0, half), pl.ds(half, half)
        to_across, to_along = {"seq": across}, {"seq": along}
        self.copies = [
            push(x.at[far, top], self.pair.at[0], send, recv, 0, to_across),
            push(x.at[far, low], self.pair.at[1], send, recv, 1, to_along),
            push(x.at[across, top], got.at[0, top], send, recv, 2, to_across),
            push(x.at[along, low], got.at[1, low], send, recv, 3, to_along),
        ]

    def relay(self):
        if not self.square:
            return
        x, pair, got, send, recv = self.x, self.pair, self.got, self.send, self.recv
        _, across, along, _ = corners()
        half = x.shape[1] // 2
        top, low = pl.ds(0, half), pl.ds(half, half)
        self.copies[0].wait_recv()
        pair[2] = (pair[0].astype(F32) + x[along, top].astype(F32)).astype(pair.dtype)
        self.copies.append(push(pair.at[2], got.at[1, top], send, recv, 4, {"seq": along}))
        self.copies[1].wait_recv()
        pair[3] = (pair[1].astype(F32) + x[across, low].astype(F32)).astype(pair.dtype)
        self.copies.append(push(pair.at[3], got.at[0, low], send, recv, 5, {"seq": across}))

    def end(self):
        for at, copy in enumerate(self.copies):
            copy.wait_send()
            if not self.square or at > 1:
                copy.wait_recv()

    def total(self, rows):
        value = self.x[lax.axis_index("seq"), rows].astype(F32)
        for at in range(2 if self.square else self.count - 1):
            value = value + self.got[at, rows].astype(F32)
        return value

    @staticmethod
    def scratch(count, rows, wide, dtype):
        slots = 6 if count == 4 else count - 1
        return [
            pltpu.VMEM((4, rows // 2, wide), dtype),
            pltpu.VMEM((2 if count == 4 else count - 1, rows, wide), dtype),
            pltpu.SemaphoreType.DMA((slots,)),
            pltpu.SemaphoreType.DMA((slots,)),
        ]


class LineSum:

    def __init__(self, dps, block, pair, moving, line_s, line_r, pair_s, pair_r):
        self.block, self.pair, self.moving = block, pair, moving
        self.sems = (line_s, line_r, pair_s, pair_r)
        self.chips, self.chip, self.core, self.ends, self.sides, self.sibling = line_place(dps)
        self.pieces = pair.shape[1]

    def share(self, owner, owner_core, piece):
        at = (owner, piece)
        return remote(
            self.block(2 * owner + owner_core).at[piece],
            self.pair.at[at],
            self.sems[2].at[at],
            self.sems[3].at[at],
            self.sibling,
        )

    def onward(self, side, owner, piece):
        at = (side, owner, piece)
        return remote(
            self.pair.at[owner, piece],
            self.moving.at[at],
            self.sems[0].at[at],
            self.sems[1].at[at],
            self.sides[side],
        )

    def begin(self):
        order = [
            at for both in zip(range(self.chips - 1, -1, -1), range(self.chips)) for at in both
        ]
        for owner in dict.fromkeys(order):
            for piece in range(self.pieces):
                self.share(owner, 1 - self.core, piece).start()

    def add(self, owner, piece, side):
        own = self.block(2 * owner + self.core)

        def one(here):
            value = self.pair[owner, piece, here].astype(F32) + own[piece, here].astype(F32)
            if side is not None:
                value = value + self.moving[side, owner, piece, here].astype(F32)
            self.pair[owner, piece, here] = value.astype(self.pair.dtype)

        by_chunks(self.pair.shape[2], one)

    def step(self, at):
        for piece in range(self.pieces):
            for side in range(2):
                owner = self.chips - 1 - at if side == 0 else at
                passing = self.chip < owner if side == 0 else self.chip > owner
                fed = jnp.logical_and(passing, self.ends[1 - side])

                @pl.when(passing)
                def _(owner=owner, piece=piece):
                    self.share(owner, self.core, piece).wait_recv()

                @pl.when(fed)
                def _(side=side, owner=owner, piece=piece):
                    self.onward(side, owner, piece).wait_recv()
                    self.add(owner, piece, side)

                @pl.when(jnp.logical_and(passing, jnp.logical_not(fed)))
                def _(owner=owner, piece=piece):
                    self.add(owner, piece, None)

                @pl.when(passing)
                def _(side=side, owner=owner, piece=piece):
                    self.onward(side, owner, piece).start()

    def end(self):
        for owner in range(self.chips):
            for piece in range(self.pieces):

                @pl.when(self.chip == owner)
                def _(owner=owner, piece=piece):
                    self.share(owner, self.core, piece).wait_recv()

                for side in range(2):

                    @pl.when(jnp.logical_and(self.chip == owner, self.ends[1 - side]))
                    def _(side=side, owner=owner, piece=piece):
                        self.onward(side, owner, piece).wait_recv()

        for side in range(2):

            @pl.when(jnp.logical_not(self.ends[1 - side]))
            def _(side=side):
                self.moving[side, self.chip] = jnp.zeros(self.moving.shape[2:], self.moving.dtype)

    def total(self, piece, here):
        own = self.block(2 * self.chip + self.core)
        value = own[piece, here].astype(F32) + self.pair[self.chip, piece, here].astype(F32)
        for side in range(2):
            value = value + self.moving[side, self.chip, piece, here].astype(F32)
        return value

    def drain(self):
        for owner in range(self.chips):
            for piece in range(self.pieces):
                for side in range(2):
                    passing = self.chip < owner if side == 0 else self.chip > owner

                    @pl.when(passing)
                    def _(side=side, owner=owner, piece=piece):
                        self.onward(side, owner, piece).wait_send()

                self.share(owner, 1 - self.core, piece).wait_send()

    @staticmethod
    def scratch(dps, shape, dtype):
        dma, chips, pieces = pltpu.SemaphoreType.DMA, dps // 2, shape[0]
        return [
            pltpu.VMEM((chips,) + shape, dtype),
            pltpu.VMEM((2, chips) + shape, dtype),
            dma((2, chips, pieces)),
            dma((2, chips, pieces)),
            dma((chips, pieces)),
            dma((chips, pieces)),
        ]


class PlaneGather:

    def __init__(self, count, x_ref, o_ref, send, recv, local):
        self.count, self.x, self.o = count, x_ref, o_ref
        self.send, self.recv, self.local = send, recv, local
        self.square = count == 4

    def begin(self):
        x, o, send, recv = self.x, self.o, self.send, self.recv
        me = lax.axis_index("seq")
        if self.square:
            _, across, along, _ = corners()
            half = x.shape[0] // 2
            top, low = pl.ds(0, half), pl.ds(half, half)
            to_across, to_along = {"seq": across}, {"seq": along}
            self.copies = [
                push(x.at[top], o.at[me, top], send, recv, 0, to_across),
                push(x.at[low], o.at[me, low], send, recv, 1, to_along),
                push(x.at[low], o.at[me, low], send, recv, 2, to_across),
                push(x.at[top], o.at[me, top], send, recv, 3, to_along),
            ]
        else:
            self.copies = [
                push(x, o.at[me], send, recv, step - 1, {"seq": lax.rem(me + step, self.count)})
                for step in range(1, self.count)
            ]
        self.own = pltpu.make_async_copy(x, o.at[me], self.local)
        self.own.start()

    def relay(self):
        if not self.square:
            return
        o, send, recv = self.o, self.send, self.recv
        _, across, along, _ = corners()
        half = self.x.shape[0] // 2
        top, low = pl.ds(0, half), pl.ds(half, half)
        self.copies[0].wait_recv()
        self.copies.append(
            push(o.at[across, top], o.at[across, top], send, recv, 4, {"seq": along})
        )
        self.copies[1].wait_recv()
        self.copies.append(
            push(o.at[along, low], o.at[along, low], send, recv, 5, {"seq": across})
        )

    def end(self):
        for at, copy in enumerate(self.copies):
            copy.wait_send()
            if not self.square or at > 1:
                copy.wait_recv()
        self.own.wait()

    @staticmethod
    def scratch(count):
        slots = 6 if count == 4 else count - 1
        dma = pltpu.SemaphoreType.DMA
        return [dma((slots,)), dma((slots,)), dma]


class LineGather:

    def __init__(self, dps, x_ref, o_ref, line_s, line_r, pair_s, pair_r, local):
        self.x, self.o, self.local = x_ref, o_ref, local
        self.sems = (line_s, line_r, pair_s, pair_r)
        self.chips, self.chip, self.core, self.ends, self.sides, self.sibling = line_place(dps)

    def onward(self, side, hop, owner, source=None):
        block = self.o.at[2 * owner + self.core]
        at = (side, hop)
        return remote(
            block if source is None else source,
            block,
            self.sems[0].at[at],
            self.sems[1].at[at],
            self.sides[side],
        )

    def share(self, owner, owner_core, source=None):
        block = self.o.at[2 * owner + owner_core]
        return remote(
            block if source is None else source,
            block,
            self.sems[2].at[owner],
            self.sems[3].at[owner],
            self.sibling,
        )

    def begin(self):
        for side in range(2):

            @pl.when(self.ends[side])
            def _(side=side):
                self.onward(side, 0, self.chip, self.x).start()

        self.share(self.chip, self.core, self.x).start()
        self.own = pltpu.make_async_copy(
            self.x, self.o.at[2 * self.chip + self.core], self.local
        )
        self.own.start()

    def hop(self, hop):
        for side in range(2):
            origin = self.chip - 1 - hop if side == 0 else self.chip + 1 + hop
            there = origin >= 0 if side == 0 else origin < self.chips

            @pl.when(there)
            def _(side=side, origin=origin):
                self.onward(side, hop, origin).wait_recv()

            if hop < self.chips - 2:

                @pl.when(jnp.logical_and(there, self.ends[side]))
                def _(side=side, origin=origin):
                    self.onward(side, hop + 1, origin).start()

            @pl.when(there)
            def _(origin=origin):
                self.share(origin, self.core).start()

    def end(self):
        self.own.wait()
        for hop in range(self.chips - 1):
            for side in range(2):
                origin = self.chip - hop if side == 0 else self.chip + hop
                there = origin >= 0 if side == 0 else origin < self.chips

                @pl.when(jnp.logical_and(there, self.ends[side]))
                def _(side=side, hop=hop, origin=origin):
                    self.onward(side, hop, origin).wait_send()

        for owner in range(self.chips):
            self.share(owner, self.core).wait_send()
            self.share(owner, 1 - self.core).wait_recv()

    @staticmethod
    def scratch(dps):
        dma, chips = pltpu.SemaphoreType.DMA, dps // 2
        return [dma((2, chips - 1)), dma((2, chips - 1)), dma((chips,)), dma((chips,)), dma]


CHUNK = 16


def by_chunks(rows, body):
    @pl.loop(0, rows // CHUNK)
    def _(at):
        body(pl.ds(pl.multiple_of(at * CHUNK, CHUNK), CHUNK))


PIECES = 2


def by_pieces(rows, body):
    size = rows // PIECES
    for piece in range(PIECES):

        @pl.loop(0, size // CHUNK)
        def _(at, piece=piece):
            here = pl.multiple_of(at * CHUNK, CHUNK)
            body(pl.ds(pl.multiple_of(piece * size + here, CHUNK), CHUNK), piece, pl.ds(here, CHUNK))


def meet_cross(ways):
    seqs, dps = ways
    seq, dp = lax.axis_index("seq"), lax.axis_index("dp")
    seq_peers = [lax.rem(seq + step, seqs) for step in range(1, seqs)]
    dp_peers = [lax.rem(dp + step, dps) for step in range(1, dps)]
    meet([{"seq": peer} for peer in seq_peers] + [{"dp": peer} for peer in dp_peers])
    return seq_peers, dp_peers


def turning(ways, part_ref, resid_ref, gain_ref, grad_ref, out_ref, both_ref, *rest):
    seqs, dps = ways
    total_ref, all_ref, sums_ref, layer_ref, rows_ref = rest[:5]
    line = LineSum(dps, lambda owner: part_ref.at[owner], *rest[5:11])
    own = rest[11]
    gathered = PlaneGather(seqs, own, all_ref, *rest[12:15])
    outs = LineSum(dps, lambda owner: out_ref.at[owner], *rest[15:21])
    both = Plane(seqs, both_ref, *rest[21:25])
    chips = dps // 2
    meet_cross(ways)
    line.begin()
    both.begin()
    line.step(0)
    both.relay()
    outs.begin()
    for at in range(1, chips):
        line.step(at)
    outs.step(0)
    line.end()
    sums_ref[...] = jnp.zeros(sums_ref.shape, F32)
    gain = gain_ref[...]

    def one(here, piece, inner):
        grad = line.total(piece, inner)
        normed, inverse = normalize(resid_ref[here, :])
        sums_ref[2:3, :] += jnp.sum(grad * normed, axis=0, keepdims=True)
        sums_ref[3:4, :] += jnp.sum(grad, axis=0, keepdims=True)
        total = grad_ref[here, :].astype(F32) + norm_back(grad, normed, inverse, gain)
        total_ref[here, :] = total
        own[here, :] = total.astype(own.dtype)

    by_pieces(resid_ref.shape[0], one)
    gathered.begin()
    if chips > 1:
        outs.step(1)
    gathered.relay()
    for at in range(2, chips):
        outs.step(at)
    both.end()

    def two(here):
        rows_ref[here, :] = both.total(here).astype(rows_ref.dtype)

    by_chunks(rows_ref.shape[0], two)
    gathered.end()
    outs.end()

    def three(here, piece, inner):
        layer_ref[here, :] = (resid_ref[here, :] + outs.total(piece, inner)).astype(layer_ref.dtype)

    by_pieces(resid_ref.shape[0], three)
    line.drain()
    outs.drain()


def turn_all(ways, part, resid, gain, grad_out, out_part, both, tag):
    seqs, dps = ways
    rows, wide = resid.shape
    cut = (both.shape[0] // seqs, both.shape[1])
    vmem, anywhere = (pl.BlockSpec(memory_space=space) for space in (pltpu.VMEM, pl.ANY))
    total, gathered, sums, layer, both = pl.pallas_call(
        functools.partial(turning, ways),
        out_shape=(
            jax.ShapeDtypeStruct((rows, wide), F32),
            jax.ShapeDtypeStruct((seqs, rows, wide), BF16),
            jax.ShapeDtypeStruct((8, wide), F32),
            jax.ShapeDtypeStruct((rows, wide), BF16),
            jax.ShapeDtypeStruct(cut, BF16),
        ),
        in_specs=[vmem] * 6,
        out_specs=(vmem, anywhere, vmem, vmem, vmem),
        scratch_shapes=LineSum.scratch(dps, (PIECES, rows // PIECES, wide), BF16)
        + [pltpu.VMEM((rows, wide), BF16)]
        + PlaneGather.scratch(seqs)
        + LineSum.scratch(dps, (PIECES, rows // PIECES, wide), BF16)
        + Plane.scratch(seqs, cut[0], cut[1], BF16),
        cost_estimate=lasting(85),
        compiler_params=pltpu.CompilerParams(
            collective_id=tag, has_side_effects=True, vmem_limit_bytes=60 * 2**20
        ),
    )(
        part.reshape(dps, PIECES, rows // PIECES, wide),
        resid,
        gain,
        grad_out,
        out_part.reshape(dps, PIECES, rows // PIECES, wide),
        both.reshape((seqs,) + cut),
    )
    return total, gathered.reshape(seqs * rows, wide), sums, layer, both


class SwapDp:

    def __init__(self, dps, x_ref, o_ref, send, recv, local):
        dp = lax.axis_index("dp")
        self.peers = [lax.rem(dp + step, dps) for step in range(1, dps)]
        self.parts = (x_ref, o_ref, send, recv, local, dp)

    def begin(self):
        x, o, send, recv, local, dp = self.parts
        self.copies = [
            push(x.at[peer], o.at[dp], send, recv, at, {"dp": peer})
            for at, peer in enumerate(self.peers)
        ]
        self.own = pltpu.make_async_copy(x.at[dp], o.at[dp], local)
        self.own.start()

    def end(self):
        for copy in self.copies:
            copy.wait()
        self.own.wait()

    @staticmethod
    def scratch(dps):
        dma = pltpu.SemaphoreType.DMA
        return [dma((dps - 1,)), dma((dps - 1,)), dma]


def halves():
    lane = lax.broadcasted_iota(jnp.int32, (1, 128), 1)
    return lane, (lane < HEAD_DIM, lane >= HEAD_DIM)


def reversing(
    ways, grads_ref, out_ref, qkv_ref, lse_ref, table_ref, w_ref, attn_ref, att_ref, both_ref, *rest
):
    dps = ways[1]
    part_ref, rows_ref, bias_ref, outs_ref, swapped_ref = rest[:5]
    swap = SwapDp(dps, both_ref, swapped_ref, *rest[5:8])
    pg_ref, grad_ref = rest[8:10]
    dp = lax.axis_index("dp")
    meet([{"dp": lax.rem(dp + step, dps)} for step in range(1, dps)])
    swap.begin()
    length, wide = grads_ref.shape
    group = out_ref.shape[0]
    scale = HEAD_DIM ** (-0.5)
    size = min(256, length)
    tile = min(256, group)

    @pl.loop(0, group // tile)
    def _(at):
        columns = pl.ds(pl.multiple_of(at * tile, tile), tile)
        grad_ref[:, columns] = contract_cols(grads_ref[...], out_ref[columns, :]).astype(
            grad_ref.dtype
        )

    _, sides = halves()
    triangle = lax.broadcasted_iota(jnp.int32, (size, size), 0) <= lax.broadcasted_iota(
        jnp.int32, (size, size), 1
    )

    @pl.loop(0, group // 128)
    def _(at):
        base = pl.multiple_of(at * 128, 128)
        query_lanes, key_lanes, value_lanes = (
            pl.ds(third * group + base, 128) for third in range(3)
        )
        key_sums = [[None] * (length // size) for _ in range(2)]
        value_sums = [[None] * (length // size) for _ in range(2)]
        for block in range(length // size):
            rows = pl.ds(block * size, size)
            seen = (block + 1) * size
            query = qkv_ref[rows, query_lanes]
            key = qkv_ref[pl.ds(0, seen), key_lanes]
            value = qkv_ref[pl.ds(0, seen), value_lanes]
            grad = grad_ref[rows, pl.ds(base, 128)]
            query_sums = []
            for half in range(2):
                mine = jnp.where(sides[half], query, jnp.zeros_like(query))
                given = jnp.where(sides[half], grad, jnp.zeros_like(grad))
                scores = contract_cols(key, mine) * scale
                total = lse_ref[pl.ds(2 * at + half, 1), rows]
                probs = jnp.exp(scores - total)
                last = jnp.where(triangle, probs[block * size :], 0.0)
                probs = jnp.concatenate([probs[: block * size], last], 0) if block else last
                probs_grad = contract_cols(value, given)
                tilt = jnp.sum(probs * probs_grad, axis=0, keepdims=True)
                scores_grad = (probs * (probs_grad - tilt)).astype(BF16)
                probs_low = probs.astype(BF16)
                query_sums.append(contract_rows(scores_grad, key))
                for part in range(block + 1):
                    cut = slice(part * size, (part + 1) * size)
                    for sums, left, right in (
                        (key_sums, scores_grad, query),
                        (value_sums, probs_low, grad),
                    ):
                        more = dot(left[cut], right)
                        held = sums[half][part]
                        sums[half][part] = more if held is None else held + more
            total = (jnp.where(sides[0], query_sums[0], query_sums[1]) * scale).astype(BF16)
            table = table_ref.at[:, rows]
            pg_ref[rows, query_lanes] = turn_lanes(total.astype(F32), table, -1.0).astype(BF16)
        for part in range(length // size):
            rows = pl.ds(part * size, size)
            total = jnp.where(sides[0], key_sums[0][part], key_sums[1][part]) * scale
            table = table_ref.at[:, rows]
            total = total.astype(BF16).astype(F32)
            pg_ref[rows, key_lanes] = turn_lanes(total, table, -1.0).astype(BF16)
            total = jnp.where(sides[0], value_sums[0][part], value_sums[1][part])
            pg_ref[rows, value_lanes] = total.astype(BF16)

    bias_ref[...] = jnp.zeros(bias_ref.shape, F32)

    @pl.loop(0, length // CHUNK)
    def _(at):
        here = pl.ds(pl.multiple_of(at * CHUNK, CHUNK), CHUNK)
        bias_ref[0:1, :] += jnp.sum(pg_ref[here, :].astype(F32), axis=0, keepdims=True)

    step = min(256, wide)

    @pl.loop(0, wide // step)
    def _(at):
        columns = pl.ds(pl.multiple_of(at * step, step), step)
        part_ref[:, columns] = contract_cols(pg_ref[...], w_ref[columns, :]).astype(part_ref.dtype)
        rows_ref[columns, :] = contract_rows(attn_ref[:, columns], pg_ref[...]).astype(
            rows_ref.dtype
        )
        outs_ref[:, columns] = contract_rows(att_ref[...], grads_ref[:, columns]).astype(
            outs_ref.dtype
        )

    swap.end()


def reverse_all(ways, grads, out_full, qkv, lse, table, qkv_full, attn_all, attended, both, tag):
    length, wide = grads.shape
    group = out_full.shape[0]
    vmem, anywhere = (pl.BlockSpec(memory_space=space) for space in (pltpu.VMEM, pl.ANY))
    return pl.pallas_call(
        functools.partial(reversing, ways),
        out_shape=(
            jax.ShapeDtypeStruct((length, wide), BF16),
            jax.ShapeDtypeStruct((wide, 3 * group), BF16),
            jax.ShapeDtypeStruct((8, 3 * group), F32),
            jax.ShapeDtypeStruct((group, wide), BF16),
            jax.ShapeDtypeStruct(both.shape, BF16),
        ),
        in_specs=[vmem] * 9,
        out_specs=(vmem,) * 4 + (anywhere,),
        scratch_shapes=SwapDp.scratch(ways[1])
        + [pltpu.VMEM((length, 3 * group), BF16), pltpu.VMEM((length, group), BF16)],
        cost_estimate=lasting(45),
        compiler_params=pltpu.CompilerParams(
            collective_id=tag, has_side_effects=True, vmem_limit_bytes=60 * 2**20
        ),
    )(grads, out_full, qkv, lse, table, qkv_full, attn_all, attended, both)


def closing(ways, w_ref, g_ref, sums_ref, x_ref, gain_ref, resid_ref, both_ref, *rest):
    seqs, dps = ways
    qkv_ref, grad_ref, tiny_ref, gate_ref, up_ref = rest[:5]
    plane = Plane(seqs, g_ref, *rest[5:9])
    line = LineSum(dps, lambda owner: w_ref.at[:, owner], *rest[9:15])
    landed, mine, near, far, part_sum = rest[15:20]
    swap_s, swap_r, near_s, near_r, far_s, far_r = rest[20:]
    seq, dp = lax.axis_index("seq"), lax.axis_index("dp")
    seq_peers, dp_peers = meet_cross(ways)
    line.begin()
    plane.begin()
    plane.relay()
    line.step(0)
    plane.end()
    part_sum[...] = sums_ref[...]
    gain = gain_ref[...]

    def one(here):
        grad = plane.total(here)
        normed, inverse = normalize(x_ref[here, :].astype(F32))
        part_sum[0:1, :] += jnp.sum(grad * normed, axis=0, keepdims=True)
        part_sum[1:2, :] += jnp.sum(grad, axis=0, keepdims=True)
        grad_ref[here, :] = (
            resid_ref[here, :] + norm_back(grad, normed, inverse, gain)
        ).astype(grad_ref.dtype)

    by_chunks(x_ref.shape[0], one)
    wide = x_ref.shape[1]
    nears = [
        push(part_sum, near.at[seq], near_s, near_r, at, {"seq": peer})
        for at, peer in enumerate(seq_peers)
    ]
    near[seq] = part_sum[...]
    line.step(1)
    for copy in nears:
        copy.wait()
    far[dp] = jnp.sum(near[...], axis=0)
    units = gate_ref.shape[1] // (seqs * dps)
    for at, weight in enumerate((gate_ref, up_ref)):
        for source in range(seqs):
            for owner in range(dps):
                weight[:, pl.ds((source * dps + owner) * units, units)] = both_ref[
                    owner, :, pl.ds((at * seqs + source) * units, units)
                ].astype(F32)
    fars = [
        push(far.at[dp], far.at[dp], far_s, far_r, at, {"dp": peer})
        for at, peer in enumerate(dp_peers)
    ]
    for at in range(2, dps // 2):
        line.step(at)
    line.end()
    for source in range(seqs):

        def three(here, source=source):
            mine[source, here] = line.total(source, here).astype(mine.dtype)

        by_chunks(mine.shape[1], three)
    swaps = [
        push(mine.at[peer], landed.at[seq], swap_s, swap_r, at, {"seq": peer})
        for at, peer in enumerate(seq_peers)
    ]
    landed[seq] = mine[seq]
    for copy in fars:
        copy.wait()
    tiny_ref[...] = jnp.sum(far[...], axis=0)
    for copy in swaps:
        copy.wait()
    group = w_ref.shape[3] // 3
    for source in range(seqs):
        for third in range(3):
            qkv_ref[:, pl.ds(third * wide + source * group, group)] = landed[
                source, :, pl.ds(third * group, group)
            ].astype(F32)
    line.drain()


def close_all(ways, qkv_rows, attn_part, sums, inputs, gain, resid, both, tag):
    seqs, dps = ways
    part = qkv_rows.shape[0] // (seqs * dps)
    wide3 = qkv_rows.shape[1]
    rows, wide = inputs.shape
    dma = pltpu.SemaphoreType.DMA
    vmem = pl.BlockSpec(memory_space=pltpu.VMEM)
    return pl.pallas_call(
        functools.partial(closing, ways),
        out_shape=(
            jax.ShapeDtypeStruct((part, 3 * wide), F32),
            jax.ShapeDtypeStruct((rows, wide), BF16),
            jax.ShapeDtypeStruct(sums.shape, F32),
            jax.ShapeDtypeStruct((part, dps * both.shape[2] // 2), F32),
            jax.ShapeDtypeStruct((part, dps * both.shape[2] // 2), F32),
        ),
        in_specs=[vmem] * 7,
        out_specs=(vmem,) * 5,
        scratch_shapes=Plane.scratch(seqs, rows, wide, BF16)
        + LineSum.scratch(dps, (seqs, part, wide3), BF16)
        + [
            pltpu.VMEM((seqs, part, wide3), BF16),
            pltpu.VMEM((seqs, part, wide3), BF16),
            pltpu.VMEM((seqs,) + sums.shape, F32),
            pltpu.VMEM((dps,) + sums.shape, F32),
            pltpu.VMEM(sums.shape, F32),
            dma((seqs - 1,)),
            dma((seqs - 1,)),
            dma((seqs - 1,)),
            dma((seqs - 1,)),
            dma((dps - 1,)),
            dma((dps - 1,)),
        ],
        cost_estimate=lasting(75),
        compiler_params=pltpu.CompilerParams(collective_id=tag, has_side_effects=True),
    )(
        qkv_rows.reshape(seqs, dps, part, wide3),
        attn_part.reshape(seqs, rows, wide),
        sums,
        inputs,
        gain,
        resid,
        both,
    )


def front(
    ways,
    qkv_weight_ref,
    in_ref,
    small_ref,
    gate_ref,
    up_ref,
    out_weight_ref,
    grad_ref,
    table_ref,
    w_ref,
    attn_ref,
    qkv_ref,
    att_ref,
    lse_ref,
    out_ref,
    vec_ref,
    resid_ref,
    all_ref,
    grads_ref,
    both_ref,
    *rest,
):
    seqs, dps = ways
    chips, count = dps // 2, seqs * dps
    rest = list(rest)

    def take(size):
        taken = rest[:size]
        del rest[:size]
        return taken

    x_ref, given_ref, bias_ref, cut_ref, swapped_ref, branch_ref, own_ref = take(7)
    gathered = PlaneGather(seqs, in_ref, x_ref, *take(3))
    outs = LineGather(dps, out_weight_ref, out_ref, *take(5))
    swap = SwapDp(dps, cut_ref, swapped_ref, *take(3))
    plane = Plane(seqs, branch_ref, *take(4))
    moved = LineGather(dps, own_ref, all_ref, *take(5))
    grads = LineGather(dps, grad_ref, grads_ref, *take(5))
    gates = PlaneGather(seqs, swapped_ref, both_ref, *take(3))
    swap_s, swap_r, line_s, line_r, pair_s, pair_r, small_s, small_r, own_sem = take(9)
    seq, dp = lax.axis_index("seq"), lax.axis_index("dp")
    _, chip, core, ends, sides, sibling = line_place(dps)
    me = seq * dps + dp
    part, group = qkv_weight_ref.shape[0], w_ref.shape[1] // 3
    rows, width = in_ref.shape
    length = rows * seqs
    barrier = pltpu.get_barrier_semaphore()

    def other(step):
        at = lax.rem(me + step, count)
        return {"seq": at // dps, "dp": lax.rem(at, dps)}

    @pl.loop(1, count)
    def _(step):
        pl.semaphore_signal(barrier, inc=1, device_id=other(step), device_id_type=MESH)

    pl.semaphore_wait(barrier, count - 1)

    def block(source, owner):
        return w_ref.at[pl.ds(pl.multiple_of((source * dps + owner) * part, part), part), :]

    def piece(source, third):
        here = pl.ds(pl.multiple_of((source * dps + dp) * part, part), part)
        return w_ref.at[here, pl.ds(third * group, group)]

    def columns(target, third):
        at = pl.multiple_of(third * width + target * group, 128)
        return qkv_weight_ref.at[:, pl.ds(at, group)]

    swaps = []
    for step in range(1, seqs):
        target = lax.rem(seq + step, seqs)
        for third in range(3):
            at = 3 * (step - 1) + third
            swaps.append(
                push(
                    columns(target, third),
                    piece(seq, third),
                    swap_s,
                    swap_r,
                    at,
                    {"seq": target},
                )
            )
    owns = [
        pltpu.make_async_copy(columns(seq, third), piece(seq, third), own_sem.at[third])
        for third in range(3)
    ]
    for own in owns:
        own.start()

    def small_copy(step):
        return remote(
            small_ref, given_ref.at[me], small_s.at[step - 1], small_r.at[step - 1], other(step)
        )

    @pl.loop(1, count)
    def _(step):
        small_copy(step).start()

    given_ref[me] = small_ref[...]
    gathered.begin()

    def onward(side, hop, source, owner_chip):
        part_of = block(source[1], 2 * owner_chip + core)
        at = (side, hop, source[0])
        return remote(part_of, part_of, line_s.at[at], line_r.at[at], sides[side])

    def share(source, owner_chip, owner_core):
        part_of = block(source[1], 2 * owner_chip + owner_core)
        at = (owner_chip, source[0])
        return remote(part_of, part_of, pair_s.at[at], pair_r.at[at], sibling)

    sources = [(back, lax.rem(seq - back + seqs, seqs)) for back in range(seqs)]
    for source in sources:
        if source[0] == 0:
            for own in owns:
                own.wait()
        else:
            for third in range(3):
                swaps[3 * (source[0] - 1) + third].wait_recv()
        for side in range(2):

            @pl.when(ends[side])
            def _(side=side, source=source):
                onward(side, 0, source, chip).start()

        share(source, chip, core).start()
    gathered.relay()

    def pass_on(hop):
        for source in sources:
            for side in range(2):
                origin = chip - 1 - hop if side == 0 else chip + 1 + hop
                there = origin >= 0 if side == 0 else origin < chips

                @pl.when(there)
                def _(side=side, source=source, origin=origin):
                    onward(side, hop, source, origin).wait_recv()
                    share(source, origin, core).start()

                if hop < chips - 2:

                    @pl.when(jnp.logical_and(there, ends[side]))
                    def _(side=side, source=source, origin=origin):
                        onward(side, hop + 1, source, origin).start()

    units = gate_ref.shape[1] // count
    for at, weight in enumerate((gate_ref, up_ref)):
        for source in range(seqs):
            for owner in range(dps):
                cut_ref[owner, :, pl.ds((at * seqs + source) * units, units)] = weight[
                    :, pl.ds((source * dps + owner) * units, units)
                ]
    pass_on(0)

    @pl.loop(1, count)
    def _(step):
        small_copy(step).wait()

    lane, sides_of = halves()
    per = 128 // part

    def row_of(pick):
        value = jnp.zeros((1, 128), F32)
        for unit in range(per):
            found = pick(unit)
            found = pltpu.roll(found, unit * part, 1) if unit else found
            mask = (lane >= unit * part) & (lane < (unit + 1) * part)
            value = jnp.where(mask, found, value)
        return value

    for kind in range(4):
        for chunk in range(width // 128):
            vec_ref[kind : kind + 1, pl.ds(chunk * 128, 128)] = row_of(
                lambda unit, kind=kind, chunk=chunk: given_ref[chunk * per + unit, kind : kind + 1]
            )
    for chunk in range(3 * group // 128):
        third, inner = chunk * 128 // group, chunk * 128 % group // part
        first = third * count + seq * dps + inner

        def pick(unit, first=first):
            at = first + unit
            return given_ref[at // 3, pl.ds(4 + lax.rem(at, 3), 1)]

        bias_ref[0:1, pl.ds(chunk * 128, 128)] = row_of(pick)
    for hop in range(1, chips - 1):
        pass_on(hop)
    outs.begin()
    gathered.end()
    gain_one, shift_one = vec_ref[0:1, :], vec_ref[1:2, :]

    for source in range(seqs):

        def norm(here, source=source):
            normed, _ = normalize(x_ref[source, here, :].astype(F32))
            at = pl.ds(pl.multiple_of(source * rows + here.start, CHUNK), CHUNK)
            attn_ref[at, :] = (normed * gain_one + shift_one).astype(attn_ref.dtype)

        by_chunks(rows, norm)
    for owner in range(chips):
        for source in sources:
            share(source, owner, 1 - core).wait_recv()
    tile = min(256, group)

    def product(at):
        here = pl.ds(pl.multiple_of(at * tile, tile), tile)
        return here, dot(attn_ref[...], w_ref[:, here]) + bias_ref[0:1, here]

    @pl.loop(0, 2 * group // tile)
    def _(at):
        _, value = product(at)
        for half in range(tile // 128):
            turned = turn_lanes(value[:, half * 128 : (half + 1) * 128], table_ref, 1.0)
            here = pl.ds(pl.multiple_of(at * tile + half * 128, 128), 128)
            qkv_ref[:, here] = turned.astype(qkv_ref.dtype)

    outs.hop(0)

    @pl.loop(2 * group // tile, 3 * group // tile)
    def _(at):
        here, value = product(at)
        qkv_ref[:, here] = value.astype(qkv_ref.dtype)

    for hop in range(1, chips - 1):
        outs.hop(hop)
    swap.begin()
    scale = HEAD_DIM ** (-0.5)
    size = min(256, length)
    triangle = lax.broadcasted_iota(jnp.int32, (size, size), 1) <= lax.broadcasted_iota(
        jnp.int32, (size, size), 0
    )

    @pl.loop(0, group // 128)
    def _(at):
        base = pl.multiple_of(at * 128, 128)
        for part_at in range(length // size):
            here = pl.ds(part_at * size, size)
            seen = (part_at + 1) * size
            query = qkv_ref[here, pl.ds(base, 128)]
            key = qkv_ref[pl.ds(0, seen), pl.ds(group + base, 128)]
            value = qkv_ref[pl.ds(0, seen), pl.ds(2 * group + base, 128)]
            mixed = []
            for half in range(2):
                mine = jnp.where(sides_of[half], query, jnp.zeros_like(query))
                scores = contract_cols(mine, key) * scale
                last = jnp.where(triangle, scores[:, part_at * size :], -jnp.inf)
                if part_at:
                    scores = jnp.concatenate([scores[:, : part_at * size], last], 1)
                else:
                    scores = last
                largest = jnp.max(scores, axis=1, keepdims=True)
                exponent = jnp.exp(scores - largest)
                totals = jnp.sum(exponent, axis=1, keepdims=True)
                probs = (exponent * (1.0 / totals)).astype(value.dtype)
                mixed.append(dot(probs, value))
                lse_ref[here, :] = jnp.where(
                    lane == 2 * at + half, largest + jnp.log(totals), lse_ref[here, :]
                )
            att_ref[here, pl.ds(base, 128)] = jnp.where(sides_of[0], mixed[0], mixed[1]).astype(
                att_ref.dtype
            )

    outs.end()
    step = min(256, width)

    @pl.loop(0, width // step)
    def _(at):
        here = pl.ds(pl.multiple_of(at * step, step), step)
        value = jnp.zeros((length, step), F32)
        for owner in range(dps):
            value = value + dot(att_ref[:, pl.ds(owner * part, part)], out_ref[owner, :, here])
        for source in range(seqs):
            branch_ref[source, :, here] = value[source * rows : (source + 1) * rows].astype(
                branch_ref.dtype
            )

    plane.begin()
    grads.begin()
    plane.relay()
    plane.end()
    swap.end()
    gates.begin()
    gain_two, shift_two = vec_ref[2:3, :], vec_ref[3:4, :]

    def one(here):
        resid = in_ref[here, :].astype(F32) + plane.total(here)
        resid_ref[here, :] = resid
        normed, _ = normalize(resid)
        own_ref[here, :] = (normed * gain_two + shift_two).astype(own_ref.dtype)

    by_chunks(rows, one)
    moved.begin()
    for hop in range(chips - 1):
        grads.hop(hop)
        if hop == min(1, chips - 2):
            gates.relay()
        moved.hop(hop)
    grads.end()
    moved.end()
    gates.end()

    for swapped in swaps:
        swapped.wait_send()
    for hop in range(chips - 1):
        for source in sources:
            for side in range(2):
                origin = chip - hop if side == 0 else chip + hop
                there = origin >= 0 if side == 0 else origin < chips

                @pl.when(jnp.logical_and(there, ends[side]))
                def _(side=side, hop=hop, source=source, origin=origin):
                    onward(side, hop, source, origin).wait_send()

    for owner in range(chips):
        for source in sources:
            share(source, owner, core).wait_send()


def front_all(ways, qkv_weight, inputs, small, gate, up, out_weight, grad_out, table, tag):
    seqs, dps = ways
    chips, count = dps // 2, seqs * dps
    part, width = out_weight.shape
    rows = inputs.shape[0]
    length, group, cols = rows * seqs, width // seqs, 2 * gate.shape[1] // dps
    dma = pltpu.SemaphoreType.DMA
    vmem, anywhere = (pl.BlockSpec(memory_space=space) for space in (pltpu.VMEM, pl.ANY))

    def made(dtype, *shape):
        return jax.ShapeDtypeStruct(shape, dtype)

    return pl.pallas_call(
        functools.partial(front, ways),
        out_shape=(
            made(BF16, width, 3 * group),
            made(BF16, length, width),
            made(BF16, length, 3 * group),
            made(BF16, length, group),
            made(F32, length, 128),
            made(BF16, dps, part, width),
            made(F32, 8, width),
            made(F32, rows, width),
            made(BF16, dps, rows, width),
            made(BF16, dps, rows, width),
            made(BF16, seqs, dps, part, cols),
        ),
        in_specs=[vmem] * 8,
        out_specs=(vmem,) * 8 + (anywhere,) * 3,
        scratch_shapes=[
            pltpu.VMEM((seqs, rows, width), BF16),
            pltpu.VMEM((count, 8, 128), F32),
            pltpu.VMEM((8, 3 * group), F32),
            pltpu.VMEM((dps, part, cols), BF16),
            pltpu.VMEM((dps, part, cols), BF16),
            pltpu.VMEM((seqs, rows, width), BF16),
            pltpu.VMEM((rows, width), BF16),
        ]
        + PlaneGather.scratch(seqs)
        + LineGather.scratch(dps)
        + SwapDp.scratch(dps)
        + Plane.scratch(seqs, rows, width, BF16)
        + LineGather.scratch(dps)
        + LineGather.scratch(dps)
        + PlaneGather.scratch(seqs)
        + [
            dma((3 * (seqs - 1),)),
            dma((3 * (seqs - 1),)),
            dma((2, chips - 1, seqs)),
            dma((2, chips - 1, seqs)),
            dma((chips, seqs)),
            dma((chips, seqs)),
            dma((count - 1,)),
            dma((count - 1,)),
            dma((3,)),
        ],
        cost_estimate=lasting(180),
        compiler_params=pltpu.CompilerParams(
            collective_id=tag, has_side_effects=True, vmem_limit_bytes=60 * 2**20
        ),
    )(qkv_weight, inputs, small, gate, up, out_weight, grad_out, table)


def after(value, *earlier):
    return lax.optimization_barrier((value,) + earlier)[0]


def shards(
    ways,
    inputs,
    first_gain,
    first_shift,
    qkv_weight,
    qkv_bias,
    out_weight,
    second_gain,
    second_shift,
    gate_weight,
    up_weight,
    down_weight,
    out_cotangent,
):
    seqs, dps = ways
    width = inputs.shape[2]
    rows = inputs.shape[1]
    length = rows * seqs
    part = width // (seqs * dps)
    units = down_weight.shape[0]
    group = width // seqs
    me_seq = lax.axis_index("seq")
    grad_out = out_cotangent[0]

    small = [item[None] for item in (first_gain, first_shift, second_gain, second_shift)]
    small = jnp.concatenate(small + [qkv_bias.reshape(3, part)]).astype(F32)
    small = jnp.pad(small, ((0, 1), (0, 128 - part)))
    table = tables(length)
    down_full = gather(down_weight, "seq")
    (
        qkv_full,
        attn_all,
        qkv,
        attended,
        log_total,
        out_full,
        vectors,
        residual,
        mlp_all,
        grad_all,
        gate_up,
    ) = front_all(
        ways,
        qkv_weight,
        inputs[0],
        small,
        gate_weight,
        up_weight,
        out_weight,
        grad_out,
        table,
        0,
    )
    out_full = out_full.reshape(group, width)
    gain_one, gain_two = vectors[0:1], vectors[2:3]
    mlp_all = mlp_all.reshape(dps * rows, width)
    grad_all = grad_all.reshape(dps * rows, width)
    gate_up = gate_up.reshape(width, 2 * seqs * units)
    wide = seqs * units

    both = dot(mlp_all, gate_up)
    gate_value = both[:, :wide]
    up_value = both[:, wide:]
    sigmoid_gate = jax.nn.sigmoid(gate_value)
    activated = gate_value * sigmoid_gate
    hidden = (activated * up_value).astype(BF16)
    out_part = dot(hidden, down_full).astype(BF16)

    hidden_grad = contract_cols(grad_all, down_full)
    gate_grad = (
        hidden_grad * up_value * (sigmoid_gate * (1.0 + gate_value * (1.0 - sigmoid_gate)))
    ).astype(BF16)
    up_grad = (hidden_grad * activated).astype(BF16)
    both_grad = jnp.concatenate([gate_grad, up_grad], 1)
    mlp_part = contract_cols(both_grad, gate_up).astype(BF16)
    both_rows = contract_rows(mlp_all, after(both_grad, mlp_part)).astype(BF16)
    down_rows = contract_rows(hidden, grad_all).astype(BF16)
    mlp_part = after(mlp_part, both_rows, down_rows)
    residual_grad, branch_all, sums, layer_out, both_rows = turn_all(
        ways, mlp_part, residual, gain_two, grad_out, out_part, both_rows, 2
    )
    down_rows = after(down_rows, residual_grad)
    down_shard = scatter_sum(down_rows, "seq").astype(F32)

    attn_part, qkv_rows, bias_term, out_rows, both_rows = reverse_all(
        ways,
        branch_all,
        out_full,
        qkv,
        log_total.T,
        table,
        qkv_full,
        attn_all,
        attended,
        both_rows.reshape(dps, part, 2 * seqs * units),
        5,
    )
    out_shard = scatter_sum(out_rows, "dp").astype(F32)
    bias_term = bias_term[0].reshape(3, 1, group)
    here = (jnp.arange(seqs, dtype=jnp.int32) == me_seq).astype(F32)[None, :, None]
    bias_term = jnp.pad((bias_term * here).reshape(3, width), ((4, 1), (0, 0)))
    sums = sums + bias_term
    qkv_shard, input_grad, tiny, gate_shard, up_shard = close_all(
        ways,
        qkv_rows,
        attn_part,
        sums,
        inputs[0],
        gain_one,
        residual_grad,
        both_rows,
        3,
    )
    me = me_seq * dps + lax.axis_index("dp")
    mine = lax.dynamic_slice_in_dim(tiny, me * part, part, 1)
    bias_shard = lax.dynamic_slice_in_dim(tiny[4:7].reshape(-1), me * 3 * part, 3 * part, 0)

    return (
        layer_out[None],
        input_grad[None],
        mine[0],
        mine[1],
        qkv_shard,
        bias_shard,
        out_shard,
        mine[2],
        mine[3],
        gate_shard,
        up_shard,
        down_shard,
    )


def solution(mesh):
    split = ("seq", "dp")
    tokens = P("dp", "seq", None)
    in_specs = (
        tokens,
        P(split),
        P(split),
        P(split, None),
        P(split),
        P(split, None),
        P(split),
        P(split),
        P(split, None),
        P(split, None),
        P(split, None),
        tokens,
    )
    out_specs = (
        tokens,
        tokens,
        P(split),
        P(split),
        P(split, None),
        P(split),
        P(split, None),
        P(split),
        P(split),
        P(split, None),
        P(split, None),
        P(split, None),
    )
    ways = (mesh.shape["seq"], mesh.shape["dp"])

    def local(*args):
        return shards(ways, *args)

    return jax.shard_map(local, mesh=mesh, in_specs=in_specs, out_specs=out_specs, check_vma=False)
```

```python
import functools

import jax
import jax.numpy as jnp
from jax import lax
from jax.experimental import pallas as pl
from jax.experimental.pallas import tpu as pltpu
from jax.sharding import PartitionSpec as P


HEAD_DIM = 64
ROT = 16
F32 = jnp.float32
BF16 = jnp.bfloat16


def normalize(values):
    center = values - jnp.mean(values, axis=-1, keepdims=True)
    variance = jnp.mean(center * center, axis=-1, keepdims=True)
    inverse = lax.rsqrt(variance + 1e-05)
    return (center * inverse, inverse)


def norm_back(grad_normed, normed, inverse, gain):
    scaled = grad_normed * gain
    centered = scaled - jnp.mean(scaled, axis=-1, keepdims=True)
    return inverse * (centered - normed * jnp.mean(scaled * normed, axis=-1, keepdims=True))


def dot(left, right):
    return jnp.dot(left, right, preferred_element_type=F32)


def contract_rows(left, right):
    return lax.dot_general(left, right, (((0,), (0,)), ((), ())), preferred_element_type=F32)


def contract_cols(left, right):
    return lax.dot_general(left, right, (((1,), (1,)), ((), ())), preferred_element_type=F32)


def tables(length):
    half_rot = ROT // 2
    lane = lax.rem(lax.broadcasted_iota(jnp.int32, (length, 128), 1), HEAD_DIM)
    position = lax.broadcasted_iota(jnp.int32, (length, 128), 0).astype(F32)
    freqs = 10000.0 ** (-(2.0 * lax.rem(lane, half_rot).astype(F32)) / ROT)
    angles = position * freqs
    cosine, sine = jnp.cos(angles), jnp.sin(angles)
    return jnp.stack(
        [
            jnp.where(lane < ROT, cosine, 1.0),
            jnp.where(lane < half_rot, -sine, 0.0),
            jnp.where((lane >= half_rot) & (lane < ROT), sine, 0.0),
        ]
    )


def turn_lanes(value, table_ref, sign):
    half_rot = ROT // 2
    ahead, behind = pltpu.roll(value, 128 - half_rot, 1), pltpu.roll(value, half_rot, 1)
    return value * table_ref[0] + sign * (ahead * table_ref[1] + behind * table_ref[2])


def gather(value, axis):
    return lax.all_gather(value, axis, axis=0, tiled=True)


def scatter_sum(value, axis):
    return lax.psum_scatter(value, axis, scatter_dimension=0, tiled=True)


MESH = pl.DeviceIdType.MESH


def lasting(micros):
    return pl.CostEstimate(flops=0, transcendentals=0, bytes_accessed=int(micros * 3.0e6))


def meet(peers):
    barrier = pltpu.get_barrier_semaphore()
    for peer in peers:
        pl.semaphore_signal(barrier, inc=1, device_id=peer, device_id_type=MESH)
    pl.semaphore_wait(barrier, len(peers))


def push(source, target, send, recv, at, peer):
    copy = pltpu.make_async_remote_copy(
        src_ref=source,
        dst_ref=target,
        send_sem=send.at[at],
        recv_sem=recv.at[at],
        device_id=peer,
        device_id_type=MESH,
    )
    copy.start()
    return copy


def corners():
    me = lax.axis_index("seq")
    high, low = me // 2, lax.rem(me, 2)
    across = high * 2 + (1 - low)
    along = (1 - high) * 2 + low
    return me, across, along, 3 - me


def remote(source, target, send, recv, peer):
    return pltpu.make_async_remote_copy(
        src_ref=source,
        dst_ref=target,
        send_sem=send,
        recv_sem=recv,
        device_id=peer,
        device_id_type=MESH,
    )


def line_place(dps):
    dp = lax.axis_index("dp")
    chip, core = dp // 2, lax.rem(dp, 2)
    chips = dps // 2
    ends = (chip + 1 < chips, chip >= 1)
    sides = ({"dp": lax.rem(dp + 2, dps)}, {"dp": lax.rem(dp - 2 + dps, dps)})
    return chips, chip, core, ends, sides, {"dp": 2 * chip + (1 - core)}


class Plane:

    def __init__(self, count, x_ref, pair, got, send, recv):
        self.count, self.x, self.pair, self.got = count, x_ref, pair, got
        self.send, self.recv = send, recv
        self.square = count == 4

    def begin(self, make=None):
        x, got, send, recv = self.x, self.got, self.send, self.recv
        make = make or (lambda block: None)
        me = lax.axis_index("seq")
        self.copies = []
        if not self.square:
            for at, step in enumerate(range(1, self.count)):
                target = lax.rem(me + step, self.count)
                make(target)
                self.copies.append(push(x.at[target], got.at[at], send, recv, at, {"seq": target}))
            make(me)
            return
        _, across, along, far = corners()
        half = x.shape[1] // 2
        top, low = pl.ds(0, half), pl.ds(half, half)
        to_across, to_along = {"seq": across}, {"seq": along}
        make(far)
        self.copies = [
            push(x.at[far, top], self.pair.at[0], send, recv, 0, to_across),
            push(x.at[far, low], self.pair.at[1], send, recv, 1, to_along),
        ]
        make(across)
        self.copies.append(push(x.at[across, top], got.at[0, top], send, recv, 2, to_across))
        make(along)
        self.copies.append(push(x.at[along, low], got.at[1, low], send, recv, 3, to_along))
        make(me)

    def relay(self):
        if not self.square:
            return
        x, pair, got, send, recv = self.x, self.pair, self.got, self.send, self.recv
        _, across, along, _ = corners()
        half = x.shape[1] // 2
        top, low = pl.ds(0, half), pl.ds(half, half)
        self.copies[0].wait_recv()
        pair[2] = (pair[0].astype(F32) + x[along, top].astype(F32)).astype(pair.dtype)
        self.copies.append(push(pair.at[2], got.at[1, top], send, recv, 4, {"seq": along}))
        self.copies[1].wait_recv()
        pair[3] = (pair[1].astype(F32) + x[across, low].astype(F32)).astype(pair.dtype)
        self.copies.append(push(pair.at[3], got.at[0, low], send, recv, 5, {"seq": across}))

    def end(self):
        for at, copy in enumerate(self.copies):
            copy.wait_send()
            if not self.square or at > 1:
                copy.wait_recv()

    def total(self, rows):
        value = self.x[lax.axis_index("seq"), rows].astype(F32)
        for at in range(2 if self.square else self.count - 1):
            value = value + self.got[at, rows].astype(F32)
        return value

    @staticmethod
    def scratch(count, rows, wide, dtype):
        slots = 6 if count == 4 else count - 1
        return [
            pltpu.VMEM((4, rows // 2, wide), dtype),
            pltpu.VMEM((2 if count == 4 else count - 1, rows, wide), dtype),
            pltpu.SemaphoreType.DMA((slots,)),
            pltpu.SemaphoreType.DMA((slots,)),
        ]


class LineSum:

    def __init__(self, dps, block, pair, moving, line_s, line_r, pair_s, pair_r):
        self.block, self.pair, self.moving = block, pair, moving
        self.sems = (line_s, line_r, pair_s, pair_r)
        self.chips, self.chip, self.core, self.ends, self.sides, self.sibling = line_place(dps)
        self.pieces = pair.shape[1]

    def share(self, owner, owner_core, piece):
        at = (owner, piece)
        return remote(
            self.block(2 * owner + owner_core).at[piece],
            self.pair.at[at],
            self.sems[2].at[at],
            self.sems[3].at[at],
            self.sibling,
        )

    def onward(self, side, owner, piece):
        at = (side, owner, piece)
        return remote(
            self.pair.at[owner, piece],
            self.moving.at[at],
            self.sems[0].at[at],
            self.sems[1].at[at],
            self.sides[side],
        )

    def begin(self):
        order = [
            at for both in zip(range(self.chips - 1, -1, -1), range(self.chips)) for at in both
        ]
        for owner in dict.fromkeys(order):
            for piece in range(self.pieces):
                self.share(owner, 1 - self.core, piece).start()

    def add(self, owner, piece, side):
        own = self.block(2 * owner + self.core)

        def one(here):
            value = self.pair[owner, piece, here].astype(F32) + own[piece, here].astype(F32)
            if side is not None:
                value = value + self.moving[side, owner, piece, here].astype(F32)
            self.pair[owner, piece, here] = value.astype(self.pair.dtype)

        by_chunks(self.pair.shape[2], one)

    def lead(self):
        for at in range(self.chips):
            for piece in range(self.pieces):
                for side in range(2):
                    owner = self.chips - 1 - at if side == 0 else at
                    passing = self.chip < owner if side == 0 else self.chip > owner

                    @pl.when(jnp.logical_and(passing, jnp.logical_not(self.ends[1 - side])))
                    def _(side=side, owner=owner, piece=piece):
                        self.share(owner, self.core, piece).wait_recv()
                        self.add(owner, piece, None)
                        self.onward(side, owner, piece).start()

    def step(self, at):
        for piece in range(self.pieces):
            for side in range(2):
                owner = self.chips - 1 - at if side == 0 else at
                passing = self.chip < owner if side == 0 else self.chip > owner

                @pl.when(jnp.logical_and(passing, self.ends[1 - side]))
                def _(side=side, owner=owner, piece=piece):
                    self.share(owner, self.core, piece).wait_recv()
                    self.onward(side, owner, piece).wait_recv()
                    self.add(owner, piece, side)
                    self.onward(side, owner, piece).start()

    def end(self):
        for owner in range(self.chips):
            for piece in range(self.pieces):

                @pl.when(self.chip == owner)
                def _(owner=owner, piece=piece):
                    self.share(owner, self.core, piece).wait_recv()

                for side in range(2):

                    @pl.when(jnp.logical_and(self.chip == owner, self.ends[1 - side]))
                    def _(side=side, owner=owner, piece=piece):
                        self.onward(side, owner, piece).wait_recv()

        for side in range(2):

            @pl.when(jnp.logical_not(self.ends[1 - side]))
            def _(side=side):
                self.moving[side, self.chip] = jnp.zeros(self.moving.shape[2:], self.moving.dtype)

    def total(self, piece, here):
        own = self.block(2 * self.chip + self.core)
        value = own[piece, here].astype(F32) + self.pair[self.chip, piece, here].astype(F32)
        for side in range(2):
            value = value + self.moving[side, self.chip, piece, here].astype(F32)
        return value

    def drain(self):
        for owner in range(self.chips):
            for piece in range(self.pieces):
                for side in range(2):
                    passing = self.chip < owner if side == 0 else self.chip > owner

                    @pl.when(passing)
                    def _(side=side, owner=owner, piece=piece):
                        self.onward(side, owner, piece).wait_send()

                self.share(owner, 1 - self.core, piece).wait_send()

    @staticmethod
    def scratch(dps, shape, dtype):
        dma, chips, pieces = pltpu.SemaphoreType.DMA, dps // 2, shape[0]
        return [
            pltpu.VMEM((chips,) + shape, dtype),
            pltpu.VMEM((2, chips) + shape, dtype),
            dma((2, chips, pieces)),
            dma((2, chips, pieces)),
            dma((chips, pieces)),
            dma((chips, pieces)),
        ]


class PlaneGather:

    def __init__(self, count, x_ref, o_ref, send, recv, local):
        self.count, self.x, self.o = count, x_ref, o_ref
        self.send, self.recv, self.local = send, recv, local
        self.square = count == 4

    def begin(self):
        x, o, send, recv = self.x, self.o, self.send, self.recv
        me = lax.axis_index("seq")
        if self.square:
            _, across, along, _ = corners()
            half = x.shape[0] // 2
            top, low = pl.ds(0, half), pl.ds(half, half)
            to_across, to_along = {"seq": across}, {"seq": along}
            self.copies = [
                push(x.at[top], o.at[me, top], send, recv, 0, to_across),
                push(x.at[low], o.at[me, low], send, recv, 1, to_along),
                push(x.at[low], o.at[me, low], send, recv, 2, to_across),
                push(x.at[top], o.at[me, top], send, recv, 3, to_along),
            ]
        else:
            self.copies = [
                push(x, o.at[me], send, recv, step - 1, {"seq": lax.rem(me + step, self.count)})
                for step in range(1, self.count)
            ]
        self.own = pltpu.make_async_copy(x, o.at[me], self.local)
        self.own.start()

    def relay(self):
        if not self.square:
            return
        o, send, recv = self.o, self.send, self.recv
        _, across, along, _ = corners()
        half = self.x.shape[0] // 2
        top, low = pl.ds(0, half), pl.ds(half, half)
        self.copies[0].wait_recv()
        self.copies.append(
            push(o.at[across, top], o.at[across, top], send, recv, 4, {"seq": along})
        )
        self.copies[1].wait_recv()
        self.copies.append(
            push(o.at[along, low], o.at[along, low], send, recv, 5, {"seq": across})
        )

    def end(self):
        for at, copy in enumerate(self.copies):
            copy.wait_send()
            if not self.square or at > 1:
                copy.wait_recv()
        self.own.wait()

    @staticmethod
    def scratch(count):
        slots = 6 if count == 4 else count - 1
        dma = pltpu.SemaphoreType.DMA
        return [dma((slots,)), dma((slots,)), dma]


class LineGather:

    def __init__(self, dps, x_ref, o_ref, line_s, line_r, pair_s, pair_r, local):
        self.x, self.o, self.local = x_ref, o_ref, local
        self.sems = (line_s, line_r, pair_s, pair_r)
        self.chips, self.chip, self.core, self.ends, self.sides, self.sibling = line_place(dps)

    def onward(self, side, hop, owner, source=None):
        block = self.o.at[2 * owner + self.core]
        at = (side, hop)
        return remote(
            block if source is None else source,
            block,
            self.sems[0].at[at],
            self.sems[1].at[at],
            self.sides[side],
        )

    def share(self, owner, owner_core, source=None):
        block = self.o.at[2 * owner + owner_core]
        return remote(
            block if source is None else source,
            block,
            self.sems[2].at[owner],
            self.sems[3].at[owner],
            self.sibling,
        )

    def begin(self):
        for side in range(2):

            @pl.when(self.ends[side])
            def _(side=side):
                self.onward(side, 0, self.chip, self.x).start()

        self.share(self.chip, self.core, self.x).start()
        self.own = pltpu.make_async_copy(
            self.x, self.o.at[2 * self.chip + self.core], self.local
        )
        self.own.start()

    def hop(self, hop):
        for side in range(2):
            origin = self.chip - 1 - hop if side == 0 else self.chip + 1 + hop
            there = origin >= 0 if side == 0 else origin < self.chips

            @pl.when(there)
            def _(side=side, origin=origin):
                self.onward(side, hop, origin).wait_recv()

            if hop < self.chips - 2:

                @pl.when(jnp.logical_and(there, self.ends[side]))
                def _(side=side, origin=origin):
                    self.onward(side, hop + 1, origin).start()

            @pl.when(there)
            def _(origin=origin):
                self.share(origin, self.core).start()

    def end(self):
        self.own.wait()
        for hop in range(self.chips - 1):
            for side in range(2):
                origin = self.chip - hop if side == 0 else self.chip + hop
                there = origin >= 0 if side == 0 else origin < self.chips

                @pl.when(jnp.logical_and(there, self.ends[side]))
                def _(side=side, hop=hop, origin=origin):
                    self.onward(side, hop, origin).wait_send()

        for owner in range(self.chips):
            self.share(owner, self.core).wait_send()
            self.share(owner, 1 - self.core).wait_recv()

    @staticmethod
    def scratch(dps):
        dma, chips = pltpu.SemaphoreType.DMA, dps // 2
        return [dma((2, chips - 1)), dma((2, chips - 1)), dma((chips,)), dma((chips,)), dma]


CHUNK = 16


def by_chunks(rows, body):
    @pl.loop(0, rows // CHUNK)
    def _(at):
        body(pl.ds(pl.multiple_of(at * CHUNK, CHUNK), CHUNK))


PIECES = 2


def by_pieces(rows, body):
    size = rows // PIECES
    for piece in range(PIECES):

        @pl.loop(0, size // CHUNK)
        def _(at, piece=piece):
            here = pl.multiple_of(at * CHUNK, CHUNK)
            body(pl.ds(pl.multiple_of(piece * size + here, CHUNK), CHUNK), piece, pl.ds(here, CHUNK))


def meet_cross(ways):
    seqs, dps = ways
    seq, dp = lax.axis_index("seq"), lax.axis_index("dp")
    seq_peers = [lax.rem(seq + step, seqs) for step in range(1, seqs)]
    dp_peers = [lax.rem(dp + step, dps) for step in range(1, dps)]
    meet([{"seq": peer} for peer in seq_peers] + [{"dp": peer} for peer in dp_peers])
    return seq_peers, dp_peers


def turning(ways, inside, part_ref, resid_ref, gain_ref, grad_ref, *rest):
    seqs, dps = ways
    rest = list(rest)

    def take(size):
        taken = rest[:size]
        del rest[:size]
        return taken

    if inside:
        hidden_ref, down_ref, mlp_ref, back_ref, grads_ref = take(5)
    else:
        out_ref, both_ref = take(2)
    total_ref, all_ref, sums_ref, layer_ref, rows_ref = take(5)
    if inside:
        (down_rows_ref,) = take(1)
    line = LineSum(dps, lambda owner: part_ref.at[owner], *take(6))
    (own,) = take(1)
    gathered = PlaneGather(seqs, own, all_ref, *take(3))
    outs_refs, both_refs = take(6), take(4)
    if inside:
        out_ref, both_ref = take(2)
    outs = LineSum(dps, lambda owner: out_ref.at[owner], *outs_refs)
    both = Plane(seqs, both_ref, *both_refs)
    chips = dps // 2
    group, wide = both_ref.shape[1], resid_ref.shape[1]
    tile = min(256, group)

    def both_rows(source):
        @pl.loop(0, group // tile)
        def _(at):
            columns = pl.ds(pl.multiple_of(source * group + at * tile, tile), tile)
            here = pl.ds(pl.multiple_of(at * tile, tile), tile)
            both_ref[source, here, :] = contract_rows(mlp_ref[:, columns], back_ref[...]).astype(
                both_ref.dtype
            )

    def out_part():
        step = min(256, wide)

        @pl.loop(0, wide // step)
        def _(at):
            here = pl.ds(pl.multiple_of(at * step, step), step)
            value = dot(hidden_ref[...], down_ref[:, here]).astype(out_ref.dtype)
            out_ref[:, :, :, here] = value.reshape(out_ref.shape[:3] + (step,))

    def down_rows():
        count = down_rows_ref.shape[0]
        for first in range(0, count, 256):
            here = slice(first, min(first + 256, count))
            down_rows_ref[here, :] = contract_rows(hidden_ref[:, here], grads_ref[...]).astype(
                down_rows_ref.dtype
            )

    meet_cross(ways)
    line.begin()
    line.lead()
    served = []

    def make(source):
        if inside:
            both_rows(source)
        if len(served) == 1:
            line.step(0)
        served.append(source)

    both.begin(make)
    if inside:
        out_part()
    outs.begin()
    line.step(1)
    both.relay()
    for at in range(2, chips):
        line.step(at)
    outs.lead()
    line.end()
    sums_ref[...] = jnp.zeros(sums_ref.shape, F32)
    gain = gain_ref[...]

    def one(here, piece, inner):
        grad = line.total(piece, inner)
        normed, inverse = normalize(resid_ref[here, :])
        sums_ref[2:3, :] += jnp.sum(grad * normed, axis=0, keepdims=True)
        sums_ref[3:4, :] += jnp.sum(grad, axis=0, keepdims=True)
        total = grad_ref[here, :].astype(F32) + norm_back(grad, normed, inverse, gain)
        total_ref[here, :] = total
        own[here, :] = total.astype(own.dtype)

    by_pieces(resid_ref.shape[0], one)
    gathered.begin()
    outs.step(0)
    gathered.relay()
    for at in range(1, chips):
        outs.step(at)
    if inside:
        down_rows()
    both.end()

    def two(here):
        rows_ref[here, :] = both.total(here).astype(rows_ref.dtype)

    by_chunks(rows_ref.shape[0], two)
    gathered.end()
    outs.end()

    def three(here, piece, inner):
        layer_ref[here, :] = (resid_ref[here, :] + outs.total(piece, inner)).astype(layer_ref.dtype)

    by_pieces(resid_ref.shape[0], three)
    line.drain()
    outs.drain()


def turn_all(ways, part, resid, gain, grad_out, hidden, down_full, mlp_all, both_grad, grad_all, tag):
    seqs, dps = ways
    rows, wide = resid.shape
    cut = (wide // seqs, both_grad.shape[1])
    inside = dps * rows <= 1024
    pieces = (dps, PIECES, rows // PIECES, wide)
    vmem, anywhere = (pl.BlockSpec(memory_space=space) for space in (pltpu.VMEM, pl.ANY))
    operands = [part.reshape(pieces), resid, gain, grad_out]
    made = [
        jax.ShapeDtypeStruct((rows, wide), F32),
        jax.ShapeDtypeStruct((seqs, rows, wide), BF16),
        jax.ShapeDtypeStruct((8, wide), F32),
        jax.ShapeDtypeStruct((rows, wide), BF16),
        jax.ShapeDtypeStruct(cut, BF16),
    ]
    places = [vmem, anywhere, vmem, vmem, vmem]
    scratch = (
        LineSum.scratch(dps, pieces[1:], BF16)
        + [pltpu.VMEM((rows, wide), BF16)]
        + PlaneGather.scratch(seqs)
        + LineSum.scratch(dps, pieces[1:], BF16)
        + Plane.scratch(seqs, cut[0], cut[1], BF16)
    )
    if inside:
        operands += [hidden, down_full, mlp_all, both_grad, grad_all]
        made.append(jax.ShapeDtypeStruct((hidden.shape[1], wide), BF16))
        places.append(vmem)
        scratch += [pltpu.VMEM(pieces, BF16), pltpu.VMEM((seqs,) + cut, BF16)]
    else:
        out_part = dot(hidden, down_full).astype(BF16)
        both = contract_rows(mlp_all, both_grad).astype(BF16)
        down_rows = contract_rows(hidden, grad_all).astype(BF16)
        operands += [out_part.reshape(pieces), both.reshape((seqs,) + cut)]
    results = pl.pallas_call(
        functools.partial(turning, ways, inside),
        out_shape=tuple(made),
        in_specs=[vmem] * len(operands),
        out_specs=tuple(places),
        scratch_shapes=scratch,
        cost_estimate=lasting(85),
        compiler_params=pltpu.CompilerParams(
            collective_id=tag, has_side_effects=True, vmem_limit_bytes=63 * 2**20
        ),
    )(*operands)
    total, gathered, sums, layer, both = results[:5]
    if inside:
        down_rows = results[5]
    return total, gathered.reshape(seqs * rows, wide), sums, layer, both, down_rows


class SwapDp:

    def __init__(self, dps, x_ref, o_ref, send, recv, local):
        dp = lax.axis_index("dp")
        self.peers = [lax.rem(dp + step, dps) for step in range(1, dps)]
        self.parts = (x_ref, o_ref, send, recv, local, dp)

    def begin(self):
        x, o, send, recv, local, dp = self.parts
        self.copies = [
            push(x.at[peer], o.at[dp], send, recv, at, {"dp": peer})
            for at, peer in enumerate(self.peers)
        ]
        self.own = pltpu.make_async_copy(x.at[dp], o.at[dp], local)
        self.own.start()

    def end(self):
        for copy in self.copies:
            copy.wait()
        self.own.wait()

    @staticmethod
    def scratch(dps):
        dma = pltpu.SemaphoreType.DMA
        return [dma((dps - 1,)), dma((dps - 1,)), dma]


def halves():
    lane = lax.broadcasted_iota(jnp.int32, (1, 128), 1)
    return lane, (lane < HEAD_DIM, lane >= HEAD_DIM)


def reversing(
    ways, grads_ref, out_ref, qkv_ref, lse_ref, table_ref, w_ref, attn_ref, att_ref, both_ref, *rest
):
    dps = ways[1]
    part_ref, rows_ref, bias_ref, outs_ref, swapped_ref = rest[:5]
    swap = SwapDp(dps, both_ref, swapped_ref, *rest[5:8])
    pg_ref, grad_ref = rest[8:10]
    dp = lax.axis_index("dp")
    meet([{"dp": lax.rem(dp + step, dps)} for step in range(1, dps)])
    length, wide = grads_ref.shape
    group = out_ref.shape[0]
    share = outs_ref.shape[2]
    step = min(256, wide)
    swap.begin()
    scale = HEAD_DIM ** (-0.5)
    size = min(256, length)
    tile = min(256, group)

    @pl.loop(0, group // tile)
    def _(at):
        columns = pl.ds(pl.multiple_of(at * tile, tile), tile)
        grad_ref[:, columns] = contract_cols(grads_ref[...], out_ref[columns, :]).astype(
            grad_ref.dtype
        )

    _, sides = halves()
    triangle = lax.broadcasted_iota(jnp.int32, (size, size), 0) <= lax.broadcasted_iota(
        jnp.int32, (size, size), 1
    )

    @pl.loop(0, group // 128)
    def _(at):
        base = pl.multiple_of(at * 128, 128)
        query_lanes, key_lanes, value_lanes = (
            pl.ds(third * group + base, 128) for third in range(3)
        )
        key_sums = [[None] * (length // size) for _ in range(2)]
        value_sums = [[None] * (length // size) for _ in range(2)]
        for block in range(length // size):
            rows = pl.ds(block * size, size)
            seen = (block + 1) * size
            query = qkv_ref[rows, query_lanes]
            key = qkv_ref[pl.ds(0, seen), key_lanes]
            value = qkv_ref[pl.ds(0, seen), value_lanes]
            grad = grad_ref[rows, pl.ds(base, 128)]
            query_sums = []
            for half in range(2):
                mine = jnp.where(sides[half], query, jnp.zeros_like(query))
                given = jnp.where(sides[half], grad, jnp.zeros_like(grad))
                scores = contract_cols(key, mine) * scale
                total = lse_ref[pl.ds(2 * at + half, 1), rows]
                probs = jnp.exp(scores - total)
                last = jnp.where(triangle, probs[block * size :], 0.0)
                probs = jnp.concatenate([probs[: block * size], last], 0) if block else last
                probs_grad = contract_cols(value, given)
                tilt = jnp.sum(probs * probs_grad, axis=0, keepdims=True)
                scores_grad = (probs * (probs_grad - tilt)).astype(BF16)
                probs_low = probs.astype(BF16)
                query_sums.append(contract_rows(scores_grad, key))
                for part in range(block + 1):
                    cut = slice(part * size, (part + 1) * size)
                    for sums, left, right in (
                        (key_sums, scores_grad, query),
                        (value_sums, probs_low, grad),
                    ):
                        more = dot(left[cut], right)
                        held = sums[half][part]
                        sums[half][part] = more if held is None else held + more
            total = (jnp.where(sides[0], query_sums[0], query_sums[1]) * scale).astype(BF16)
            table = table_ref.at[:, rows]
            pg_ref[rows, query_lanes] = turn_lanes(total.astype(F32), table, -1.0).astype(BF16)
        for part in range(length // size):
            rows = pl.ds(part * size, size)
            total = jnp.where(sides[0], key_sums[0][part], key_sums[1][part]) * scale
            table = table_ref.at[:, rows]
            total = total.astype(BF16).astype(F32)
            pg_ref[rows, key_lanes] = turn_lanes(total, table, -1.0).astype(BF16)
            total = jnp.where(sides[0], value_sums[0][part], value_sums[1][part])
            pg_ref[rows, value_lanes] = total.astype(BF16)

    bias_ref[...] = jnp.zeros(bias_ref.shape, F32)

    @pl.loop(0, length // CHUNK)
    def _(at):
        here = pl.ds(pl.multiple_of(at * CHUNK, CHUNK), CHUNK)
        bias_ref[0:1, :] += jnp.sum(pg_ref[here, :].astype(F32), axis=0, keepdims=True)

    @pl.loop(0, wide // step)
    def _(at):
        columns = pl.ds(pl.multiple_of(at * step, step), step)
        part_ref[:, columns] = contract_cols(pg_ref[...], w_ref[columns, :]).astype(part_ref.dtype)
        rows_ref[columns, :] = contract_rows(attn_ref[:, columns], pg_ref[...]).astype(
            rows_ref.dtype
        )

    @pl.loop(0, wide // step)
    def _(at):
        columns = pl.ds(pl.multiple_of(at * step, step), step)
        value = contract_rows(att_ref[...], grads_ref[:, columns]).astype(outs_ref.dtype)
        outs_ref[:, 0, :, columns] = value.reshape(dps, share, step)

    swap.end()


def reverse_all(ways, grads, out_full, qkv, lse, table, qkv_full, attn_all, attended, both, tag):
    length, wide = grads.shape
    group = out_full.shape[0]
    vmem, anywhere = (pl.BlockSpec(memory_space=space) for space in (pltpu.VMEM, pl.ANY))
    return pl.pallas_call(
        functools.partial(reversing, ways),
        out_shape=(
            jax.ShapeDtypeStruct((length, wide), BF16),
            jax.ShapeDtypeStruct((wide, 3 * group), BF16),
            jax.ShapeDtypeStruct((8, 3 * group), F32),
            jax.ShapeDtypeStruct((ways[1], 1, group // ways[1], wide), BF16),
            jax.ShapeDtypeStruct(both.shape, BF16),
        ),
        in_specs=[vmem] * 9,
        out_specs=(vmem,) * 4 + (anywhere,),
        scratch_shapes=SwapDp.scratch(ways[1])
        + [pltpu.VMEM((length, 3 * group), BF16), pltpu.VMEM((length, group), BF16)],
        cost_estimate=lasting(45),
        compiler_params=pltpu.CompilerParams(
            collective_id=tag, has_side_effects=True, vmem_limit_bytes=60 * 2**20
        ),
    )(grads, out_full, qkv, lse, table, qkv_full, attn_all, attended, both)


def closing(ways, w_ref, g_ref, sums_ref, x_ref, gain_ref, resid_ref, both_ref, o_ref, *rest):
    seqs, dps = ways
    qkv_ref, grad_ref, tiny_ref, gate_ref, up_ref, shard_ref = rest[:6]
    rest = rest[1:]
    plane = Plane(seqs, g_ref, *rest[5:9])
    line = LineSum(dps, lambda owner: w_ref.at[:, owner], *rest[9:15])
    landed, mine, near, far, part_sum = rest[15:20]
    swap_s, swap_r, near_s, near_r, far_s, far_r = rest[20:26]
    outs = LineSum(dps, lambda owner: o_ref.at[owner], *rest[26:32])
    seq, dp = lax.axis_index("seq"), lax.axis_index("dp")
    seq_peers, dp_peers = meet_cross(ways)
    line.begin()
    plane.begin()
    line.lead()
    outs.begin()
    outs.lead()
    plane.relay()
    line.step(0)
    plane.end()
    part_sum[...] = sums_ref[...]
    gain = gain_ref[...]

    def one(here):
        grad = plane.total(here)
        normed, inverse = normalize(x_ref[here, :].astype(F32))
        part_sum[0:1, :] += jnp.sum(grad * normed, axis=0, keepdims=True)
        part_sum[1:2, :] += jnp.sum(grad, axis=0, keepdims=True)
        grad_ref[here, :] = (
            resid_ref[here, :] + norm_back(grad, normed, inverse, gain)
        ).astype(grad_ref.dtype)

    by_chunks(x_ref.shape[0], one)
    wide = x_ref.shape[1]
    nears = [
        push(part_sum, near.at[seq], near_s, near_r, at, {"seq": peer})
        for at, peer in enumerate(seq_peers)
    ]
    near[seq] = part_sum[...]
    line.step(1)
    for copy in nears:
        copy.wait()
    far[dp] = jnp.sum(near[...], axis=0)
    units = gate_ref.shape[1] // (seqs * dps)
    for at, weight in enumerate((gate_ref, up_ref)):
        for source in range(seqs):
            for owner in range(dps):
                weight[:, pl.ds((source * dps + owner) * units, units)] = both_ref[
                    owner, :, pl.ds((at * seqs + source) * units, units)
                ].astype(F32)
    fars = [
        push(far.at[dp], far.at[dp], far_s, far_r, at, {"dp": peer})
        for at, peer in enumerate(dp_peers)
    ]
    for at in range(2, dps // 2):
        line.step(at)
    line.end()
    for source in range(seqs):

        def three(here, source=source):
            mine[source, here] = line.total(source, here).astype(mine.dtype)

        by_chunks(mine.shape[1], three)
    swaps = [
        push(mine.at[peer], landed.at[seq], swap_s, swap_r, at, {"seq": peer})
        for at, peer in enumerate(seq_peers)
    ]
    landed[seq] = mine[seq]
    for at in range(dps // 2):
        outs.step(at)
    for copy in fars:
        copy.wait()
    tiny_ref[...] = jnp.sum(far[...], axis=0)
    for copy in swaps:
        copy.wait()
    group = w_ref.shape[3] // 3
    for source in range(seqs):
        for third in range(3):
            qkv_ref[:, pl.ds(third * wide + source * group, group)] = landed[
                source, :, pl.ds(third * group, group)
            ].astype(F32)
    outs.end()

    def last(here):
        shard_ref[here, :] = outs.total(0, here)

    by_chunks(shard_ref.shape[0], last)
    line.drain()
    outs.drain()


def close_all(ways, qkv_rows, attn_part, sums, inputs, gain, resid, both, out_rows, tag):
    seqs, dps = ways
    part = qkv_rows.shape[0] // (seqs * dps)
    wide3 = qkv_rows.shape[1]
    rows, wide = inputs.shape
    dma = pltpu.SemaphoreType.DMA
    vmem = pl.BlockSpec(memory_space=pltpu.VMEM)
    return pl.pallas_call(
        functools.partial(closing, ways),
        out_shape=(
            jax.ShapeDtypeStruct((part, 3 * wide), F32),
            jax.ShapeDtypeStruct((rows, wide), BF16),
            jax.ShapeDtypeStruct(sums.shape, F32),
            jax.ShapeDtypeStruct((part, dps * both.shape[2] // 2), F32),
            jax.ShapeDtypeStruct((part, dps * both.shape[2] // 2), F32),
            jax.ShapeDtypeStruct((part, wide), F32),
        ),
        in_specs=[vmem] * 8,
        out_specs=(vmem,) * 6,
        scratch_shapes=Plane.scratch(seqs, rows, wide, BF16)
        + LineSum.scratch(dps, (seqs, part, wide3), BF16)
        + [
            pltpu.VMEM((seqs, part, wide3), BF16),
            pltpu.VMEM((seqs, part, wide3), BF16),
            pltpu.VMEM((seqs,) + sums.shape, F32),
            pltpu.VMEM((dps,) + sums.shape, F32),
            pltpu.VMEM(sums.shape, F32),
            dma((seqs - 1,)),
            dma((seqs - 1,)),
            dma((seqs - 1,)),
            dma((seqs - 1,)),
            dma((dps - 1,)),
            dma((dps - 1,)),
        ]
        + LineSum.scratch(dps, out_rows.shape[1:], BF16),
        cost_estimate=lasting(75),
        compiler_params=pltpu.CompilerParams(collective_id=tag, has_side_effects=True),
    )(
        qkv_rows.reshape(seqs, dps, part, wide3),
        attn_part.reshape(seqs, rows, wide),
        sums,
        inputs,
        gain,
        resid,
        both,
        out_rows,
    )


def front(
    ways,
    qkv_weight_ref,
    in_ref,
    small_ref,
    gate_ref,
    up_ref,
    out_weight_ref,
    grad_ref,
    table_ref,
    w_ref,
    attn_ref,
    qkv_ref,
    att_ref,
    lse_ref,
    out_ref,
    vec_ref,
    resid_ref,
    all_ref,
    grads_ref,
    both_ref,
    *rest,
):
    seqs, dps = ways
    chips, count = dps // 2, seqs * dps
    rest = list(rest)

    def take(size):
        taken = rest[:size]
        del rest[:size]
        return taken

    x_ref, given_ref, bias_ref, cut_ref, swapped_ref, branch_ref, own_ref = take(7)
    gathered = PlaneGather(seqs, in_ref, x_ref, *take(3))
    outs = LineGather(dps, out_weight_ref, out_ref, *take(5))
    swap = SwapDp(dps, cut_ref, swapped_ref, *take(3))
    plane = Plane(seqs, branch_ref, *take(4))
    moved = LineGather(dps, own_ref, all_ref, *take(5))
    grads = LineGather(dps, grad_ref, grads_ref, *take(5))
    gates = PlaneGather(seqs, swapped_ref, both_ref, *take(3))
    swap_s, swap_r, line_s, line_r, pair_s, pair_r, small_s, small_r, own_sem = take(9)
    seq, dp = lax.axis_index("seq"), lax.axis_index("dp")
    _, chip, core, ends, sides, sibling = line_place(dps)
    me = seq * dps + dp
    part, group = qkv_weight_ref.shape[0], w_ref.shape[1] // 3
    rows, width = in_ref.shape
    length = rows * seqs
    barrier = pltpu.get_barrier_semaphore()

    def other(step):
        at = lax.rem(me + step, count)
        return {"seq": at // dps, "dp": lax.rem(at, dps)}

    @pl.loop(1, count)
    def _(step):
        pl.semaphore_signal(barrier, inc=1, device_id=other(step), device_id_type=MESH)

    pl.semaphore_wait(barrier, count - 1)

    def block(source, owner):
        return w_ref.at[pl.ds(pl.multiple_of((source * dps + owner) * part, part), part), :]

    def piece(source, third):
        here = pl.ds(pl.multiple_of((source * dps + dp) * part, part), part)
        return w_ref.at[here, pl.ds(third * group, group)]

    def columns(target, third):
        at = pl.multiple_of(third * width + target * group, 128)
        return qkv_weight_ref.at[:, pl.ds(at, group)]

    swaps = []
    for step in range(1, seqs):
        target = lax.rem(seq + step, seqs)
        for third in range(3):
            at = 3 * (step - 1) + third
            swaps.append(
                push(
                    columns(target, third),
                    piece(seq, third),
                    swap_s,
                    swap_r,
                    at,
                    {"seq": target},
                )
            )
    owns = [
        pltpu.make_async_copy(columns(seq, third), piece(seq, third), own_sem.at[third])
        for third in range(3)
    ]
    for own in owns:
        own.start()

    def small_copy(step):
        return remote(
            small_ref, given_ref.at[me], small_s.at[step - 1], small_r.at[step - 1], other(step)
        )

    @pl.loop(1, count)
    def _(step):
        small_copy(step).start()

    given_ref[me] = small_ref[...]
    gathered.begin()

    def onward(side, hop, source, owner_chip):
        part_of = block(source[1], 2 * owner_chip + core)
        at = (side, hop, source[0])
        return remote(part_of, part_of, line_s.at[at], line_r.at[at], sides[side])

    def share(source, owner_chip, owner_core):
        part_of = block(source[1], 2 * owner_chip + owner_core)
        at = (owner_chip, source[0])
        return remote(part_of, part_of, pair_s.at[at], pair_r.at[at], sibling)

    sources = [(back, lax.rem(seq - back + seqs, seqs)) for back in range(seqs)]
    for source in sources:
        if source[0] == 0:
            for own in owns:
                own.wait()
        else:
            for third in range(3):
                swaps[3 * (source[0] - 1) + third].wait_recv()
        for side in range(2):

            @pl.when(ends[side])
            def _(side=side, source=source):
                onward(side, 0, source, chip).start()

        share(source, chip, core).start()
    gathered.relay()

    def pass_on(hop):
        for source in sources:
            for side in range(2):
                origin = chip - 1 - hop if side == 0 else chip + 1 + hop
                there = origin >= 0 if side == 0 else origin < chips

                @pl.when(there)
                def _(side=side, source=source, origin=origin):
                    onward(side, hop, source, origin).wait_recv()
                    share(source, origin, core).start()

                if hop < chips - 2:

                    @pl.when(jnp.logical_and(there, ends[side]))
                    def _(side=side, source=source, origin=origin):
                        onward(side, hop + 1, source, origin).start()

    units = gate_ref.shape[1] // count
    for at, weight in enumerate((gate_ref, up_ref)):
        for source in range(seqs):
            for owner in range(dps):
                cut_ref[owner, :, pl.ds((at * seqs + source) * units, units)] = weight[
                    :, pl.ds((source * dps + owner) * units, units)
                ]
    pass_on(0)

    @pl.loop(1, count)
    def _(step):
        small_copy(step).wait()

    lane, sides_of = halves()
    per = 128 // part

    def row_of(pick):
        value = jnp.zeros((1, 128), F32)
        for unit in range(per):
            found = pick(unit)
            found = pltpu.roll(found, unit * part, 1) if unit else found
            mask = (lane >= unit * part) & (lane < (unit + 1) * part)
            value = jnp.where(mask, found, value)
        return value

    for kind in range(4):
        for chunk in range(width // 128):
            vec_ref[kind : kind + 1, pl.ds(chunk * 128, 128)] = row_of(
                lambda unit, kind=kind, chunk=chunk: given_ref[chunk * per + unit, kind : kind + 1]
            )
    for chunk in range(3 * group // 128):
        third, inner = chunk * 128 // group, chunk * 128 % group // part
        first = third * count + seq * dps + inner

        def pick(unit, first=first):
            at = first + unit
            return given_ref[at // 3, pl.ds(4 + lax.rem(at, 3), 1)]

        bias_ref[0:1, pl.ds(chunk * 128, 128)] = row_of(pick)
    for hop in range(1, chips - 1):
        pass_on(hop)
    outs.begin()
    gathered.end()
    gain_one, shift_one = vec_ref[0:1, :], vec_ref[1:2, :]

    for source in range(seqs):

        def norm(here, source=source):
            normed, _ = normalize(x_ref[source, here, :].astype(F32))
            at = pl.ds(pl.multiple_of(source * rows + here.start, CHUNK), CHUNK)
            attn_ref[at, :] = (normed * gain_one + shift_one).astype(attn_ref.dtype)

        by_chunks(rows, norm)
    for owner in range(chips):
        for source in sources:
            share(source, owner, 1 - core).wait_recv()
    tile = min(256, group)

    def product(at):
        here = pl.ds(pl.multiple_of(at * tile, tile), tile)
        return here, dot(attn_ref[...], w_ref[:, here]) + bias_ref[0:1, here]

    @pl.loop(0, 2 * group // tile)
    def _(at):
        _, value = product(at)
        for half in range(tile // 128):
            turned = turn_lanes(value[:, half * 128 : (half + 1) * 128], table_ref, 1.0)
            here = pl.ds(pl.multiple_of(at * tile + half * 128, 128), 128)
            qkv_ref[:, here] = turned.astype(qkv_ref.dtype)

    outs.hop(0)

    @pl.loop(2 * group // tile, 3 * group // tile)
    def _(at):
        here, value = product(at)
        qkv_ref[:, here] = value.astype(qkv_ref.dtype)

    for hop in range(1, chips - 1):
        outs.hop(hop)
    swap.begin()
    scale = HEAD_DIM ** (-0.5)
    size = min(256, length)
    triangle = lax.broadcasted_iota(jnp.int32, (size, size), 1) <= lax.broadcasted_iota(
        jnp.int32, (size, size), 0
    )

    @pl.loop(0, group // 128)
    def _(at):
        base = pl.multiple_of(at * 128, 128)
        for part_at in range(length // size):
            here = pl.ds(part_at * size, size)
            seen = (part_at + 1) * size
            query = qkv_ref[here, pl.ds(base, 128)]
            key = qkv_ref[pl.ds(0, seen), pl.ds(group + base, 128)]
            value = qkv_ref[pl.ds(0, seen), pl.ds(2 * group + base, 128)]
            mixed = []
            for half in range(2):
                mine = jnp.where(sides_of[half], query, jnp.zeros_like(query))
                scores = contract_cols(mine, key) * scale
                last = jnp.where(triangle, scores[:, part_at * size :], -jnp.inf)
                if part_at:
                    scores = jnp.concatenate([scores[:, : part_at * size], last], 1)
                else:
                    scores = last
                largest = jnp.max(scores, axis=1, keepdims=True)
                exponent = jnp.exp(scores - largest)
                totals = jnp.sum(exponent, axis=1, keepdims=True)
                probs = (exponent * (1.0 / totals)).astype(value.dtype)
                mixed.append(dot(probs, value))
                lse_ref[here, :] = jnp.where(
                    lane == 2 * at + half, largest + jnp.log(totals), lse_ref[here, :]
                )
            att_ref[here, pl.ds(base, 128)] = jnp.where(sides_of[0], mixed[0], mixed[1]).astype(
                att_ref.dtype
            )

    outs.end()
    step = min(256, width)

    @pl.loop(0, width // step)
    def _(at):
        here = pl.ds(pl.multiple_of(at * step, step), step)
        value = jnp.zeros((length, step), F32)
        for owner in range(dps):
            value = value + dot(att_ref[:, pl.ds(owner * part, part)], out_ref[owner, :, here])
        for source in range(seqs):
            branch_ref[source, :, here] = value[source * rows : (source + 1) * rows].astype(
                branch_ref.dtype
            )

    plane.begin()
    grads.begin()
    plane.relay()
    plane.end()
    swap.end()
    gates.begin()
    gain_two, shift_two = vec_ref[2:3, :], vec_ref[3:4, :]

    def one(here):
        resid = in_ref[here, :].astype(F32) + plane.total(here)
        resid_ref[here, :] = resid
        normed, _ = normalize(resid)
        own_ref[here, :] = (normed * gain_two + shift_two).astype(own_ref.dtype)

    by_chunks(rows, one)
    moved.begin()
    for hop in range(chips - 1):
        grads.hop(hop)
        if hop == min(1, chips - 2):
            gates.relay()
        moved.hop(hop)
    grads.end()
    moved.end()
    gates.end()

    for swapped in swaps:
        swapped.wait_send()
    for hop in range(chips - 1):
        for source in sources:
            for side in range(2):
                origin = chip - hop if side == 0 else chip + hop
                there = origin >= 0 if side == 0 else origin < chips

                @pl.when(jnp.logical_and(there, ends[side]))
                def _(side=side, hop=hop, source=source, origin=origin):
                    onward(side, hop, source, origin).wait_send()

    for owner in range(chips):
        for source in sources:
            share(source, owner, core).wait_send()


def front_all(ways, qkv_weight, inputs, small, gate, up, out_weight, grad_out, table, tag):
    seqs, dps = ways
    chips, count = dps // 2, seqs * dps
    part, width = out_weight.shape
    rows = inputs.shape[0]
    length, group, cols = rows * seqs, width // seqs, 2 * gate.shape[1] // dps
    dma = pltpu.SemaphoreType.DMA
    vmem, anywhere = (pl.BlockSpec(memory_space=space) for space in (pltpu.VMEM, pl.ANY))

    def made(dtype, *shape):
        return jax.ShapeDtypeStruct(shape, dtype)

    return pl.pallas_call(
        functools.partial(front, ways),
        out_shape=(
            made(BF16, width, 3 * group),
            made(BF16, length, width),
            made(BF16, length, 3 * group),
            made(BF16, length, group),
            made(F32, length, 128),
            made(BF16, dps, part, width),
            made(F32, 8, width),
            made(F32, rows, width),
            made(BF16, dps, rows, width),
            made(BF16, dps, rows, width),
            made(BF16, seqs, dps, part, cols),
        ),
        in_specs=[vmem] * 8,
        out_specs=(vmem,) * 8 + (anywhere,) * 3,
        scratch_shapes=[
            pltpu.VMEM((seqs, rows, width), BF16),
            pltpu.VMEM((count, 8, 128), F32),
            pltpu.VMEM((8, 3 * group), F32),
            pltpu.VMEM((dps, part, cols), BF16),
            pltpu.VMEM((dps, part, cols), BF16),
            pltpu.VMEM((seqs, rows, width), BF16),
            pltpu.VMEM((rows, width), BF16),
        ]
        + PlaneGather.scratch(seqs)
        + LineGather.scratch(dps)
        + SwapDp.scratch(dps)
        + Plane.scratch(seqs, rows, width, BF16)
        + LineGather.scratch(dps)
        + LineGather.scratch(dps)
        + PlaneGather.scratch(seqs)
        + [
            dma((3 * (seqs - 1),)),
            dma((3 * (seqs - 1),)),
            dma((2, chips - 1, seqs)),
            dma((2, chips - 1, seqs)),
            dma((chips, seqs)),
            dma((chips, seqs)),
            dma((count - 1,)),
            dma((count - 1,)),
            dma((3,)),
        ],
        cost_estimate=lasting(180),
        compiler_params=pltpu.CompilerParams(
            collective_id=tag, has_side_effects=True, vmem_limit_bytes=60 * 2**20
        ),
    )(qkv_weight, inputs, small, gate, up, out_weight, grad_out, table)


def shards(
    ways,
    inputs,
    first_gain,
    first_shift,
    qkv_weight,
    qkv_bias,
    out_weight,
    second_gain,
    second_shift,
    gate_weight,
    up_weight,
    down_weight,
    out_cotangent,
):
    seqs, dps = ways
    width = inputs.shape[2]
    rows = inputs.shape[1]
    length = rows * seqs
    part = width // (seqs * dps)
    units = down_weight.shape[0]
    group = width // seqs
    me_seq = lax.axis_index("seq")
    grad_out = out_cotangent[0]

    small = [item[None] for item in (first_gain, first_shift, second_gain, second_shift)]
    small = jnp.concatenate(small + [qkv_bias.reshape(3, part)]).astype(F32)
    small = jnp.pad(small, ((0, 1), (0, 128 - part)))
    table = tables(length)
    down_full = gather(down_weight, "seq")
    (
        qkv_full,
        attn_all,
        qkv,
        attended,
        log_total,
        out_full,
        vectors,
        residual,
        mlp_all,
        grad_all,
        gate_up,
    ) = front_all(
        ways,
        qkv_weight,
        inputs[0],
        small,
        gate_weight,
        up_weight,
        out_weight,
        grad_out,
        table,
        0,
    )
    out_full = out_full.reshape(group, width)
    gain_one, gain_two = vectors[0:1], vectors[2:3]
    mlp_all = mlp_all.reshape(dps * rows, width)
    grad_all = grad_all.reshape(dps * rows, width)
    gate_up = gate_up.reshape(width, 2 * seqs * units)
    wide = seqs * units

    both = dot(mlp_all, gate_up)
    gate_value = both[:, :wide]
    up_value = both[:, wide:]
    sigmoid_gate = jax.nn.sigmoid(gate_value)
    activated = gate_value * sigmoid_gate
    hidden = (activated * up_value).astype(BF16)

    hidden_grad = contract_cols(grad_all, down_full)
    gate_grad = (
        hidden_grad * up_value * (sigmoid_gate * (1.0 + gate_value * (1.0 - sigmoid_gate)))
    ).astype(BF16)
    up_grad = (hidden_grad * activated).astype(BF16)
    both_grad = jnp.concatenate([gate_grad, up_grad], 1)
    mlp_part = contract_cols(both_grad, gate_up).astype(BF16)
    residual_grad, branch_all, sums, layer_out, both_rows, down_rows = turn_all(
        ways,
        mlp_part,
        residual,
        gain_two,
        grad_out,
        hidden,
        down_full,
        mlp_all,
        both_grad,
        grad_all,
        2,
    )
    down_shard = scatter_sum(down_rows, "seq").astype(F32)

    attn_part, qkv_rows, bias_term, out_rows, both_rows = reverse_all(
        ways,
        branch_all,
        out_full,
        qkv,
        log_total.T,
        table,
        qkv_full,
        attn_all,
        attended,
        both_rows.reshape(dps, part, 2 * seqs * units),
        5,
    )
    bias_term = bias_term[0].reshape(3, 1, group)
    here = (jnp.arange(seqs, dtype=jnp.int32) == me_seq).astype(F32)[None, :, None]
    bias_term = jnp.pad((bias_term * here).reshape(3, width), ((4, 1), (0, 0)))
    sums = sums + bias_term
    qkv_shard, input_grad, tiny, gate_shard, up_shard, out_shard = close_all(
        ways,
        qkv_rows,
        attn_part,
        sums,
        inputs[0],
        gain_one,
        residual_grad,
        both_rows,
        out_rows,
        3,
    )
    me = me_seq * dps + lax.axis_index("dp")
    mine = lax.dynamic_slice_in_dim(tiny, me * part, part, 1)
    bias_shard = lax.dynamic_slice_in_dim(tiny[4:7].reshape(-1), me * 3 * part, 3 * part, 0)

    return (
        layer_out[None],
        input_grad[None],
        mine[0],
        mine[1],
        qkv_shard,
        bias_shard,
        out_shard,
        mine[2],
        mine[3],
        gate_shard,
        up_shard,
        down_shard,
    )


def solution(mesh):
    split = ("seq", "dp")
    tokens = P("dp", "seq", None)
    in_specs = (
        tokens,
        P(split),
        P(split),
        P(split, None),
        P(split),
        P(split, None),
        P(split),
        P(split),
        P(split, None),
        P(split, None),
        P(split, None),
        tokens,
    )
    out_specs = (
        tokens,
        tokens,
        P(split),
        P(split),
        P(split, None),
        P(split),
        P(split, None),
        P(split),
        P(split),
        P(split, None),
        P(split, None),
        P(split, None),
    )
    ways = (mesh.shape["seq"], mesh.shape["dp"])

    def local(*args):
        return shards(ways, *args)

    return jax.shard_map(local, mesh=mesh, in_specs=in_specs, out_specs=out_specs, check_vma=False)
```

```python
import functools

import jax
import jax.numpy as jnp
from jax import lax
from jax.experimental import pallas as pl
from jax.experimental.pallas import tpu as pltpu
from jax.sharding import PartitionSpec as P


HEAD_DIM = 64
ROT = 16
F32 = jnp.float32
BF16 = jnp.bfloat16


def normalize(values):
    center = values - jnp.mean(values, axis=-1, keepdims=True)
    variance = jnp.mean(center * center, axis=-1, keepdims=True)
    inverse = lax.rsqrt(variance + 1e-05)
    return (center * inverse, inverse)


def norm_back(grad_normed, normed, inverse, gain):
    scaled = grad_normed * gain
    centered = scaled - jnp.mean(scaled, axis=-1, keepdims=True)
    return inverse * (centered - normed * jnp.mean(scaled * normed, axis=-1, keepdims=True))


def dot(left, right):
    return jnp.dot(left, right, preferred_element_type=F32)


def contract_rows(left, right):
    return lax.dot_general(left, right, (((0,), (0,)), ((), ())), preferred_element_type=F32)


def contract_cols(left, right):
    return lax.dot_general(left, right, (((1,), (1,)), ((), ())), preferred_element_type=F32)


def tables(length):
    half_rot = ROT // 2
    lane = lax.rem(lax.broadcasted_iota(jnp.int32, (length, 128), 1), HEAD_DIM)
    position = lax.broadcasted_iota(jnp.int32, (length, 128), 0).astype(F32)
    freqs = 10000.0 ** (-(2.0 * lax.rem(lane, half_rot).astype(F32)) / ROT)
    angles = position * freqs
    cosine, sine = jnp.cos(angles), jnp.sin(angles)
    return jnp.stack(
        [
            jnp.where(lane < ROT, cosine, 1.0),
            jnp.where(lane < half_rot, -sine, 0.0),
            jnp.where((lane >= half_rot) & (lane < ROT), sine, 0.0),
        ]
    )


def turn_lanes(value, table_ref, sign):
    half_rot = ROT // 2
    ahead, behind = pltpu.roll(value, 128 - half_rot, 1), pltpu.roll(value, half_rot, 1)
    return value * table_ref[0] + sign * (ahead * table_ref[1] + behind * table_ref[2])


def gather(value, axis):
    return lax.all_gather(value, axis, axis=0, tiled=True)


def scatter_sum(value, axis):
    return lax.psum_scatter(value, axis, scatter_dimension=0, tiled=True)


MESH = pl.DeviceIdType.MESH


def lasting(micros):
    return pl.CostEstimate(flops=0, transcendentals=0, bytes_accessed=int(micros * 3.0e6))


def meet(peers):
    barrier = pltpu.get_barrier_semaphore()
    for peer in peers:
        pl.semaphore_signal(barrier, inc=1, device_id=peer, device_id_type=MESH)
    pl.semaphore_wait(barrier, len(peers))


def push(source, target, send, recv, at, peer):
    copy = pltpu.make_async_remote_copy(
        src_ref=source,
        dst_ref=target,
        send_sem=send.at[at],
        recv_sem=recv.at[at],
        device_id=peer,
        device_id_type=MESH,
    )
    copy.start()
    return copy


def corners():
    me = lax.axis_index("seq")
    high, low = me // 2, lax.rem(me, 2)
    across = high * 2 + (1 - low)
    along = (1 - high) * 2 + low
    return me, across, along, 3 - me


def remote(source, target, send, recv, peer):
    return pltpu.make_async_remote_copy(
        src_ref=source,
        dst_ref=target,
        send_sem=send,
        recv_sem=recv,
        device_id=peer,
        device_id_type=MESH,
    )


def line_place(dps):
    dp = lax.axis_index("dp")
    chip, core = dp // 2, lax.rem(dp, 2)
    chips = dps // 2
    ends = (chip + 1 < chips, chip >= 1)
    sides = ({"dp": lax.rem(dp + 2, dps)}, {"dp": lax.rem(dp - 2 + dps, dps)})
    return chips, chip, core, ends, sides, {"dp": 2 * chip + (1 - core)}


class Plane:

    def __init__(self, count, x_ref, pair, got, send, recv):
        self.count, self.x, self.pair, self.got = count, x_ref, pair, got
        self.send, self.recv = send, recv
        self.square = count == 4

    def begin(self, make=None):
        x, got, send, recv = self.x, self.got, self.send, self.recv
        me = lax.axis_index("seq")
        if self.square:
            _, across, along, far = corners()
            half = x.shape[1] // 2
            top, low = pl.ds(0, half), pl.ds(half, half)
            to_across, to_along = {"seq": across}, {"seq": along}
            targets = (far, across, along)
            plan = [
                (0, x.at[far, top], self.pair.at[0], to_across),
                (0, x.at[far, low], self.pair.at[1], to_along),
                (1, x.at[across, top], got.at[0, top], to_across),
                (2, x.at[along, low], got.at[1, low], to_along),
            ]
        else:
            targets = [lax.rem(me + step, self.count) for step in range(1, self.count)]
            plan = [
                (at, x.at[target], got.at[at], {"seq": target})
                for at, target in enumerate(targets)
            ]
        self.copies = [
            remote(source, target, send.at[at], recv.at[at], peer)
            for at, (_, source, target, peer) in enumerate(plan)
        ]
        if make is None:
            for copy in self.copies:
                copy.start()
            return

        @pl.loop(0, self.count)
        def _(at):
            block = me
            for step, target in enumerate(targets):
                block = jnp.where(at == step, target, block)
            make(at, block)
            for step in range(len(targets)):

                @pl.when(at == step)
                def _(step=step):
                    for copy, item in zip(self.copies, plan):
                        if item[0] == step:
                            copy.start()

    def relay(self):
        if not self.square:
            return
        x, pair, got, send, recv = self.x, self.pair, self.got, self.send, self.recv
        _, across, along, _ = corners()
        half = x.shape[1] // 2
        top, low = pl.ds(0, half), pl.ds(half, half)
        self.copies[0].wait_recv()
        pair[2] = (pair[0].astype(F32) + x[along, top].astype(F32)).astype(pair.dtype)
        self.copies.append(push(pair.at[2], got.at[1, top], send, recv, 4, {"seq": along}))
        self.copies[1].wait_recv()
        pair[3] = (pair[1].astype(F32) + x[across, low].astype(F32)).astype(pair.dtype)
        self.copies.append(push(pair.at[3], got.at[0, low], send, recv, 5, {"seq": across}))

    def end(self):
        for at, copy in enumerate(self.copies):
            copy.wait_send()
            if not self.square or at > 1:
                copy.wait_recv()

    def total(self, rows):
        value = self.x[lax.axis_index("seq"), rows].astype(F32)
        for at in range(2 if self.square else self.count - 1):
            value = value + self.got[at, rows].astype(F32)
        return value

    @staticmethod
    def scratch(count, rows, wide, dtype):
        slots = 6 if count == 4 else count - 1
        return [
            pltpu.VMEM((4, rows // 2, wide), dtype),
            pltpu.VMEM((2 if count == 4 else count - 1, rows, wide), dtype),
            pltpu.SemaphoreType.DMA((slots,)),
            pltpu.SemaphoreType.DMA((slots,)),
        ]


class LineSum:

    def __init__(self, dps, block, pair, moving, line_s, line_r, pair_s, pair_r):
        self.block, self.pair, self.moving = block, pair, moving
        self.sems = (line_s, line_r, pair_s, pair_r)
        self.chips, self.chip, self.core, self.ends, self.sides, self.sibling = line_place(dps)
        self.pieces = pair.shape[1]

    def share(self, owner, owner_core, piece):
        at = (owner, piece)
        return remote(
            self.block(2 * owner + owner_core).at[piece],
            self.pair.at[at],
            self.sems[2].at[at],
            self.sems[3].at[at],
            self.sibling,
        )

    def onward(self, side, owner, piece):
        at = (side, owner, piece)
        return remote(
            self.pair.at[owner, piece],
            self.moving.at[at],
            self.sems[0].at[at],
            self.sems[1].at[at],
            self.sides[side],
        )

    def begin(self):
        order = [
            at for both in zip(range(self.chips - 1, -1, -1), range(self.chips)) for at in both
        ]
        for owner in dict.fromkeys(order):
            for piece in range(self.pieces):
                self.share(owner, 1 - self.core, piece).start()

    def add(self, owner, piece, side):
        own = self.block(2 * owner + self.core)

        def one(here):
            value = self.pair[owner, piece, here].astype(F32) + own[piece, here].astype(F32)
            if side is not None:
                value = value + self.moving[side, owner, piece, here].astype(F32)
            self.pair[owner, piece, here] = value.astype(self.pair.dtype)

        by_chunks(self.pair.shape[2], one)

    def lead(self):
        for at in range(self.chips):
            for piece in range(self.pieces):
                for side in range(2):
                    owner = self.chips - 1 - at if side == 0 else at
                    passing = self.chip < owner if side == 0 else self.chip > owner

                    @pl.when(jnp.logical_and(passing, jnp.logical_not(self.ends[1 - side])))
                    def _(side=side, owner=owner, piece=piece):
                        self.share(owner, self.core, piece).wait_recv()
                        self.add(owner, piece, None)
                        self.onward(side, owner, piece).start()

    def step(self, at):
        for piece in range(self.pieces):
            for side in range(2):
                owner = self.chips - 1 - at if side == 0 else at
                passing = self.chip < owner if side == 0 else self.chip > owner

                @pl.when(jnp.logical_and(passing, self.ends[1 - side]))
                def _(side=side, owner=owner, piece=piece):
                    self.share(owner, self.core, piece).wait_recv()
                    self.onward(side, owner, piece).wait_recv()
                    self.add(owner, piece, side)
                    self.onward(side, owner, piece).start()

    def end(self):
        for owner in range(self.chips):
            for piece in range(self.pieces):

                @pl.when(self.chip == owner)
                def _(owner=owner, piece=piece):
                    self.share(owner, self.core, piece).wait_recv()

                for side in range(2):

                    @pl.when(jnp.logical_and(self.chip == owner, self.ends[1 - side]))
                    def _(side=side, owner=owner, piece=piece):
                        self.onward(side, owner, piece).wait_recv()

        for side in range(2):

            @pl.when(jnp.logical_not(self.ends[1 - side]))
            def _(side=side):
                self.moving[side, self.chip] = jnp.zeros(self.moving.shape[2:], self.moving.dtype)

    def total(self, piece, here):
        own = self.block(2 * self.chip + self.core)
        value = own[piece, here].astype(F32) + self.pair[self.chip, piece, here].astype(F32)
        for side in range(2):
            value = value + self.moving[side, self.chip, piece, here].astype(F32)
        return value

    def drain(self):
        for owner in range(self.chips):
            for piece in range(self.pieces):
                for side in range(2):
                    passing = self.chip < owner if side == 0 else self.chip > owner

                    @pl.when(passing)
                    def _(side=side, owner=owner, piece=piece):
                        self.onward(side, owner, piece).wait_send()

                self.share(owner, 1 - self.core, piece).wait_send()

    @staticmethod
    def scratch(dps, shape, dtype):
        dma, chips, pieces = pltpu.SemaphoreType.DMA, dps // 2, shape[0]
        return [
            pltpu.VMEM((chips,) + shape, dtype),
            pltpu.VMEM((2, chips) + shape, dtype),
            dma((2, chips, pieces)),
            dma((2, chips, pieces)),
            dma((chips, pieces)),
            dma((chips, pieces)),
        ]


class PlaneGather:

    def __init__(self, count, x_ref, o_ref, send, recv, local):
        self.count, self.x, self.o = count, x_ref, o_ref
        self.send, self.recv, self.local = send, recv, local
        self.square = count == 4

    def begin(self):
        x, o, send, recv = self.x, self.o, self.send, self.recv
        me = lax.axis_index("seq")
        if self.square:
            _, across, along, _ = corners()
            half = x.shape[0] // 2
            top, low = pl.ds(0, half), pl.ds(half, half)
            to_across, to_along = {"seq": across}, {"seq": along}
            self.copies = [
                push(x.at[top], o.at[me, top], send, recv, 0, to_across),
                push(x.at[low], o.at[me, low], send, recv, 1, to_along),
                push(x.at[low], o.at[me, low], send, recv, 2, to_across),
                push(x.at[top], o.at[me, top], send, recv, 3, to_along),
            ]
        else:
            self.copies = [
                push(x, o.at[me], send, recv, step - 1, {"seq": lax.rem(me + step, self.count)})
                for step in range(1, self.count)
            ]
        self.own = pltpu.make_async_copy(x, o.at[me], self.local)
        self.own.start()

    def relay(self):
        if not self.square:
            return
        o, send, recv = self.o, self.send, self.recv
        _, across, along, _ = corners()
        half = self.x.shape[0] // 2
        top, low = pl.ds(0, half), pl.ds(half, half)
        self.copies[0].wait_recv()
        self.copies.append(
            push(o.at[across, top], o.at[across, top], send, recv, 4, {"seq": along})
        )
        self.copies[1].wait_recv()
        self.copies.append(
            push(o.at[along, low], o.at[along, low], send, recv, 5, {"seq": across})
        )

    def end(self):
        for at, copy in enumerate(self.copies):
            copy.wait_send()
            if not self.square or at > 1:
                copy.wait_recv()
        self.own.wait()

    @staticmethod
    def scratch(count):
        slots = 6 if count == 4 else count - 1
        dma = pltpu.SemaphoreType.DMA
        return [dma((slots,)), dma((slots,)), dma]


class LineGather:

    def __init__(self, dps, x_ref, o_ref, line_s, line_r, pair_s, pair_r, local):
        self.x, self.o, self.local = x_ref, o_ref, local
        self.sems = (line_s, line_r, pair_s, pair_r)
        self.chips, self.chip, self.core, self.ends, self.sides, self.sibling = line_place(dps)

    def onward(self, side, hop, owner, source=None):
        block = self.o.at[2 * owner + self.core]
        at = (side, hop)
        return remote(
            block if source is None else source,
            block,
            self.sems[0].at[at],
            self.sems[1].at[at],
            self.sides[side],
        )

    def share(self, owner, owner_core, source=None):
        block = self.o.at[2 * owner + owner_core]
        return remote(
            block if source is None else source,
            block,
            self.sems[2].at[owner],
            self.sems[3].at[owner],
            self.sibling,
        )

    def begin(self):
        for side in range(2):

            @pl.when(self.ends[side])
            def _(side=side):
                self.onward(side, 0, self.chip, self.x).start()

        self.share(self.chip, self.core, self.x).start()
        self.own = pltpu.make_async_copy(
            self.x, self.o.at[2 * self.chip + self.core], self.local
        )
        self.own.start()

    def hop(self, hop):
        for side in range(2):
            origin = self.chip - 1 - hop if side == 0 else self.chip + 1 + hop
            there = origin >= 0 if side == 0 else origin < self.chips

            @pl.when(there)
            def _(side=side, origin=origin):
                self.onward(side, hop, origin).wait_recv()

            if hop < self.chips - 2:

                @pl.when(jnp.logical_and(there, self.ends[side]))
                def _(side=side, origin=origin):
                    self.onward(side, hop + 1, origin).start()

            @pl.when(there)
            def _(origin=origin):
                self.share(origin, self.core).start()

    def end(self):
        self.own.wait()
        for hop in range(self.chips - 1):
            for side in range(2):
                origin = self.chip - hop if side == 0 else self.chip + hop
                there = origin >= 0 if side == 0 else origin < self.chips

                @pl.when(jnp.logical_and(there, self.ends[side]))
                def _(side=side, hop=hop, origin=origin):
                    self.onward(side, hop, origin).wait_send()

        for owner in range(self.chips):
            self.share(owner, self.core).wait_send()
            self.share(owner, 1 - self.core).wait_recv()

    @staticmethod
    def scratch(dps):
        dma, chips = pltpu.SemaphoreType.DMA, dps // 2
        return [dma((2, chips - 1)), dma((2, chips - 1)), dma((chips,)), dma((chips,)), dma]


CHUNK = 16


def by_chunks(rows, body):
    @pl.loop(0, rows // CHUNK)
    def _(at):
        body(pl.ds(pl.multiple_of(at * CHUNK, CHUNK), CHUNK))


def fetch(pairs, sems):
    copies = [
        pltpu.make_async_copy(source, target, sems.at[at])
        for at, (source, target) in enumerate(pairs)
    ]
    for copy in copies:
        copy.start()
    return copies


PIECES = 2


def by_pieces(rows, body):
    size = rows // PIECES
    for piece in range(PIECES):

        @pl.loop(0, size // CHUNK)
        def _(at, piece=piece):
            here = pl.multiple_of(at * CHUNK, CHUNK)
            body(pl.ds(pl.multiple_of(piece * size + here, CHUNK), CHUNK), piece, pl.ds(here, CHUNK))


def meet_cross(ways):
    seqs, dps = ways
    seq, dp = lax.axis_index("seq"), lax.axis_index("dp")
    seq_peers = [lax.rem(seq + step, seqs) for step in range(1, seqs)]
    dp_peers = [lax.rem(dp + step, dps) for step in range(1, dps)]
    meet([{"seq": peer} for peer in seq_peers] + [{"dp": peer} for peer in dp_peers])
    return seq_peers, dp_peers


def turning(ways, inside, part_ref, resid_ref, gain_ref, grad_ref, *rest):
    seqs, dps = ways
    rest = list(rest)

    def take(size):
        taken = rest[:size]
        del rest[:size]
        return taken

    if inside:
        far_refs = take(5)
    else:
        out_ref, both_ref = take(2)
    total_ref, all_ref, sums_ref, layer_ref, rows_ref = take(5)
    if inside:
        (down_rows_ref,) = take(1)
    line = LineSum(dps, lambda owner: part_ref.at[owner], *take(6))
    (own,) = take(1)
    gathered = PlaneGather(seqs, own, all_ref, *take(3))
    outs_refs, both_refs = take(6), take(4)
    if inside:
        out_ref, both_ref = take(2)
        near_refs = take(5)
        hidden_ref, down_ref, mlp_ref, back_ref, grads_ref = near_refs
        (fetch_sem,) = take(1)
        order = (2, 3, 0, 1, 4)
        fetched = fetch([(far_refs[at], near_refs[at]) for at in order], fetch_sem)
    outs = LineSum(dps, lambda owner: out_ref.at[owner], *outs_refs)
    both = Plane(seqs, both_ref, *both_refs)
    chips = dps // 2
    group, wide = both_ref.shape[1], resid_ref.shape[1]
    tile = min(256, group)

    def both_rows(source):
        @pl.loop(0, group // tile)
        def _(at):
            columns = pl.ds(pl.multiple_of(source * group + at * tile, tile), tile)
            here = pl.ds(pl.multiple_of(at * tile, tile), tile)
            both_ref[source, here, :] = contract_rows(mlp_ref[:, columns], back_ref[...]).astype(
                both_ref.dtype
            )

    def out_part():
        step = min(256, wide)

        @pl.loop(0, wide // step)
        def _(at):
            here = pl.ds(pl.multiple_of(at * step, step), step)
            value = dot(hidden_ref[...], down_ref[:, here]).astype(out_ref.dtype)
            out_ref[:, :, :, here] = value.reshape(out_ref.shape[:3] + (step,))

    def down_rows():
        count = down_rows_ref.shape[0]

        def one(here):
            down_rows_ref[here, :] = contract_rows(hidden_ref[:, here], grads_ref[...]).astype(
                down_rows_ref.dtype
            )

        @pl.loop(0, count // 128)
        def _(at):
            one(pl.ds(pl.multiple_of(at * 128, 128), 128))

        if count % 128:
            one(pl.ds(count // 128 * 128, count % 128))

    meet_cross(ways)
    line.begin()
    line.lead()
    if inside:
        fetched[0].wait()
        fetched[1].wait()

    def make(at, source):
        both_rows(source)

        @pl.when(at == 1)
        def _():
            line.step(0)

    if inside:
        both.begin(make)
    else:
        both.begin()
        line.step(0)
    if inside:
        fetched[2].wait()
        fetched[3].wait()
        out_part()
    outs.begin()
    line.step(1)
    both.relay()
    for at in range(2, chips):
        line.step(at)
    outs.lead()
    if inside:
        fetched[4].wait()
        down_rows()
    line.end()
    sums_ref[...] = jnp.zeros(sums_ref.shape, F32)
    gain = gain_ref[...]

    def one(here, piece, inner):
        grad = line.total(piece, inner)
        normed, inverse = normalize(resid_ref[here, :])
        sums_ref[2:3, :] += jnp.sum(grad * normed, axis=0, keepdims=True)
        sums_ref[3:4, :] += jnp.sum(grad, axis=0, keepdims=True)
        total = grad_ref[here, :].astype(F32) + norm_back(grad, normed, inverse, gain)
        total_ref[here, :] = total
        own[here, :] = total.astype(own.dtype)

    by_pieces(resid_ref.shape[0], one)
    gathered.begin()
    outs.step(0)
    gathered.relay()
    for at in range(1, chips):
        outs.step(at)
    both.end()

    def two(here):
        rows_ref[here, :] = both.total(here).astype(rows_ref.dtype)

    by_chunks(rows_ref.shape[0], two)
    gathered.end()
    outs.end()

    def three(here, piece, inner):
        layer_ref[here, :] = (resid_ref[here, :] + outs.total(piece, inner)).astype(layer_ref.dtype)

    by_pieces(resid_ref.shape[0], three)
    line.drain()
    outs.drain()


def turn_all(ways, part, resid, gain, grad_out, hidden, down_full, mlp_all, both_grad, grad_all, tag):
    seqs, dps = ways
    rows, wide = resid.shape
    cut = (wide // seqs, both_grad.shape[1])
    inside = dps * rows <= 1024
    pieces = (dps, PIECES, rows // PIECES, wide)
    vmem, anywhere = (pl.BlockSpec(memory_space=space) for space in (pltpu.VMEM, pl.ANY))
    operands = [part.reshape(pieces), resid, gain, grad_out]
    made = [
        jax.ShapeDtypeStruct((rows, wide), F32),
        jax.ShapeDtypeStruct((seqs, rows, wide), BF16),
        jax.ShapeDtypeStruct((8, wide), F32),
        jax.ShapeDtypeStruct((rows, wide), BF16),
        jax.ShapeDtypeStruct(cut, BF16),
    ]
    places = [vmem, anywhere, vmem, vmem, vmem]
    scratch = (
        LineSum.scratch(dps, pieces[1:], BF16)
        + [pltpu.VMEM((rows, wide), BF16)]
        + PlaneGather.scratch(seqs)
        + LineSum.scratch(dps, pieces[1:], BF16)
        + Plane.scratch(seqs, cut[0], cut[1], BF16)
    )
    if inside:
        far = [hidden, down_full, mlp_all, both_grad, grad_all]
        made.append(jax.ShapeDtypeStruct((hidden.shape[1], wide), BF16))
        places.append(vmem)
        scratch += [pltpu.VMEM(pieces, BF16), pltpu.VMEM((seqs,) + cut, BF16)]
        scratch += [pltpu.VMEM(item.shape, item.dtype) for item in far]
        scratch += [pltpu.SemaphoreType.DMA((5,))]
    else:
        out_part = dot(hidden, down_full).astype(BF16)
        both = contract_rows(mlp_all, both_grad).astype(BF16)
        down_rows = contract_rows(hidden, grad_all).astype(BF16)
        operands += [out_part.reshape(pieces), both.reshape((seqs,) + cut)]
        far = []
    results = pl.pallas_call(
        functools.partial(turning, ways, inside),
        out_shape=tuple(made),
        in_specs=[vmem] * len(operands) + [anywhere] * len(far),
        out_specs=tuple(places),
        scratch_shapes=scratch,
        cost_estimate=lasting(85),
        compiler_params=pltpu.CompilerParams(
            collective_id=tag, has_side_effects=True, vmem_limit_bytes=63 * 2**20
        ),
    )(*operands, *far)
    total, gathered, sums, layer, both = results[:5]
    if inside:
        down_rows = results[5]
    return total, gathered.reshape(seqs * rows, wide), sums, layer, both, down_rows


class SwapDp:

    def __init__(self, dps, x_ref, o_ref, send, recv, local):
        dp = lax.axis_index("dp")
        self.peers = [lax.rem(dp + step, dps) for step in range(1, dps)]
        self.parts = (x_ref, o_ref, send, recv, local, dp)

    def begin(self):
        x, o, send, recv, local, dp = self.parts
        self.copies = [
            push(x.at[peer], o.at[dp], send, recv, at, {"dp": peer})
            for at, peer in enumerate(self.peers)
        ]
        self.own = pltpu.make_async_copy(x.at[dp], o.at[dp], local)
        self.own.start()

    def end(self):
        for copy in self.copies:
            copy.wait()
        self.own.wait()

    @staticmethod
    def scratch(dps):
        dma = pltpu.SemaphoreType.DMA
        return [dma((dps - 1,)), dma((dps - 1,)), dma]


def halves():
    lane = lax.broadcasted_iota(jnp.int32, (1, 128), 1)
    return lane, (lane < HEAD_DIM, lane >= HEAD_DIM)


def reversing(
    ways, grads_ref, out_ref, qkv_ref, lse_ref, table_ref, w_far, attn_far, att_ref, both_ref, *rest
):
    dps = ways[1]
    part_ref, rows_ref, bias_ref, outs_ref, swapped_ref = rest[:5]
    swap = SwapDp(dps, both_ref, swapped_ref, *rest[5:8])
    pg_ref, grad_ref, w_ref, attn_ref, fetch_sem = rest[8:13]
    fetched = fetch([(w_far, w_ref), (attn_far, attn_ref)], fetch_sem)
    dp = lax.axis_index("dp")
    meet([{"dp": lax.rem(dp + step, dps)} for step in range(1, dps)])
    length, wide = grads_ref.shape
    group = out_ref.shape[0]
    share = outs_ref.shape[2]
    step = min(256, wide)
    swap.begin()
    scale = HEAD_DIM ** (-0.5)
    size = min(256, length)
    tile = min(256, group)

    @pl.loop(0, group // tile)
    def _(at):
        columns = pl.ds(pl.multiple_of(at * tile, tile), tile)
        grad_ref[:, columns] = contract_cols(grads_ref[...], out_ref[columns, :]).astype(
            grad_ref.dtype
        )

    _, sides = halves()
    triangle = lax.broadcasted_iota(jnp.int32, (size, size), 0) <= lax.broadcasted_iota(
        jnp.int32, (size, size), 1
    )

    @pl.loop(0, group // 128)
    def _(at):
        base = pl.multiple_of(at * 128, 128)
        query_lanes, key_lanes, value_lanes = (
            pl.ds(third * group + base, 128) for third in range(3)
        )
        key_sums = [[None] * (length // size) for _ in range(2)]
        value_sums = [[None] * (length // size) for _ in range(2)]
        for block in range(length // size):
            rows = pl.ds(block * size, size)
            seen = (block + 1) * size
            query = qkv_ref[rows, query_lanes]
            key = qkv_ref[pl.ds(0, seen), key_lanes]
            value = qkv_ref[pl.ds(0, seen), value_lanes]
            grad = grad_ref[rows, pl.ds(base, 128)]
            query_sums = []
            for half in range(2):
                mine = jnp.where(sides[half], query, jnp.zeros_like(query))
                given = jnp.where(sides[half], grad, jnp.zeros_like(grad))
                scores = contract_cols(key, mine) * scale
                total = lse_ref[pl.ds(2 * at + half, 1), rows]
                probs = jnp.exp(scores - total)
                last = jnp.where(triangle, probs[block * size :], 0.0)
                probs = jnp.concatenate([probs[: block * size], last], 0) if block else last
                probs_grad = contract_cols(value, given)
                tilt = jnp.sum(probs * probs_grad, axis=0, keepdims=True)
                scores_grad = (probs * (probs_grad - tilt)).astype(BF16)
                probs_low = probs.astype(BF16)
                query_sums.append(contract_rows(scores_grad, key))
                for part in range(block + 1):
                    cut = slice(part * size, (part + 1) * size)
                    for sums, left, right in (
                        (key_sums, scores_grad, query),
                        (value_sums, probs_low, grad),
                    ):
                        more = dot(left[cut], right)
                        held = sums[half][part]
                        sums[half][part] = more if held is None else held + more
            total = (jnp.where(sides[0], query_sums[0], query_sums[1]) * scale).astype(BF16)
            table = table_ref.at[:, rows]
            pg_ref[rows, query_lanes] = turn_lanes(total.astype(F32), table, -1.0).astype(BF16)
        for part in range(length // size):
            rows = pl.ds(part * size, size)
            total = jnp.where(sides[0], key_sums[0][part], key_sums[1][part]) * scale
            table = table_ref.at[:, rows]
            total = total.astype(BF16).astype(F32)
            pg_ref[rows, key_lanes] = turn_lanes(total, table, -1.0).astype(BF16)
            total = jnp.where(sides[0], value_sums[0][part], value_sums[1][part])
            pg_ref[rows, value_lanes] = total.astype(BF16)

    bias_ref[...] = jnp.zeros(bias_ref.shape, F32)

    @pl.loop(0, length // CHUNK)
    def _(at):
        here = pl.ds(pl.multiple_of(at * CHUNK, CHUNK), CHUNK)
        bias_ref[0:1, :] += jnp.sum(pg_ref[here, :].astype(F32), axis=0, keepdims=True)

    for copy in fetched:
        copy.wait()

    @pl.loop(0, wide // step)
    def _(at):
        columns = pl.ds(pl.multiple_of(at * step, step), step)
        part_ref[:, columns] = contract_cols(pg_ref[...], w_ref[columns, :]).astype(part_ref.dtype)
        rows_ref[columns, :] = contract_rows(attn_ref[:, columns], pg_ref[...]).astype(
            rows_ref.dtype
        )

    @pl.loop(0, wide // step)
    def _(at):
        columns = pl.ds(pl.multiple_of(at * step, step), step)
        value = contract_rows(att_ref[...], grads_ref[:, columns]).astype(outs_ref.dtype)
        outs_ref[:, 0, :, columns] = value.reshape(dps, share, step)

    swap.end()


def reverse_all(ways, grads, out_full, qkv, lse, table, qkv_full, attn_all, attended, both, tag):
    length, wide = grads.shape
    group = out_full.shape[0]
    vmem, anywhere = (pl.BlockSpec(memory_space=space) for space in (pltpu.VMEM, pl.ANY))
    return pl.pallas_call(
        functools.partial(reversing, ways),
        out_shape=(
            jax.ShapeDtypeStruct((length, wide), BF16),
            jax.ShapeDtypeStruct((wide, 3 * group), BF16),
            jax.ShapeDtypeStruct((8, 3 * group), F32),
            jax.ShapeDtypeStruct((ways[1], 1, group // ways[1], wide), BF16),
            jax.ShapeDtypeStruct(both.shape, BF16),
        ),
        in_specs=[vmem] * 5 + [anywhere] * 2 + [vmem] * 2,
        out_specs=(vmem,) * 4 + (anywhere,),
        scratch_shapes=SwapDp.scratch(ways[1])
        + [
            pltpu.VMEM((length, 3 * group), BF16),
            pltpu.VMEM((length, group), BF16),
            pltpu.VMEM(qkv_full.shape, BF16),
            pltpu.VMEM(attn_all.shape, BF16),
            pltpu.SemaphoreType.DMA((2,)),
        ],
        cost_estimate=lasting(45),
        compiler_params=pltpu.CompilerParams(
            collective_id=tag, has_side_effects=True, vmem_limit_bytes=60 * 2**20
        ),
    )(grads, out_full, qkv, lse, table, qkv_full, attn_all, attended, both)


def closing(ways, w_ref, g_ref, sums_ref, x_ref, gain_ref, resid_ref, both_ref, o_ref, *rest):
    seqs, dps = ways
    qkv_ref, grad_ref, tiny_ref, gate_ref, up_ref, shard_ref = rest[:6]
    rest = rest[1:]
    plane = Plane(seqs, g_ref, *rest[5:9])
    line = LineSum(dps, lambda owner: w_ref.at[:, owner], *rest[9:15])
    landed, mine, near, far, part_sum = rest[15:20]
    swap_s, swap_r, near_s, near_r, far_s, far_r = rest[20:26]
    outs = LineSum(dps, lambda owner: o_ref.at[owner], *rest[26:32])
    seq, dp = lax.axis_index("seq"), lax.axis_index("dp")
    seq_peers, dp_peers = meet_cross(ways)
    line.begin()
    plane.begin()
    line.lead()
    outs.begin()
    outs.lead()
    plane.relay()
    line.step(0)
    plane.end()
    part_sum[...] = sums_ref[...]
    gain = gain_ref[...]

    def one(here):
        grad = plane.total(here)
        normed, inverse = normalize(x_ref[here, :].astype(F32))
        part_sum[0:1, :] += jnp.sum(grad * normed, axis=0, keepdims=True)
        part_sum[1:2, :] += jnp.sum(grad, axis=0, keepdims=True)
        grad_ref[here, :] = (
            resid_ref[here, :] + norm_back(grad, normed, inverse, gain)
        ).astype(grad_ref.dtype)

    by_chunks(x_ref.shape[0], one)
    wide = x_ref.shape[1]
    nears = [
        push(part_sum, near.at[seq], near_s, near_r, at, {"seq": peer})
        for at, peer in enumerate(seq_peers)
    ]
    near[seq] = part_sum[...]
    line.step(1)
    for copy in nears:
        copy.wait()
    far[dp] = jnp.sum(near[...], axis=0)
    units = gate_ref.shape[1] // (seqs * dps)
    for at, weight in enumerate((gate_ref, up_ref)):
        for source in range(seqs):
            for owner in range(dps):
                weight[:, pl.ds((source * dps + owner) * units, units)] = both_ref[
                    owner, :, pl.ds((at * seqs + source) * units, units)
                ].astype(F32)
    fars = [
        push(far.at[dp], far.at[dp], far_s, far_r, at, {"dp": peer})
        for at, peer in enumerate(dp_peers)
    ]
    for at in range(2, dps // 2):
        line.step(at)
    line.end()
    for source in range(seqs):

        def three(here, source=source):
            mine[source, here] = line.total(source, here).astype(mine.dtype)

        by_chunks(mine.shape[1], three)
    swaps = [
        push(mine.at[peer], landed.at[seq], swap_s, swap_r, at, {"seq": peer})
        for at, peer in enumerate(seq_peers)
    ]
    landed[seq] = mine[seq]
    for at in range(dps // 2):
        outs.step(at)
    for copy in fars:
        copy.wait()
    tiny_ref[...] = jnp.sum(far[...], axis=0)
    for copy in swaps:
        copy.wait()
    group = w_ref.shape[3] // 3
    for source in range(seqs):
        for third in range(3):
            qkv_ref[:, pl.ds(third * wide + source * group, group)] = landed[
                source, :, pl.ds(third * group, group)
            ].astype(F32)
    outs.end()

    def last(here):
        shard_ref[here, :] = outs.total(0, here)

    by_chunks(shard_ref.shape[0], last)
    line.drain()
    outs.drain()


def close_all(ways, qkv_rows, attn_part, sums, inputs, gain, resid, both, out_rows, tag):
    seqs, dps = ways
    part = qkv_rows.shape[0] // (seqs * dps)
    wide3 = qkv_rows.shape[1]
    rows, wide = inputs.shape
    dma = pltpu.SemaphoreType.DMA
    vmem = pl.BlockSpec(memory_space=pltpu.VMEM)
    return pl.pallas_call(
        functools.partial(closing, ways),
        out_shape=(
            jax.ShapeDtypeStruct((part, 3 * wide), F32),
            jax.ShapeDtypeStruct((rows, wide), BF16),
            jax.ShapeDtypeStruct(sums.shape, F32),
            jax.ShapeDtypeStruct((part, dps * both.shape[2] // 2), F32),
            jax.ShapeDtypeStruct((part, dps * both.shape[2] // 2), F32),
            jax.ShapeDtypeStruct((part, wide), F32),
        ),
        in_specs=[vmem] * 8,
        out_specs=(vmem,) * 6,
        scratch_shapes=Plane.scratch(seqs, rows, wide, BF16)
        + LineSum.scratch(dps, (seqs, part, wide3), BF16)
        + [
            pltpu.VMEM((seqs, part, wide3), BF16),
            pltpu.VMEM((seqs, part, wide3), BF16),
            pltpu.VMEM((seqs,) + sums.shape, F32),
            pltpu.VMEM((dps,) + sums.shape, F32),
            pltpu.VMEM(sums.shape, F32),
            dma((seqs - 1,)),
            dma((seqs - 1,)),
            dma((seqs - 1,)),
            dma((seqs - 1,)),
            dma((dps - 1,)),
            dma((dps - 1,)),
        ]
        + LineSum.scratch(dps, out_rows.shape[1:], BF16),
        cost_estimate=lasting(75),
        compiler_params=pltpu.CompilerParams(collective_id=tag, has_side_effects=True),
    )(
        qkv_rows.reshape(seqs, dps, part, wide3),
        attn_part.reshape(seqs, rows, wide),
        sums,
        inputs,
        gain,
        resid,
        both,
        out_rows,
    )


def front(
    ways,
    qkv_weight_ref,
    in_ref,
    small_ref,
    gate_ref,
    up_ref,
    out_weight_ref,
    grad_ref,
    table_ref,
    w_far,
    attn_far,
    qkv_far,
    att_far,
    lse_ref,
    out_far,
    vec_ref,
    resid_ref,
    all_ref,
    grads_ref,
    both_ref,
    *rest,
):
    seqs, dps = ways
    chips, count = dps // 2, seqs * dps
    rest = list(rest)

    def take(size):
        taken = rest[:size]
        del rest[:size]
        return taken

    x_ref, given_ref, bias_ref, cut_ref, swapped_ref, branch_ref, own_ref = take(7)
    w_ref, attn_ref, qkv_ref, att_ref, out_ref, keep_sem = take(6)
    kept = []

    def keep(source, target):
        kept.append(pltpu.make_async_copy(source, target, keep_sem.at[len(kept)]))
        kept[-1].start()

    gathered = PlaneGather(seqs, in_ref, x_ref, *take(3))
    outs = LineGather(dps, out_weight_ref, out_ref, *take(5))
    swap = SwapDp(dps, cut_ref, swapped_ref, *take(3))
    plane = Plane(seqs, branch_ref, *take(4))
    moved = LineGather(dps, own_ref, all_ref, *take(5))
    grads = LineGather(dps, grad_ref, grads_ref, *take(5))
    gates = PlaneGather(seqs, swapped_ref, both_ref, *take(3))
    swap_s, swap_r, line_s, line_r, pair_s, pair_r, small_s, small_r, own_sem = take(9)
    seq, dp = lax.axis_index("seq"), lax.axis_index("dp")
    _, chip, core, ends, sides, sibling = line_place(dps)
    me = seq * dps + dp
    part, group = qkv_weight_ref.shape[0], w_ref.shape[1] // 3
    rows, width = in_ref.shape
    length = rows * seqs
    barrier = pltpu.get_barrier_semaphore()

    def other(step):
        at = lax.rem(me + step, count)
        return {"seq": at // dps, "dp": lax.rem(at, dps)}

    @pl.loop(1, count)
    def _(step):
        pl.semaphore_signal(barrier, inc=1, device_id=other(step), device_id_type=MESH)

    pl.semaphore_wait(barrier, count - 1)

    def block(source, owner):
        return w_ref.at[pl.ds(pl.multiple_of((source * dps + owner) * part, part), part), :]

    def piece(source, third):
        here = pl.ds(pl.multiple_of((source * dps + dp) * part, part), part)
        return w_ref.at[here, pl.ds(third * group, group)]

    def columns(target, third):
        at = pl.multiple_of(third * width + target * group, 128)
        return qkv_weight_ref.at[:, pl.ds(at, group)]

    swaps = []
    for step in range(1, seqs):
        target = lax.rem(seq + step, seqs)
        for third in range(3):
            at = 3 * (step - 1) + third
            swaps.append(
                push(
                    columns(target, third),
                    piece(seq, third),
                    swap_s,
                    swap_r,
                    at,
                    {"seq": target},
                )
            )
    owns = [
        pltpu.make_async_copy(columns(seq, third), piece(seq, third), own_sem.at[third])
        for third in range(3)
    ]
    for own in owns:
        own.start()

    def small_copy(step):
        return remote(
            small_ref, given_ref.at[me], small_s.at[step - 1], small_r.at[step - 1], other(step)
        )

    @pl.loop(1, count)
    def _(step):
        small_copy(step).start()

    given_ref[me] = small_ref[...]
    gathered.begin()

    def onward(side, hop, source, owner_chip):
        part_of = block(source[1], 2 * owner_chip + core)
        at = (side, hop, source[0])
        return remote(part_of, part_of, line_s.at[at], line_r.at[at], sides[side])

    def share(source, owner_chip, owner_core):
        part_of = block(source[1], 2 * owner_chip + owner_core)
        at = (owner_chip, source[0])
        return remote(part_of, part_of, pair_s.at[at], pair_r.at[at], sibling)

    sources = [(back, lax.rem(seq - back + seqs, seqs)) for back in range(seqs)]
    for source in sources:
        if source[0] == 0:
            for own in owns:
                own.wait()
        else:
            for third in range(3):
                swaps[3 * (source[0] - 1) + third].wait_recv()
        for side in range(2):

            @pl.when(ends[side])
            def _(side=side, source=source):
                onward(side, 0, source, chip).start()

        share(source, chip, core).start()
    gathered.relay()

    def pass_on(hop):
        for source in sources:
            for side in range(2):
                origin = chip - 1 - hop if side == 0 else chip + 1 + hop
                there = origin >= 0 if side == 0 else origin < chips

                @pl.when(there)
                def _(side=side, source=source, origin=origin):
                    onward(side, hop, source, origin).wait_recv()
                    share(source, origin, core).start()

                if hop < chips - 2:

                    @pl.when(jnp.logical_and(there, ends[side]))
                    def _(side=side, source=source, origin=origin):
                        onward(side, hop + 1, source, origin).start()

    units = gate_ref.shape[1] // count
    for at, weight in enumerate((gate_ref, up_ref)):
        for source in range(seqs):
            for owner in range(dps):
                cut_ref[owner, :, pl.ds((at * seqs + source) * units, units)] = weight[
                    :, pl.ds((source * dps + owner) * units, units)
                ]
    pass_on(0)

    @pl.loop(1, count)
    def _(step):
        small_copy(step).wait()

    lane, sides_of = halves()
    per = 128 // part

    def row_of(pick):
        value = jnp.zeros((1, 128), F32)
        for unit in range(per):
            found = pick(unit)
            found = pltpu.roll(found, unit * part, 1) if unit else found
            mask = (lane >= unit * part) & (lane < (unit + 1) * part)
            value = jnp.where(mask, found, value)
        return value

    for kind in range(4):

        @pl.loop(0, width // 128)
        def _(chunk, kind=kind):
            vec_ref[kind : kind + 1, pl.ds(pl.multiple_of(chunk * 128, 128), 128)] = row_of(
                lambda unit: given_ref[chunk * per + unit, kind : kind + 1]
            )

    lot = group // 128

    @pl.loop(0, 3 * lot)
    def _(chunk):
        first = chunk // lot * count + seq * dps + lax.rem(chunk, lot) * per

        def pick(unit):
            at = first + unit
            return given_ref[at // 3, pl.ds(4 + lax.rem(at, 3), 1)]

        bias_ref[0:1, pl.ds(pl.multiple_of(chunk * 128, 128), 128)] = row_of(pick)

    for hop in range(1, chips - 1):
        pass_on(hop)
    outs.begin()
    gathered.end()
    gain_one, shift_one = vec_ref[0:1, :], vec_ref[1:2, :]

    for source in range(seqs):

        def norm(here, source=source):
            normed, _ = normalize(x_ref[source, here, :].astype(F32))
            at = pl.ds(pl.multiple_of(source * rows + here.start, CHUNK), CHUNK)
            attn_ref[at, :] = (normed * gain_one + shift_one).astype(attn_ref.dtype)

        by_chunks(rows, norm)
    for owner in range(chips):
        for source in sources:
            share(source, owner, 1 - core).wait_recv()
    keep(w_ref, w_far)
    keep(attn_ref, attn_far)
    tile = min(256, group)

    def product(at):
        here = pl.ds(pl.multiple_of(at * tile, tile), tile)
        return here, dot(attn_ref[...], w_ref[:, here]) + bias_ref[0:1, here]

    @pl.loop(0, 2 * group // tile)
    def _(at):
        _, value = product(at)
        for half in range(tile // 128):
            turned = turn_lanes(value[:, half * 128 : (half + 1) * 128], table_ref, 1.0)
            here = pl.ds(pl.multiple_of(at * tile + half * 128, 128), 128)
            qkv_ref[:, here] = turned.astype(qkv_ref.dtype)

    outs.hop(0)

    @pl.loop(2 * group // tile, 3 * group // tile)
    def _(at):
        here, value = product(at)
        qkv_ref[:, here] = value.astype(qkv_ref.dtype)

    for hop in range(1, chips - 1):
        outs.hop(hop)
    swap.begin()
    keep(qkv_ref, qkv_far)
    scale = HEAD_DIM ** (-0.5)
    size = min(256, length)
    triangle = lax.broadcasted_iota(jnp.int32, (size, size), 1) <= lax.broadcasted_iota(
        jnp.int32, (size, size), 0
    )

    @pl.loop(0, group // 128)
    def _(at):
        base = pl.multiple_of(at * 128, 128)
        for part_at in range(length // size):
            here = pl.ds(part_at * size, size)
            seen = (part_at + 1) * size
            query = qkv_ref[here, pl.ds(base, 128)]
            key = qkv_ref[pl.ds(0, seen), pl.ds(group + base, 128)]
            value = qkv_ref[pl.ds(0, seen), pl.ds(2 * group + base, 128)]
            mixed = []
            for half in range(2):
                mine = jnp.where(sides_of[half], query, jnp.zeros_like(query))
                scores = contract_cols(mine, key) * scale
                last = jnp.where(triangle, scores[:, part_at * size :], -jnp.inf)
                if part_at:
                    scores = jnp.concatenate([scores[:, : part_at * size], last], 1)
                else:
                    scores = last
                largest = jnp.max(scores, axis=1, keepdims=True)
                exponent = jnp.exp(scores - largest)
                totals = jnp.sum(exponent, axis=1, keepdims=True)
                probs = (exponent * (1.0 / totals)).astype(value.dtype)
                mixed.append(dot(probs, value))
                lse_ref[here, :] = jnp.where(
                    lane == 2 * at + half, largest + jnp.log(totals), lse_ref[here, :]
                )
            att_ref[here, pl.ds(base, 128)] = jnp.where(sides_of[0], mixed[0], mixed[1]).astype(
                att_ref.dtype
            )

    outs.end()
    keep(att_ref, att_far)
    keep(out_ref, out_far)
    step = min(256, width)

    @pl.loop(0, width // step)
    def _(at):
        here = pl.ds(pl.multiple_of(at * step, step), step)
        value = jnp.zeros((length, step), F32)
        for owner in range(dps):
            value = value + dot(att_ref[:, pl.ds(owner * part, part)], out_ref[owner, :, here])
        for source in range(seqs):
            branch_ref[source, :, here] = value[source * rows : (source + 1) * rows].astype(
                branch_ref.dtype
            )

    plane.begin()
    grads.begin()
    plane.relay()
    plane.end()
    swap.end()
    gates.begin()
    gain_two, shift_two = vec_ref[2:3, :], vec_ref[3:4, :]

    def one(here):
        resid = in_ref[here, :].astype(F32) + plane.total(here)
        resid_ref[here, :] = resid
        normed, _ = normalize(resid)
        own_ref[here, :] = (normed * gain_two + shift_two).astype(own_ref.dtype)

    by_chunks(rows, one)
    moved.begin()
    for hop in range(chips - 1):
        grads.hop(hop)
        if hop == min(1, chips - 2):
            gates.relay()
        moved.hop(hop)
    grads.end()
    moved.end()
    gates.end()

    for copy in kept:
        copy.wait()
    for swapped in swaps:
        swapped.wait_send()
    for hop in range(chips - 1):
        for source in sources:
            for side in range(2):
                origin = chip - hop if side == 0 else chip + hop
                there = origin >= 0 if side == 0 else origin < chips

                @pl.when(jnp.logical_and(there, ends[side]))
                def _(side=side, hop=hop, source=source, origin=origin):
                    onward(side, hop, source, origin).wait_send()

    for owner in range(chips):
        for source in sources:
            share(source, owner, core).wait_send()


def front_all(ways, qkv_weight, inputs, small, gate, up, out_weight, grad_out, table, tag):
    seqs, dps = ways
    chips, count = dps // 2, seqs * dps
    part, width = out_weight.shape
    rows = inputs.shape[0]
    length, group, cols = rows * seqs, width // seqs, 2 * gate.shape[1] // dps
    dma = pltpu.SemaphoreType.DMA
    vmem, anywhere = (pl.BlockSpec(memory_space=space) for space in (pltpu.VMEM, pl.ANY))

    def made(dtype, *shape):
        return jax.ShapeDtypeStruct(shape, dtype)

    return pl.pallas_call(
        functools.partial(front, ways),
        out_shape=(
            made(BF16, width, 3 * group),
            made(BF16, length, width),
            made(BF16, length, 3 * group),
            made(BF16, length, group),
            made(F32, length, 128),
            made(BF16, dps, part, width),
            made(F32, 8, width),
            made(F32, rows, width),
            made(BF16, dps, rows, width),
            made(BF16, dps, rows, width),
            made(BF16, seqs, dps, part, cols),
        ),
        in_specs=[vmem] * 8,
        out_specs=(anywhere,) * 4 + (vmem, anywhere, vmem, vmem) + (anywhere,) * 3,
        scratch_shapes=[
            pltpu.VMEM((seqs, rows, width), BF16),
            pltpu.VMEM((count, 8, 128), F32),
            pltpu.VMEM((8, 3 * group), F32),
            pltpu.VMEM((dps, part, cols), BF16),
            pltpu.VMEM((dps, part, cols), BF16),
            pltpu.VMEM((seqs, rows, width), BF16),
            pltpu.VMEM((rows, width), BF16),
            pltpu.VMEM((width, 3 * group), BF16),
            pltpu.VMEM((length, width), BF16),
            pltpu.VMEM((length, 3 * group), BF16),
            pltpu.VMEM((length, group), BF16),
            pltpu.VMEM((dps, part, width), BF16),
            dma((5,)),
        ]
        + PlaneGather.scratch(seqs)
        + LineGather.scratch(dps)
        + SwapDp.scratch(dps)
        + Plane.scratch(seqs, rows, width, BF16)
        + LineGather.scratch(dps)
        + LineGather.scratch(dps)
        + PlaneGather.scratch(seqs)
        + [
            dma((3 * (seqs - 1),)),
            dma((3 * (seqs - 1),)),
            dma((2, chips - 1, seqs)),
            dma((2, chips - 1, seqs)),
            dma((chips, seqs)),
            dma((chips, seqs)),
            dma((count - 1,)),
            dma((count - 1,)),
            dma((3,)),
        ],
        cost_estimate=lasting(180),
        compiler_params=pltpu.CompilerParams(
            collective_id=tag, has_side_effects=True, vmem_limit_bytes=60 * 2**20
        ),
    )(qkv_weight, inputs, small, gate, up, out_weight, grad_out, table)


def shards(
    ways,
    inputs,
    first_gain,
    first_shift,
    qkv_weight,
    qkv_bias,
    out_weight,
    second_gain,
    second_shift,
    gate_weight,
    up_weight,
    down_weight,
    out_cotangent,
):
    seqs, dps = ways
    width = inputs.shape[2]
    rows = inputs.shape[1]
    length = rows * seqs
    part = width // (seqs * dps)
    units = down_weight.shape[0]
    group = width // seqs
    me_seq = lax.axis_index("seq")
    grad_out = out_cotangent[0]

    small = [item[None] for item in (first_gain, first_shift, second_gain, second_shift)]
    small = jnp.concatenate(small + [qkv_bias.reshape(3, part)]).astype(F32)
    small = jnp.pad(small, ((0, 1), (0, 128 - part)))
    table = tables(length)
    down_full = gather(down_weight, "seq")
    (
        qkv_full,
        attn_all,
        qkv,
        attended,
        log_total,
        out_full,
        vectors,
        residual,
        mlp_all,
        grad_all,
        gate_up,
    ) = front_all(
        ways,
        qkv_weight,
        inputs[0],
        small,
        gate_weight,
        up_weight,
        out_weight,
        grad_out,
        table,
        0,
    )
    out_full = out_full.reshape(group, width)
    gain_one, gain_two = vectors[0:1], vectors[2:3]
    mlp_all = mlp_all.reshape(dps * rows, width)
    grad_all = grad_all.reshape(dps * rows, width)
    gate_up = gate_up.reshape(width, 2 * seqs * units)
    wide = seqs * units

    both = dot(mlp_all, gate_up)
    gate_value = both[:, :wide]
    up_value = both[:, wide:]
    sigmoid_gate = jax.nn.sigmoid(gate_value)
    activated = gate_value * sigmoid_gate
    hidden = (activated * up_value).astype(BF16)

    hidden_grad = contract_cols(grad_all, down_full)
    gate_grad = (
        hidden_grad * up_value * (sigmoid_gate * (1.0 + gate_value * (1.0 - sigmoid_gate)))
    ).astype(BF16)
    up_grad = (hidden_grad * activated).astype(BF16)
    both_grad = jnp.concatenate([gate_grad, up_grad], 1)
    mlp_part = contract_cols(both_grad, gate_up).astype(BF16)
    residual_grad, branch_all, sums, layer_out, both_rows, down_rows = turn_all(
        ways,
        mlp_part,
        residual,
        gain_two,
        grad_out,
        hidden,
        down_full,
        mlp_all,
        both_grad,
        grad_all,
        2,
    )
    down_shard = scatter_sum(down_rows, "seq").astype(F32)

    attn_part, qkv_rows, bias_term, out_rows, both_rows = reverse_all(
        ways,
        branch_all,
        out_full,
        qkv,
        log_total.T,
        table,
        qkv_full,
        attn_all,
        attended,
        both_rows.reshape(dps, part, 2 * seqs * units),
        5,
    )
    bias_term = bias_term[0].reshape(3, 1, group)
    here = (jnp.arange(seqs, dtype=jnp.int32) == me_seq).astype(F32)[None, :, None]
    bias_term = jnp.pad((bias_term * here).reshape(3, width), ((4, 1), (0, 0)))
    sums = sums + bias_term
    qkv_shard, input_grad, tiny, gate_shard, up_shard, out_shard = close_all(
        ways,
        qkv_rows,
        attn_part,
        sums,
        inputs[0],
        gain_one,
        residual_grad,
        both_rows,
        out_rows,
        3,
    )
    me = me_seq * dps + lax.axis_index("dp")
    mine = lax.dynamic_slice_in_dim(tiny, me * part, part, 1)
    bias_shard = lax.dynamic_slice_in_dim(tiny[4:7].reshape(-1), me * 3 * part, 3 * part, 0)

    return (
        layer_out[None],
        input_grad[None],
        mine[0],
        mine[1],
        qkv_shard,
        bias_shard,
        out_shard,
        mine[2],
        mine[3],
        gate_shard,
        up_shard,
        down_shard,
    )


def solution(mesh):
    split = ("seq", "dp")
    tokens = P("dp", "seq", None)
    in_specs = (
        tokens,
        P(split),
        P(split),
        P(split, None),
        P(split),
        P(split, None),
        P(split),
        P(split),
        P(split, None),
        P(split, None),
        P(split, None),
        tokens,
    )
    out_specs = (
        tokens,
        tokens,
        P(split),
        P(split),
        P(split, None),
        P(split),
        P(split, None),
        P(split),
        P(split),
        P(split, None),
        P(split, None),
        P(split, None),
    )
    ways = (mesh.shape["seq"], mesh.shape["dp"])

    def local(*args):
        return shards(ways, *args)

    return jax.shard_map(local, mesh=mesh, in_specs=in_specs, out_specs=out_specs, check_vma=False)
```
